32 devices in a mesh: dp: 8 (over z, y), head: 4 (over x, core).
Axes of the slice: x: 2, y: 2, z: 4, core: 2. Of those that a mesh axis runs over, the one named last changes fastest.
Arguments:
- tokens: bfloat16 [32768, 768], P(('dp', 'head')), may hold values from -6 to 6
- seq_lengths: int32 [64, 32], P('dp'), may hold values from 0 to 512, as said below
- qkv_weight: bfloat16 [2, 3, 768, 768], P(None, None, None, 'head'), may hold values from -0.21875 to 0.21875
- qv_bias: float32 [2, 2, 768], P(None, None, 'head'), may hold values from -3 to 3
- out_weight: bfloat16 [2, 768, 768], replicated, may hold values from -0.875 to 0.875
- out_bias: float32 [2, 768], replicated, may hold values from -3 to 3
- norm1_gain: float32 [2, 768], replicated, may hold values from 0.25 to 1.75
- norm1_shift: float32 [2, 768], replicated, may hold values from -3 to 3
- up_weight: bfloat16 [2, 768, 3072], replicated, may hold values from -0.21875 to 0.21875
- up_bias: float32 [2, 3072], replicated, may hold values from -3 to 3
- down_weight: bfloat16 [2, 3072, 768], replicated, may hold values from -0.109375 to 0.109375
- down_bias: float32 [2, 768], replicated, may hold values from -3 to 3
- norm2_gain: float32 [2, 768], replicated, may hold values from 0.25 to 1.75
- norm2_shift: float32 [2, 768], replicated, may hold values from -3 to 3
- out_grad: bfloat16 [32768, 768], P(('dp', 'head')), may hold values from -6 to 6
Outputs:
- out_state: bfloat16 [32768, 768], P(('dp', 'head'))
- input_grad: bfloat16 [32768, 768], P(('dp', 'head'))
- qkv_weight_grad: float32 [2, 3, 768, 768], P(None, None, 'dp', 'head')
- qv_bias_grad: float32 [2, 2, 768], replicated
- out_weight_grad: float32 [2, 768, 768], P(None, 'dp', 'head')
- out_bias_grad: float32 [2, 768], replicated
- norm1_gain_grad: float32 [2, 768], replicated
- norm1_shift_grad: float32 [2, 768], replicated
- up_weight_grad: float32 [2, 768, 3072], P(None, 'dp', 'head')
- up_bias_grad: float32 [2, 3072], replicated
- down_weight_grad: float32 [2, 3072, 768], P(None, 'head', 'dp')
- down_bias_grad: float32 [2, 768], replicated
- norm2_gain_grad: float32 [2, 768], replicated
- norm2_shift_grad: float32 [2, 768], replicated
The draws below stay inside these ranges and needn't reach their ends.
Inputs may be any that keep to these rules, and one draw needn't show every extreme that they name: `seq_lengths`: each slot's row sums to 512; nonzero entries come first and zero entries mark no sequence; some slot holds a single sequence of 512 rows.
All inputs are finite; a program needn't handle non-finite values.
Results may differ from the reference program's by a relative error of at most 0.025.
Values may be sent and summed in bfloat16 or wider, within the bound.
No kernel may reach another device: no remote copies, remote signals or barrier semaphores. Data moves between devices by JAX's collectives and lax.ppermute only.
A program may use at most 256 MiB of HBM per device.

```python
import jax
import jax.numpy as jnp
from jax import lax

D = 768
HEADS = 12
HD = 64
FF = 3072
L = 2
SLOT = 512
MAXSEQ = 32
SLOTS = 64
ROWS = 32768


def draw_seq_lengths(key, part):
    key_kind, key_count, key_cut = jax.random.split(key, 3)
    single = jax.random.randint(key_kind, (SLOTS,), 0, 4) == 0
    single = single.at[0].set(True)
    seq_count = jax.random.randint(key_count, (SLOTS,), 2, MAXSEQ + 1)
    seq_count = jnp.where(single, 1, seq_count)
    slot_keys = jax.random.split(key_cut, SLOTS)

    def draw_cuts(slot_key):
        return jax.random.permutation(slot_key, SLOT - 1)[:MAXSEQ - 1] + 1
    cut_points = jax.vmap(draw_cuts)(slot_keys).astype(jnp.int32)
    cut_rank = jnp.arange(MAXSEQ - 1, dtype=jnp.int32)[None, :]
    cut_points = jnp.where(cut_rank < seq_count[:, None] - 1, cut_points, SLOT)
    cut_points = jnp.sort(cut_points, axis=1)
    bounds = jnp.concatenate([jnp.zeros((SLOTS, 1), jnp.int32), cut_points, jnp.full((SLOTS, 1), SLOT, jnp.int32)], axis=1)
    return (bounds[:, 1:] - bounds[:, :-1]).astype(jnp.int32)


def spiked(entries, own_key, source, target, blocks, factor):
    def block_of(axis_at):
        return (jnp.arange(entries.shape[axis_at]) // (entries.shape[axis_at] // blocks)).reshape((-1,) + (1,) * (entries.ndim - 1 - axis_at))

    first = jax.random.permutation(own_key, blocks)[block_of(target)]
    far = (block_of(target) + blocks // 2) % blocks
    return jnp.where((block_of(source) == first) | (block_of(source) == far), factor * entries, entries)


def shard_levels(rng, dims, cuts, least, high):
    def one(axis_at, blocks):
        draws = jax.random.uniform(jax.random.fold_in(jax.random.fold_in(rng, 6), axis_at), (blocks,), jnp.float32, least / len(cuts), high / len(cuts))
        return jnp.repeat(jnp.exp(draws), dims[axis_at] // blocks).reshape((-1,) + (1,) * (len(dims) - axis_at - 1))

    level = one(*cuts[0])
    for cut in cuts[1:]:
        level = level * one(*cut)
    return level


def bell_draw(own_key, extent, width, reach, cuts=(), held_as=jnp.bfloat16):
    values = width * jax.random.normal(own_key, extent, jnp.float32)
    if cuts:
        values = values * shard_levels(own_key, extent, cuts, -0.22, 0.18)
    return jnp.clip(values, -reach, reach).astype(held_as)


def heavy_noise(stream_key, extent, width, reach, shards, heavy, kind=jnp.bfloat16):
    drawn = width * jax.random.normal(stream_key, extent, jnp.float32)
    if shards:
        drawn = drawn * shard_levels(stream_key, extent, shards, -0.22, 0.18)
    return jnp.clip(spiked(drawn, jax.random.fold_in(stream_key, 3), *heavy), -reach, reach).astype(kind)


def setup_inputs(seed: int = 0) -> dict:
    key_of = jax.random.split(jax.random.key(seed), 16)
    return {
        "tokens": bell_draw(key_of[0], (ROWS, D), 1.0, 6.0, ((0, 32),)),
        "seq_lengths": draw_seq_lengths(jax.random.fold_in(key_of[15], 71), 0),
        "qkv_weight": bell_draw(key_of[2], (L, 3, D, D), D ** -0.5, 0.21875, ((3, 4),)),
        "qv_bias": bell_draw(key_of[3], (L, 2, D), 0.5, 3.0, ((2, 4),), jnp.float32),
        "out_weight": bell_draw(key_of[4], (L, D, D), (D // 16) ** -0.5, 0.875),
        "out_bias": bell_draw(key_of[5], (L, D), 0.5, 3.0, (), jnp.float32),
        "norm1_gain": jnp.clip(1.0 + 0.15 * jax.random.normal(key_of[6], (L, D), jnp.float32), 0.25, 1.75),
        "norm1_shift": bell_draw(key_of[7], (L, D), 0.5, 3.0, (), jnp.float32),
        "up_weight": bell_draw(key_of[8], (L, D, FF), D ** -0.5, 0.21875),
        "up_bias": bell_draw(key_of[9], (L, FF), 0.5, 3.0, (), jnp.float32),
        "down_weight": bell_draw(key_of[10], (L, FF, D), FF ** -0.5, 0.109375),
        "down_bias": bell_draw(key_of[11], (L, D), 0.5, 3.0, (), jnp.float32),
        "norm2_gain": jnp.clip(1.0 + 0.15 * jax.random.normal(key_of[12], (L, D), jnp.float32), 0.25, 1.75),
        "norm2_shift": bell_draw(key_of[13], (L, D), 0.5, 3.0, (), jnp.float32),
        "out_grad": heavy_noise(key_of[14], (ROWS, D), 1.0, 6.0, ((0, 32),), (0, 1, 32, 2.75)),
    }


EPSILON = 1e-06
PRECISE = lax.Precision.HIGHEST

@jax.custom_vjp
def low(v):
    return lax.optimization_barrier(v.astype(jnp.bfloat16)).astype(jnp.float32)

@jax.custom_vjp
def low_back(v):
    return v

def low_keep(v):
    return (low(v), None)

def low_pass(kept, grad):
    return (grad,)

def back_keep(v):
    return (v, None)

def back_low(kept, grad):
    return (low(grad),)
low.defvjp(low_keep, low_pass)
low_back.defvjp(back_keep, back_low)

def matmul(left, right):
    return jnp.dot(left, right, precision=PRECISE, preferred_element_type=jnp.float32)

def norm_rows(values, gain, shift):
    centre = lax.optimization_barrier(jnp.mean(values, axis=-1, keepdims=True))
    centred = values - centre
    spread = lax.optimization_barrier(jnp.mean(centred * centred, axis=-1, keepdims=True))
    return centred * lax.rsqrt(spread + EPSILON) * gain + shift

def segment_ids(lengths, slot_rows):
    boundary = jnp.cumsum(lengths, axis=1)
    position = jnp.arange(slot_rows, dtype=jnp.int32)
    return lax.optimization_barrier(jnp.sum((position[None, :, None] >= boundary[:, None, :]).astype(jnp.int32), axis=2))

def slot_attention(queries, keys_in, values_in, segments):
    scaling = queries.shape[-1] ** (-0.5)
    scores = low_back(jnp.einsum('qhd,khd->hqk', queries, keys_in, precision=PRECISE) * scaling)
    inside = (segments[:, None] == segments[None, :])[None]
    scores = jnp.where(inside, scores, -1e+30)
    peak_score = lax.optimization_barrier(jnp.max(scores, axis=-1, keepdims=True))
    weights = jnp.exp(scores - peak_score)
    denominator = lax.optimization_barrier(jnp.sum(weights, axis=-1, keepdims=True))
    probability = low(weights / denominator)
    return jnp.einsum('hqk,khd->qhd', probability, values_in, precision=PRECISE)

def forward(hidden_state, segments, parameters):
    qkv, qvb, wout, bout, gain1, shift1, wup, bup, wdown, bdown, gain2, shift2 = parameters
    row_count = hidden_state.shape[0]
    slot_count = segments.shape[0]
    attend = jax.checkpoint(slot_attention)

    def attend_packed(packed):
        return attend(packed[0], packed[1], packed[2], packed[3])
    for layer_index in range(L):
        rounded = low(hidden_state)
        queries = low(low_back(matmul(rounded, qkv[layer_index, 0]) + qvb[layer_index, 0]))
        keys_in = low(low_back(matmul(rounded, qkv[layer_index, 1])))
        values_in = low(low_back(matmul(rounded, qkv[layer_index, 2]) + qvb[layer_index, 1]))
        shaped = (slot_count, SLOT, HEADS, HD)
        context = lax.map(attend_packed, (queries.reshape(shaped), keys_in.reshape(shaped), values_in.reshape(shaped), segments))
        context = low(low_back(context.reshape(row_count, D)))
        attended = low_back(matmul(context, wout[layer_index]) + bout[layer_index])
        normed = norm_rows(hidden_state + attended, gain1[layer_index], shift1[layer_index])
        before_gelu = low_back(matmul(low(normed), wup[layer_index]) + bup[layer_index])
        activated = low(jax.nn.gelu(before_gelu, approximate=False))
        branch = low_back(matmul(activated, wdown[layer_index]) + bdown[layer_index])
        hidden_state = norm_rows(normed + branch, gain2[layer_index], shift2[layer_index])
    return hidden_state

def reference(tokens, seq_lengths, qkv_weight, qv_bias, out_weight, out_bias, norm1_gain, norm1_shift, up_weight, up_bias, down_weight, down_bias, norm2_gain, norm2_shift, out_grad):
    parameters = tuple((item.astype(jnp.float32) for item in (qkv_weight, qv_bias, out_weight, out_bias, norm1_gain, norm1_shift, up_weight, up_bias, down_weight, down_bias, norm2_gain, norm2_shift)))
    segments = segment_ids(seq_lengths, SLOT)
    slots_block = 4
    block_count = SLOTS // slots_block
    block_rows = slots_block * SLOT
    states = tokens.astype(jnp.float32).reshape(block_count, block_rows, D)
    cotangents = out_grad.astype(jnp.float32).reshape(block_count, block_rows, D)
    block_segments = segments.reshape(block_count, slots_block, SLOT)
    zero_grads = jax.tree.map(jnp.zeros_like, parameters)

    def one_block(running, packed):
        state_in, segment_in, cotangent_in = packed

        def run_block(values, weights):
            return forward(values, segment_in, weights)
        result, pull = jax.vjp(run_block, state_in, parameters)
        grad_in, grad_weights = pull(cotangent_in)
        return (jax.tree.map(jnp.add, running, grad_weights), (result, grad_in))
    totals, (results, grads_in) = lax.scan(one_block, zero_grads, (states, block_segments, cotangents))
    out_state = results.reshape(ROWS, D).astype(jnp.bfloat16)
    input_grad = grads_in.reshape(ROWS, D).astype(jnp.bfloat16)
    return (out_state, input_grad, totals[0], totals[1], totals[2], totals[3], totals[4], totals[5], totals[6], totals[7], totals[8], totals[9], totals[10], totals[11])
```

```python
import jax
import jax.numpy as jnp
from jax import lax
from jax.sharding import PartitionSpec as P

HD = 64


EPSILON = 1e-06


def norm_rows(values, gain, shift):
    centre = jnp.mean(values, axis=-1, keepdims=True)
    centred = values - centre
    spread = jnp.mean(centred * centred, axis=-1, keepdims=True)
    return centred * lax.rsqrt(spread + EPSILON) * gain + shift


def exact_gelu(values):
    return jax.nn.gelu(values, approximate=False)


def segment_ids(lengths, slot_rows):
    order = jnp.arange(lengths.shape[1], dtype=jnp.int32)
    upto = order[:, None] <= order[None, :]
    boundary = jnp.sum(jnp.where(upto[None], lengths[:, :, None], 0), axis=1)
    position = jnp.arange(slot_rows, dtype=jnp.int32)
    return jnp.sum((position[None, :, None] >= boundary[:, None, :]).astype(jnp.int32), axis=2)


def slot_scores(queries, keys_in, segments):
    scaling = queries.shape[-1] ** (-0.5)
    scores = (
        jnp.einsum("qhd,khd->hqk", queries, keys_in, preferred_element_type=jnp.float32) * scaling
    )
    inside = (segments[:, None] == segments[None, :])[None]
    return (scores, inside)


def slot_forward(packed):
    queries, keys_in, values_in, segments = packed
    scores, inside = slot_scores(queries, keys_in, segments)
    scores = jnp.where(inside, scores, -1e30)
    peak_score = jnp.max(scores, axis=-1, keepdims=True)
    weights = jnp.exp(scores - peak_score)
    denominator = jnp.sum(weights, axis=-1, keepdims=True)
    probability = (weights / denominator).astype(jnp.bfloat16)
    context = jnp.einsum("hqk,khd->qhd", probability, values_in, preferred_element_type=jnp.float32)
    return (context.astype(jnp.bfloat16), (peak_score + jnp.log(denominator))[..., 0])


def slot_backward(packed):
    queries, keys_in, values_in, grad_context, log_total, segments = packed
    scaling = queries.shape[-1] ** (-0.5)
    scores, inside = slot_scores(queries, keys_in, segments)
    probability = jnp.where(inside, jnp.exp(scores - log_total[..., None]), 0.0)
    grad_prob = jnp.einsum(
        "qhd,khd->hqk", grad_context, values_in, preferred_element_type=jnp.float32
    )
    shares = jnp.sum(probability * grad_prob, axis=-1, keepdims=True)
    grad_score = (probability * (grad_prob - shares)).astype(jnp.bfloat16)
    grad_query = (
        jnp.einsum("hqk,khd->qhd", grad_score, keys_in, preferred_element_type=jnp.float32)
        * scaling
    )
    grad_key = (
        jnp.einsum("hqk,qhd->khd", grad_score, queries, preferred_element_type=jnp.float32)
        * scaling
    )
    grad_value = jnp.einsum(
        "hqk,qhd->khd",
        probability.astype(jnp.bfloat16),
        grad_context,
        preferred_element_type=jnp.float32,
    )
    return (
        grad_query.astype(jnp.bfloat16),
        grad_key.astype(jnp.bfloat16),
        grad_value.astype(jnp.bfloat16),
    )


def chunked(grad, dp_count, head_count):
    rows, columns = grad.shape
    split = grad.reshape(dp_count, rows // dp_count, head_count, columns // head_count)
    return jnp.transpose(split, (0, 2, 1, 3)).reshape(dp_count * head_count, -1, rows)


def on_device(
    tokens,
    seq_lengths,
    qkv_weight,
    qv_bias,
    out_weight,
    out_bias,
    norm1_gain,
    norm1_shift,
    up_weight,
    up_bias,
    down_weight,
    down_bias,
    norm2_gain,
    norm2_shift,
    out_grad,
):
    head_count = lax.axis_size("head")
    dp_count = lax.axis_size("dp")
    head_index = lax.axis_index("head")
    local_rows, model_width = tokens.shape
    slots_group = seq_lengths.shape[0]
    slot_rows = local_rows * head_count // slots_group
    slots = local_rows // slot_rows
    lengths = lax.dynamic_slice_in_dim(seq_lengths, head_index * slots, slots, 0)
    segments = segment_ids(lengths, slot_rows)
    layers = qkv_weight.shape[0]
    heads = model_width // HD
    full_bias = lax.all_gather(qv_bias, "head", axis=2, tiled=True)
    full_qkv = [
        lax.all_gather(qkv_weight[layer], "head", axis=2, tiled=True) for layer in range(layers)
    ]
    hidden_state = tokens.astype(jnp.float32)
    kept = []
    for layer in range(layers):
        rounded = hidden_state.astype(jnp.bfloat16)
        weights = full_qkv[layer]

        def project(which, bias):
            made = jnp.dot(rounded, weights[which], preferred_element_type=jnp.float32)
            if bias is not None:
                made = made + bias
            return made.astype(jnp.bfloat16).reshape(slots, slot_rows, heads, HD)

        queries = project(0, full_bias[layer, 0])
        keys_in = project(1, None)
        values_in = project(2, full_bias[layer, 1])
        context, log_total = lax.map(slot_forward, (queries, keys_in, values_in, segments))
        context = context.reshape(local_rows, model_width)
        attended = (
            jnp.dot(context, out_weight[layer], preferred_element_type=jnp.float32)
            + out_bias[layer]
        )
        first_sum = hidden_state + attended
        normed = norm_rows(first_sum, norm1_gain[layer], norm1_shift[layer])
        normed_low = normed.astype(jnp.bfloat16)
        before_gelu = (
            jnp.dot(normed_low, up_weight[layer], preferred_element_type=jnp.float32)
            + up_bias[layer]
        )
        activated = exact_gelu(before_gelu).astype(jnp.bfloat16)
        branch = jnp.dot(activated, down_weight[layer], preferred_element_type=jnp.float32)
        second_sum = normed + branch + down_bias[layer]
        hidden_state = norm_rows(second_sum, norm2_gain[layer], norm2_shift[layer])
        kept.append(
            (
                rounded,
                queries,
                keys_in,
                values_in,
                log_total,
                context,
                first_sum,
                normed_low,
                before_gelu,
                activated,
                second_sum,
            )
        )
    out_state = hidden_state.astype(jnp.bfloat16)
    grad_state = out_grad.astype(jnp.float32)
    summed = [None] * layers
    small = [None] * layers
    shifts = [None] * layers
    for layer in reversed(range(layers)):
        (
            rounded,
            queries,
            keys_in,
            values_in,
            log_total,
            context,
            first_sum,
            normed_low,
            before_gelu,
            activated,
            second_sum,
        ) = kept[layer]
        pull_second = jax.vjp(norm_rows, second_sum, norm2_gain[layer], norm2_shift[layer])[1]
        grad_second, grad_gain2, grad_shift2 = pull_second(grad_state)
        grad_branch = grad_second.astype(jnp.bfloat16)
        grad_down_shift = jnp.sum(grad_branch.astype(jnp.float32), axis=0)
        grad_down = jnp.einsum(
            "rd,rf->df", grad_branch, activated, preferred_element_type=jnp.float32
        )
        grad_act = jnp.einsum(
            "rd,fd->rf", grad_branch, down_weight[layer], preferred_element_type=jnp.float32
        )
        pull_gelu = jax.vjp(exact_gelu, before_gelu)[1]
        grad_pre = pull_gelu(grad_act)[0].astype(jnp.bfloat16)
        grad_up_shift = jnp.sum(grad_pre.astype(jnp.float32), axis=0)
        grad_up = jnp.einsum("rd,rf->df", normed_low, grad_pre, preferred_element_type=jnp.float32)
        grad_normed = grad_second + jnp.einsum(
            "rf,df->rd", grad_pre, up_weight[layer], preferred_element_type=jnp.float32
        )
        pull_first = jax.vjp(norm_rows, first_sum, norm1_gain[layer], norm1_shift[layer])[1]
        grad_first, grad_gain1, grad_shift1 = pull_first(grad_normed)
        grad_attended = grad_first.astype(jnp.bfloat16)
        grad_out_shift = jnp.sum(grad_attended.astype(jnp.float32), axis=0)
        grad_out = jnp.einsum("rd,re->de", context, grad_attended, preferred_element_type=jnp.float32)
        grad_context = jnp.einsum(
            "re,de->rd", grad_attended, out_weight[layer], preferred_element_type=jnp.float32
        ).astype(jnp.bfloat16)
        parts = lax.map(
            slot_backward,
            (
                queries,
                keys_in,
                values_in,
                grad_context.reshape(slots, slot_rows, heads, HD),
                log_total,
                segments,
            ),
        )
        parts = [part.reshape(local_rows, model_width) for part in parts]
        grad_qkv = [
            jnp.einsum("rd,re->de", rounded, part, preferred_element_type=jnp.float32)
            for part in parts
        ]
        grad_state = grad_first
        for which in range(3):
            grad_state = grad_state + jnp.einsum(
                "re,de->rd",
                parts[which],
                full_qkv[layer][which],
                preferred_element_type=jnp.float32,
            )
        packed = jnp.concatenate(
            [
                chunked(grad.astype(jnp.bfloat16), dp_count, head_count)
                for grad in (grad_up, grad_down, *grad_qkv, grad_out)
            ],
            axis=1,
        )
        summed[layer] = lax.psum_scatter(
            packed, ("dp", "head"), scatter_dimension=0, tiled=True
        )[0].astype(jnp.float32)
        small[layer] = jnp.stack(
            [
                jnp.sum(parts[0].astype(jnp.float32), axis=0),
                jnp.sum(parts[2].astype(jnp.float32), axis=0),
                grad_out_shift,
                grad_gain1,
                grad_shift1,
                grad_down_shift,
                grad_gain2,
                grad_shift2,
            ]
        )
        shifts[layer] = grad_up_shift
    input_grad = grad_state.astype(jnp.bfloat16)
    small_sum, shift_sum = lax.psum((jnp.stack(small), jnp.stack(shifts)), ("dp", "head"))
    sums = jnp.stack(summed)
    dp_rows = model_width // dp_count
    head_width = model_width // head_count
    ffn_width = up_weight.shape[2] // head_count
    tall = dp_rows * ffn_width // model_width
    short = dp_rows * head_width // model_width
    up_sum = sums[:, :tall].reshape(layers, dp_rows, ffn_width)
    down_sum = sums[:, tall : 2 * tall].reshape(layers, dp_rows, ffn_width)
    wide = sums[:, 2 * tall :].reshape(layers, 4, dp_rows, head_width)
    return (
        out_state,
        input_grad,
        wide[:, :3],
        small_sum[:, 0:2],
        wide[:, 3],
        small_sum[:, 2],
        small_sum[:, 3],
        small_sum[:, 4],
        up_sum,
        shift_sum,
        jnp.transpose(down_sum, (0, 2, 1)),
        small_sum[:, 5],
        small_sum[:, 6],
        small_sum[:, 7],
    )


def solution(mesh):
    in_specs = (
        P(("dp", "head"), None),
        P("dp", None),
        P(None, None, None, "head"),
        P(None, None, "head"),
        P(),
        P(),
        P(),
        P(),
        P(),
        P(),
        P(),
        P(),
        P(),
        P(),
        P(("dp", "head"), None),
    )
    out_specs = (
        P(("dp", "head"), None),
        P(("dp", "head"), None),
        P(None, None, "dp", "head"),
        P(),
        P(None, "dp", "head"),
        P(),
        P(),
        P(),
        P(None, "dp", "head"),
        P(),
        P(None, "head", "dp"),
        P(),
        P(),
        P(),
    )
    return jax.shard_map(
        on_device, mesh=mesh, in_specs=in_specs, out_specs=out_specs, check_vma=False
    )
```

```python
import functools

import jax
import jax.numpy as jnp
from jax import lax
from jax.experimental import pallas as pl
from jax.experimental.pallas import tpu as pltpu
from jax.sharding import PartitionSpec as P

HD = 64
EPSILON = 1e-06
GROUP = 256
LOW = jnp.bfloat16
WIDE = jnp.float32
VMEM_BYTES = 56 << 20
ROOT_HALF = 0.7071067811865476
INV_ROOT_TAU = 0.3989422804014327


def row_stats(values):
    centre = jnp.mean(values, axis=-1, keepdims=True)
    centred = values - centre
    spread = jnp.mean(centred * centred, axis=-1, keepdims=True)
    inverse = lax.rsqrt(spread + EPSILON)
    return centred * inverse, inverse


def dot_nn(left, right):
    return jnp.dot(left, right, preferred_element_type=WIDE)


def dot_nt(left, right):
    return lax.dot_general(left, right, (((1,), (1,)), ((), ())), preferred_element_type=WIDE)


def dot_tn(left, right):
    return lax.dot_general(left, right, (((0,), (0,)), ((), ())), preferred_element_type=WIDE)


def ffn_forward_kernel(
    o_ref, x_ref, wo_ref, wu_ref, wd_ref, bu_ref, small_ref,
    u1_ref, hr_ref, gr_ref, gp_ref, u2_ref, *outs, chunk,
):
    attended = dot_nn(o_ref[...], wo_ref[...])
    u1 = x_ref[...].astype(WIDE) + attended + small_ref[0:1]
    u1_ref[...] = u1
    xhat, _ = row_stats(u1)
    normed = xhat * small_ref[1:2] + small_ref[2:3]
    hr = normed.astype(LOW)
    hr_ref[...] = hr
    total = normed + small_ref[3:4]
    for start in range(0, wu_ref.shape[1], chunk):
        at = slice(start, start + chunk)
        z = dot_nn(hr, wu_ref[:, at]) + bu_ref[:, at]
        g, slope = gelu_pair(z)
        gr = g.astype(LOW)
        gr_ref[:, at] = gr
        gp_ref[:, at] = slope.astype(LOW)
        total = total + dot_nn(gr, wd_ref[at, :])
    u2_ref[...] = total
    xhat, _ = row_stats(total)
    made = xhat * small_ref[4:5] + small_ref[5:6]
    for out in outs:
        out[...] = made.astype(out.dtype)


def whole(array):
    return pl.BlockSpec(array.shape, lambda *ids: (0,) * array.ndim, pipeline_mode=pl.Buffered(1))


def params():
    return pltpu.CompilerParams(vmem_limit_bytes=VMEM_BYTES)


def rows_spec(tile, width):
    return pl.BlockSpec((tile, width), lambda i: (i, 0))


def ffn_forward(o, x, wo, wu, wd, bu, small, out_types, tile=256, chunk=512):
    rows, width = o.shape
    hidden = wu.shape[1]
    made = lambda w, t: jax.ShapeDtypeStruct((rows, w), t)
    outs = [made(width, WIDE), made(width, LOW), made(hidden, LOW), made(hidden, LOW), made(width, WIDE)]
    outs += [made(width, t) for t in out_types]
    return pl.pallas_call(
        functools.partial(ffn_forward_kernel, chunk=chunk),
        grid=(rows // tile,),
        in_specs=[rows_spec(tile, width), rows_spec(tile, width), whole(wo), whole(wu), whole(wd), whole(bu), whole(small)],
        out_specs=[rows_spec(tile, s.shape[1]) for s in outs],
        out_shape=outs,
        compiler_params=params(),
        name="ffn_forward",
    )(o, x, wo, wu, wd, bu, small)


def norm_backward(upstream, xhat, inverse, gain):
    scaled = upstream * gain
    first = jnp.mean(scaled, axis=-1, keepdims=True)
    second = jnp.mean(scaled * xhat, axis=-1, keepdims=True)
    return (scaled - first - xhat * second) * inverse


def column_sum(values):
    return jnp.sum(values, axis=0, keepdims=True)


def ffn_backward_kernel(
    gx_ref, u2_ref, u1_ref, gp_ref, wd_ref, wu_ref, wo_ref, gain_ref,
    df_ref, dz_ref, da_ref, do_ref, du_ref, sums_ref, zsum_ref, *, chunk,
):
    @pl.when(pl.program_id(0) == 0)
    def _():
        sums_ref[...] = jnp.zeros_like(sums_ref)
        zsum_ref[...] = jnp.zeros_like(zsum_ref)

    gx = gx_ref[...].astype(WIDE)
    xhat, inverse = row_stats(u2_ref[...])
    sums_ref[0:1] += column_sum(gx * xhat)
    sums_ref[1:2] += column_sum(gx)
    gv = norm_backward(gx, xhat, inverse, gain_ref[1:2])
    df = gv.astype(LOW)
    df_ref[...] = df
    sums_ref[2:3] += column_sum(df.astype(WIDE))
    total = gv
    for start in range(0, wu_ref.shape[1], chunk):
        at = slice(start, start + chunk)
        dg = dot_nt(df, wd_ref[at, :])
        dz = (dg * gp_ref[:, at].astype(WIDE)).astype(LOW)
        dz_ref[:, at] = dz
        zsum_ref[:, at] += column_sum(dz.astype(WIDE))
        total = total + dot_nt(dz, wu_ref[:, at])
    xhat, inverse = row_stats(u1_ref[...])
    sums_ref[3:4] += column_sum(total * xhat)
    sums_ref[4:5] += column_sum(total)
    du = norm_backward(total, xhat, inverse, gain_ref[0:1])
    du_ref[...] = du
    da = du.astype(LOW)
    da_ref[...] = da
    sums_ref[5:6] += column_sum(da.astype(WIDE))
    do_ref[...] = dot_nt(da, wo_ref[...]).astype(LOW)


def ffn_backward(gx, u2, u1, gp, wd, wu, wo, gains, tile=256, chunk=512):
    rows, width = gx.shape
    hidden = wu.shape[1]
    made = lambda w, t: jax.ShapeDtypeStruct((rows, w), t)
    outs = [made(width, LOW), made(hidden, LOW), made(width, LOW), made(width, LOW), made(width, WIDE)]
    sums = [jax.ShapeDtypeStruct((8, width), WIDE), jax.ShapeDtypeStruct((1, hidden), WIDE)]
    keep = lambda s: pl.BlockSpec(s.shape, lambda i: (0, 0))
    return pl.pallas_call(
        functools.partial(ffn_backward_kernel, chunk=chunk),
        grid=(rows // tile,),
        in_specs=[rows_spec(tile, width)] * 3 + [rows_spec(tile, hidden)] + [whole(wd), whole(wu), whole(wo), whole(gains)],
        out_specs=[rows_spec(tile, s.shape[1]) for s in outs] + [keep(s) for s in sums],
        out_shape=outs + sums,
        compiler_params=params(),
        name="ffn_backward",
    )(gx, u2, u1, gp, wd, wu, wo, gains)


def weight_grad_kernel(a_ref, b_ref, out_ref, t_ref):
    @pl.when(pl.program_id(0) == 0)
    def _():
        t_ref[...] = a_ref[...].T

    out_ref[...] = dot_nn(t_ref[...], b_ref[...]).astype(LOW)


def weight_grad(a, b, width):
    rows, depth = a.shape
    count = b.shape[1] // width
    return pl.pallas_call(
        weight_grad_kernel,
        grid=(count,),
        in_specs=[whole(a), pl.BlockSpec((rows, width), lambda i: (0, i))],
        out_specs=pl.BlockSpec((None, depth, width), lambda i: (i, 0, 0)),
        out_shape=jax.ShapeDtypeStruct((count, depth, width), LOW),
        scratch_shapes=[pltpu.VMEM((depth, rows), LOW)],
        compiler_params=params(),
        name="weight_grad",
    )(a, b)


def gelu_pair(z):
    cdf = 0.5 + 0.5 * lax.erf(z * ROOT_HALF)
    return z * cdf, cdf + z * (jnp.exp(z * z * -0.5) * INV_ROOT_TAU)


def head_lanes(group):
    return lax.broadcasted_iota(jnp.int32, (1, group), 1) // HD


def pick(mask, values):
    return jnp.where(mask, values, jnp.zeros_like(values))


def attention_forward_kernel(
    x_ref, w_ref, b_ref, bias_ref, q_ref, k_ref, v_ref, p_ref, o_ref, s_ref, *, tile
):
    rows, group = q_ref.shape
    x = x_ref[...]
    q = ((dot_nn(x, w_ref[0]) + b_ref[0]).astype(LOW) * HD**-0.5).astype(LOW)
    k = dot_nn(x, w_ref[1]).astype(LOW)
    v = (dot_nn(x, w_ref[2]) + b_ref[1]).astype(LOW)
    q_ref[...] = q
    k_ref[...] = k
    v_ref[...] = v
    lanes = head_lanes(group)
    total = None
    for head in range(group // HD):
        mask = lanes == head
        s_ref[head] = dot_nt(pick(mask, q), k)
        for start in range(0, rows, tile):
            at = slice(start, start + tile)
            s = s_ref[head, at] + bias_ref[at]
            e = jnp.exp(s - jnp.max(s, axis=1, keepdims=True))
            p_ref[head, at] = (e * (1.0 / jnp.sum(e, axis=1, keepdims=True))).astype(LOW)
        part = dot_nn(p_ref[head], pick(mask, v))
        total = part if total is None else total + part
    o_ref[...] = total.astype(LOW)


def attention_forward(x, w, qv_bias, bias, tile=64):
    rows, width = x.shape
    slots, slot_rows, _ = bias.shape
    groups = width // GROUP
    per = GROUP // HD
    row = pl.BlockSpec((slot_rows, GROUP), lambda s, g: (s, g))
    made = jax.ShapeDtypeStruct((rows, width), LOW)
    probs = jax.ShapeDtypeStruct((slots * groups * per, slot_rows, slot_rows), LOW)
    return pl.pallas_call(
        functools.partial(attention_forward_kernel, tile=tile),
        grid=(slots, groups),
        in_specs=[
            pl.BlockSpec((slot_rows, width), lambda s, g: (s, 0)),
            pl.BlockSpec((3, width, GROUP), lambda s, g: (0, 0, g)),
            pl.BlockSpec((2, 1, GROUP), lambda s, g: (0, 0, g)),
            pl.BlockSpec((None, slot_rows, slot_rows), lambda s, g: (s, 0, 0)),
        ],
        out_specs=[row, row, row, pl.BlockSpec((per, slot_rows, slot_rows), lambda s, g: (s * groups + g, 0, 0)), row],
        out_shape=[made, made, made, probs, made],
        scratch_shapes=[pltpu.VMEM((per, slot_rows, slot_rows), WIDE)],
        compiler_params=params(),
        name="attention_forward",
    )(x, w, qv_bias, bias)


def attention_backward_kernel(
    q_ref, k_ref, v_ref, do_ref, p_ref, dq_ref, dk_ref, dv_ref, sums_ref, t_ref, ds_ref, *, tile
):
    rows, group = q_ref.shape
    lanes = head_lanes(group)
    dq = dk = dv = None
    for head in range(group // HD):
        mask = lanes == head
        do = pick(mask, do_ref[...])
        t_ref[head] = dot_nt(do, v_ref[...])
        for start in range(0, rows, tile):
            at = slice(start, start + tile)
            p = p_ref[head, at].astype(WIDE)
            dp = t_ref[head, at]
            share = jnp.sum(p * dp, axis=1, keepdims=True)
            ds_ref[head, at] = (p * (dp - share)).astype(LOW)
        parts = (
            dot_nn(ds_ref[head], pick(mask, k_ref[...])),
            dot_tn(ds_ref[head], pick(mask, q_ref[...])),
            dot_tn(p_ref[head], do),
        )
        dq, dk, dv = parts if dq is None else (dq + parts[0], dk + parts[1], dv + parts[2])
    dq = (dq * HD**-0.5).astype(LOW)
    dv = dv.astype(LOW)
    dq_ref[...] = dq
    dk_ref[...] = dk.astype(LOW)
    dv_ref[...] = dv

    @pl.when(pl.program_id(1) == 0)
    def _():
        sums_ref[...] = jnp.zeros_like(sums_ref)

    sums_ref[0:1] += column_sum(dq.astype(WIDE))
    sums_ref[1:2] += column_sum(dv.astype(WIDE))


def attention_backward(q, k, v, do, p, tile=64):
    rows, width = q.shape
    slot_rows = p.shape[1]
    slots = rows // slot_rows
    groups = width // GROUP
    per = GROUP // HD
    row = pl.BlockSpec((slot_rows, GROUP), lambda g, s: (s, g))
    made = jax.ShapeDtypeStruct((rows, width), LOW)
    return pl.pallas_call(
        functools.partial(attention_backward_kernel, tile=tile),
        grid=(groups, slots),
        in_specs=[row] * 4 + [pl.BlockSpec((per, slot_rows, slot_rows), lambda g, s: (s * groups + g, 0, 0))],
        out_specs=[row] * 3 + [pl.BlockSpec((8, GROUP), lambda g, s: (0, g))],
        out_shape=[made] * 3 + [jax.ShapeDtypeStruct((8, width), WIDE)],
        scratch_shapes=[pltpu.VMEM((per, slot_rows, slot_rows), WIDE), pltpu.VMEM((per, slot_rows, slot_rows), LOW)],
        compiler_params=params(),
        name="attention_backward",
    )(q, k, v, do, p)


def mask_kernel(base_ref, lengths_ref, bias_ref):
    slots, rows, _ = bias_ref.shape
    count = lengths_ref.shape[1]
    across = lax.broadcasted_iota(jnp.int32, (8, rows), 1)
    down = lax.broadcasted_iota(jnp.int32, (rows, 128), 0)
    for slot in range(slots):
        reach = jnp.int32(0)
        seg_across = jnp.zeros((8, rows), jnp.int32)
        seg_down = jnp.zeros((rows, 128), jnp.int32)
        for k in range(count):
            reach = reach + lengths_ref[base_ref[0] + slot, k]
            seg_across += (across >= reach).astype(jnp.int32)
            seg_down += (down >= reach).astype(jnp.int32)
        inside = seg_down[:, 0:1] == seg_across[0:1, :]
        bias_ref[slot] = jnp.where(inside, 0.0, -1e30)


def mask_bias(lengths, base, slots, slot_rows):
    smem = pl.BlockSpec(memory_space=pltpu.SMEM)
    return pl.pallas_call(
        mask_kernel,
        in_specs=[smem, smem],
        out_shape=jax.ShapeDtypeStruct((slots, slot_rows, slot_rows), WIDE),
        compiler_params=params(),
        name="mask_bias",
    )(base, lengths)


def qkv_grads(x, o, dq, dk, dv, da, heads):
    rows, depth = x.shape
    part = depth // heads

    def kernel(x_ref, o_ref, dq_ref, dk_ref, dv_ref, da_ref, out_ref, xt_ref, ot_ref):
        @pl.when(pl.program_id(0) == 0)
        def _():
            xt_ref[...] = x_ref[...].T
            ot_ref[...] = o_ref[...].T

        for head in range(heads):

            @pl.when(pl.program_id(0) == head)
            def _():
                at = slice(head * part, (head + 1) * part)
                joined = jnp.concatenate([dq_ref[:, at], dk_ref[:, at], dv_ref[:, at]], axis=1)
                first = dot_nn(xt_ref[...], joined)
                second = dot_nn(ot_ref[...], da_ref[:, at])
                out_ref[...] = jnp.concatenate([first, second], axis=1).astype(LOW)

    return pl.pallas_call(
        kernel,
        grid=(heads,),
        in_specs=[whole(v) for v in (x, o, dq, dk, dv, da)],
        out_specs=pl.BlockSpec((None, depth, 4 * part), lambda i: (i, 0, 0)),
        out_shape=jax.ShapeDtypeStruct((heads, depth, 4 * part), LOW),
        scratch_shapes=[pltpu.VMEM((depth, rows), LOW)] * 2,
        compiler_params=params(),
        name="qkv_grads",
    )(x, o, dq, dk, dv, da)


def input_grad_kernel(du_ref, dq_ref, dk_ref, dv_ref, w_ref, out_ref):
    total = du_ref[...]
    for which, part in enumerate((dq_ref, dk_ref, dv_ref)):
        total = total + dot_nt(part[...], w_ref[which])
    out_ref[...] = total.astype(out_ref.dtype)


def input_grad(du, dq, dk, dv, w, out_type, tile=256):
    rows, width = du.shape
    return pl.pallas_call(
        input_grad_kernel,
        grid=(rows // tile,),
        in_specs=[rows_spec(tile, width)] * 4 + [whole(w)],
        out_specs=rows_spec(tile, width),
        out_shape=jax.ShapeDtypeStruct((rows, width), out_type),
        compiler_params=params(),
        name="input_grad",
    )(du, dq, dk, dv, w)


def bits_of(axis):
    size = lax.axis_size(axis)
    return [1 << bit for bit in range(size.bit_length() - 1)]


def swap(value, axis, bit):
    size = lax.axis_size(axis)
    return lax.ppermute(value, axis, [(i, i ^ bit) for i in range(size)])


def my_bit(axis, bit):
    return (lax.axis_index(axis) // bit) % 2


def gather_over(value, axis):
    blocks = [value]
    for bit in bits_of(axis):
        blocks = blocks + [swap(block, axis, bit) for block in blocks]
    mine = lax.axis_index(axis)
    stacked = jnp.stack(blocks)
    return [
        lax.dynamic_index_in_dim(stacked, block ^ mine, 0, keepdims=False)
        for block in range(len(blocks))
    ]


def sum_everywhere(value, axes):
    for axis in axes:
        for bit in bits_of(axis):
            value = value + swap(value, axis, bit)
    return value


def sum_and_scatter(value, order):
    head_count, dp_count = lax.axis_size("head"), lax.axis_size("dp")
    head_bits, dp_bits = bits_of("head")[::-1], bits_of("dp")[::-1]
    names = [("head", bit) for bit in head_bits] + [("dp", bit) for bit in dp_bits]
    rows = value.shape[1] // dp_count
    value = value.reshape([2] * len(names) + [rows, value.shape[2]])
    for step, (axis, bit) in enumerate(order):
        at = names.index((axis, bit))
        names.pop(at)
        mine = my_bit(axis, bit)
        kept = lax.dynamic_index_in_dim(value, mine, at, keepdims=False)
        sent = lax.dynamic_index_in_dim(value, 1 - mine, at, keepdims=False)
        value = kept.astype(WIDE) + swap(sent, axis, bit).astype(WIDE)
        if step < len(order) - 1:
            value = value.astype(LOW)
    return value


def stage_orders():
    head = [("head", bit) for bit in bits_of("head")]
    dp = [("dp", bit) for bit in bits_of("dp")]
    return head + dp, head[:1] + dp[:1] + head[1:] + dp[1:]


def on_device(
    tokens,
    seq_lengths,
    qkv_weight,
    qv_bias,
    out_weight,
    out_bias,
    norm1_gain,
    norm1_shift,
    up_weight,
    up_bias,
    down_weight,
    down_bias,
    norm2_gain,
    norm2_shift,
    out_grad,
):
    head_count = lax.axis_size("head")
    dp_count = lax.axis_size("dp")
    head_index = lax.axis_index("head")
    local_rows, width = tokens.shape
    slot_rows = local_rows * head_count // seq_lengths.shape[0]
    slots = local_rows // slot_rows
    layers = qkv_weight.shape[0]
    hidden = up_weight.shape[2]
    first_bias = jnp.concatenate(gather_over(qv_bias, "head"), axis=2)
    full_qkv = [jnp.concatenate(gather_over(qkv_weight[0], "head"), axis=2)]
    for layer in range(1, layers):
        full_qkv.append(lax.all_gather(qkv_weight[layer], "head", axis=2, tiled=True))
    base = (head_index * slots).astype(jnp.int32).reshape(1)
    bias = mask_bias(seq_lengths, base, slots, slot_rows)
    rounded, residual = tokens, tokens
    kept = []
    for layer in range(layers):
        q, k, v, probs, context = attention_forward(
            rounded, full_qkv[layer], first_bias[layer][:, None], bias
        )
        small = jnp.stack(
            [
                out_bias[layer],
                norm1_gain[layer],
                norm1_shift[layer],
                down_bias[layer],
                norm2_gain[layer],
                norm2_shift[layer],
            ]
        )
        last = layer == layers - 1
        u1, hr, gr, slope, u2, *made = ffn_forward(
            context,
            residual,
            out_weight[layer],
            up_weight[layer],
            down_weight[layer],
            up_bias[layer][None],
            small,
            (LOW,) if last else (LOW, WIDE),
            chunk=width,
        )
        kept.append((rounded, q, k, v, probs, context, u1, hr, gr, slope, u2))
        rounded, residual = made[0], made[-1]
    out_state = rounded
    grad_state = out_grad
    orders = stage_orders()
    summed = [None] * layers
    small_sums = [None] * layers
    hidden_sums = [None] * layers
    for layer in reversed(range(layers)):
        rounded, q, k, v, probs, context, u1, hr, gr, slope, u2 = kept[layer]
        gains = jnp.stack([norm1_gain[layer], norm2_gain[layer]])
        df, dz, da, do, du, sums, hidden_sums[layer] = ffn_backward(
            grad_state,
            u2,
            u1,
            slope,
            down_weight[layer],
            up_weight[layer],
            out_weight[layer],
            gains,
            chunk=width,
        )
        down_sum = sum_and_scatter(weight_grad(df, gr, hidden // head_count), orders[0])
        up_sum = sum_and_scatter(weight_grad(hr, dz, hidden // head_count), orders[1])
        dq, dk, dv, qv_sums = attention_backward(q, k, v, do, probs)
        wide_sum = sum_and_scatter(
            qkv_grads(rounded, context, dq, dk, dv, da, head_count), orders[0]
        )
        grad_state = input_grad(du, dq, dk, dv, full_qkv[layer], WIDE if layer else LOW)
        summed[layer] = (up_sum, down_sum, wide_sum)
        small_sums[layer] = jnp.concatenate([sums[:6], qv_sums[:2]])
    small_sum, hidden_sum = (
        sum_everywhere(jnp.stack(part), ("head", "dp")) for part in (small_sums, hidden_sums)
    )
    part = width // head_count
    wide = [layer_sums[2].reshape(-1, 4, part).transpose(1, 0, 2) for layer_sums in summed]
    return (
        out_state,
        grad_state,
        jnp.stack([w[:3] for w in wide]),
        small_sum[:, 6:8],
        jnp.stack([w[3] for w in wide]),
        small_sum[:, 5],
        small_sum[:, 3],
        small_sum[:, 4],
        jnp.stack([layer_sums[0] for layer_sums in summed]),
        hidden_sum[:, 0],
        jnp.stack([layer_sums[1].T for layer_sums in summed]),
        small_sum[:, 2],
        small_sum[:, 0],
        small_sum[:, 1],
    )


def solution(mesh):
    in_specs = (
        P(("dp", "head"), None),
        P("dp", None),
        P(None, None, None, "head"),
        P(None, None, "head"),
        P(),
        P(),
        P(),
        P(),
        P(),
        P(),
        P(),
        P(),
        P(),
        P(),
        P(("dp", "head"), None),
    )
    out_specs = (
        P(("dp", "head"), None),
        P(("dp", "head"), None),
        P(None, None, "dp", "head"),
        P(),
        P(None, "dp", "head"),
        P(),
        P(),
        P(),
        P(None, "dp", "head"),
        P(),
        P(None, "head", "dp"),
        P(),
        P(),
        P(),
    )
    return jax.shard_map(
        on_device, mesh=mesh, in_specs=in_specs, out_specs=out_specs, check_vma=False
    )
```

```python
import functools

import jax
import jax.numpy as jnp
from jax import lax
from jax.experimental import pallas as pl
from jax.experimental.pallas import tpu as pltpu
from jax.sharding import PartitionSpec as P

HD = 64
EPSILON = 1e-06
GROUP = 256
LOW = jnp.bfloat16
WIDE = jnp.float32
VMEM_BYTES = 56 << 20
ROOT_HALF = 0.7071067811865476
INV_ROOT_TAU = 0.3989422804014327


def row_stats(values):
    centre = jnp.mean(values, axis=-1, keepdims=True)
    centred = values - centre
    spread = jnp.mean(centred * centred, axis=-1, keepdims=True)
    inverse = lax.rsqrt(spread + EPSILON)
    return centred * inverse, inverse


def dot_nn(left, right):
    return jnp.dot(left, right, preferred_element_type=WIDE)


def dot_nt(left, right):
    return lax.dot_general(left, right, (((1,), (1,)), ((), ())), preferred_element_type=WIDE)


def dot_tn(left, right):
    return lax.dot_general(left, right, (((0,), (0,)), ((), ())), preferred_element_type=WIDE)


def ffn_forward_kernel(
    o_ref, x_ref, wo_ref, wu_ref, wd_ref, bu_ref, small_ref,
    u1_ref, hr_ref, gr_ref, gp_ref, u2_ref, *outs, chunk,
):
    attended = dot_nn(o_ref[...], wo_ref[...])
    u1 = x_ref[...].astype(WIDE) + attended + small_ref[0:1]
    u1_ref[...] = u1
    xhat, _ = row_stats(u1)
    normed = xhat * small_ref[1:2] + small_ref[2:3]
    hr = normed.astype(LOW)
    hr_ref[...] = hr
    total = normed + small_ref[3:4]
    for start in range(0, wu_ref.shape[1], chunk):
        at = slice(start, start + chunk)
        z = dot_nn(hr, wu_ref[:, at]) + bu_ref[:, at]
        g, slope = gelu_pair(z)
        gr = g.astype(LOW)
        gr_ref[:, at] = gr
        gp_ref[:, at] = slope.astype(LOW)
        total = total + dot_nn(gr, wd_ref[at, :])
    u2_ref[...] = total
    xhat, _ = row_stats(total)
    made = xhat * small_ref[4:5] + small_ref[5:6]
    for out in outs:
        out[...] = made.astype(out.dtype)


def whole(array):
    return pl.BlockSpec(array.shape, lambda *ids: (0,) * array.ndim, pipeline_mode=pl.Buffered(1))


def params():
    return pltpu.CompilerParams(vmem_limit_bytes=VMEM_BYTES)


def rows_spec(tile, width):
    return pl.BlockSpec((tile, width), lambda i: (i, 0))


def ffn_forward(o, x, wo, wu, wd, bu, small, out_types, tile=256, chunk=512):
    rows, width = o.shape
    hidden = wu.shape[1]
    made = lambda w, t: jax.ShapeDtypeStruct((rows, w), t)
    outs = [made(width, WIDE), made(width, LOW), made(hidden, LOW), made(hidden, LOW), made(width, WIDE)]
    outs += [made(width, t) for t in out_types]
    return pl.pallas_call(
        functools.partial(ffn_forward_kernel, chunk=chunk),
        grid=(rows // tile,),
        in_specs=[rows_spec(tile, width), rows_spec(tile, width), whole(wo), whole(wu), whole(wd), whole(bu), whole(small)],
        out_specs=[rows_spec(tile, s.shape[1]) for s in outs],
        out_shape=outs,
        compiler_params=params(),
        name="ffn_forward",
    )(o, x, wo, wu, wd, bu, small)


def norm_backward(upstream, xhat, inverse, gain):
    scaled = upstream * gain
    first = jnp.mean(scaled, axis=-1, keepdims=True)
    second = jnp.mean(scaled * xhat, axis=-1, keepdims=True)
    return (scaled - first - xhat * second) * inverse


def column_sum(values):
    return jnp.sum(values, axis=0, keepdims=True)


def ffn_backward_kernel(
    gx_ref, u2_ref, u1_ref, gp_ref, wd_ref, wu_ref, wo_ref, gain_ref,
    df_ref, dz_ref, da_ref, do_ref, du_ref, sums_ref, zsum_ref, *, chunk,
):
    @pl.when(pl.program_id(0) == 0)
    def _():
        sums_ref[...] = jnp.zeros_like(sums_ref)
        zsum_ref[...] = jnp.zeros_like(zsum_ref)

    gx = gx_ref[...].astype(WIDE)
    xhat, inverse = row_stats(u2_ref[...])
    sums_ref[0:1] += column_sum(gx * xhat)
    sums_ref[1:2] += column_sum(gx)
    gv = norm_backward(gx, xhat, inverse, gain_ref[1:2])
    df = gv.astype(LOW)
    df_ref[...] = df
    sums_ref[2:3] += column_sum(df.astype(WIDE))
    total = gv
    for start in range(0, wu_ref.shape[1], chunk):
        at = slice(start, start + chunk)
        dg = dot_nt(df, wd_ref[at, :])
        dz = (dg * gp_ref[:, at].astype(WIDE)).astype(LOW)
        dz_ref[:, at] = dz
        zsum_ref[:, at] += column_sum(dz.astype(WIDE))
        total = total + dot_nt(dz, wu_ref[:, at])
    xhat, inverse = row_stats(u1_ref[...])
    sums_ref[3:4] += column_sum(total * xhat)
    sums_ref[4:5] += column_sum(total)
    du = norm_backward(total, xhat, inverse, gain_ref[0:1])
    du_ref[...] = du
    da = du.astype(LOW)
    da_ref[...] = da
    sums_ref[5:6] += column_sum(da.astype(WIDE))
    do_ref[...] = dot_nt(da, wo_ref[...]).astype(LOW)


def ffn_backward(gx, u2, u1, gp, wd, wu, wo, gains, tile=256, chunk=512):
    rows, width = gx.shape
    hidden = wu.shape[1]
    made = lambda w, t: jax.ShapeDtypeStruct((rows, w), t)
    outs = [made(width, LOW), made(hidden, LOW), made(width, LOW), made(width, LOW), made(width, WIDE)]
    sums = [jax.ShapeDtypeStruct((8, width), WIDE), jax.ShapeDtypeStruct((1, hidden), WIDE)]
    keep = lambda s: pl.BlockSpec(s.shape, lambda i: (0, 0))
    return pl.pallas_call(
        functools.partial(ffn_backward_kernel, chunk=chunk),
        grid=(rows // tile,),
        in_specs=[rows_spec(tile, width)] * 3 + [rows_spec(tile, hidden)] + [whole(wd), whole(wu), whole(wo), whole(gains)],
        out_specs=[rows_spec(tile, s.shape[1]) for s in outs] + [keep(s) for s in sums],
        out_shape=outs + sums,
        compiler_params=params(),
        name="ffn_backward",
    )(gx, u2, u1, gp, wd, wu, wo, gains)


def reversed_bits(value, count):
    made = 0
    for bit in range(count):
        made |= (value >> bit & 1) << (count - 1 - bit)
    return made


def put_chunks(out_ref, made, dp_count):
    rows = made.shape[0] // dp_count
    rest = dp_count.bit_length() - 2
    for dp in range(dp_count):
        chunk = made[dp * rows : (dp + 1) * rows]
        out_ref[dp & 1, reversed_bits(dp >> 1, rest)] = chunk


def chunk_spec(dp_count, rows, columns, dp_first, pick_block):
    rest = dp_count // 2
    if dp_first:
        shape = (2, None, rest, rows, columns)
        return pl.BlockSpec(shape, lambda i, *refs: (0, pick_block(i), 0, 0, 0))
    return pl.BlockSpec((None, 2, rest, rows, columns), lambda i, *refs: (pick_block(i), 0, 0, 0, 0))


def first_two(i):
    return jnp.minimum(i, 1)


def last_two(i):
    return jnp.maximum(i - 2, 0)


def weight_grad_kernel(bit_ref, a_ref, b_ref, send_ref, keep_ref, t_ref, *, dp_count):
    step = pl.program_id(0)

    @pl.when(step == 0)
    def _():
        t_ref[...] = a_ref[...].T

    made = dot_nn(t_ref[...], b_ref[...]).astype(LOW)

    @pl.when(step < 2)
    def _():
        put_chunks(send_ref, made, dp_count)

    @pl.when(step >= 2)
    def _():
        put_chunks(keep_ref, made, dp_count)


def weight_grad(a, b, core, dp_count, dp_first):
    rows, depth = a.shape
    width = b.shape[1] // 4
    chunk = depth // dp_count
    made = jax.ShapeDtypeStruct((2, 2, dp_count // 2, chunk, width), LOW)

    def block(i, core_ref):
        other = 1 - core_ref[0]
        return (0, jnp.where(i < 2, 2 * i + other, 2 * (i - 2) + core_ref[0]))

    return pl.pallas_call(
        functools.partial(weight_grad_kernel, dp_count=dp_count),
        grid_spec=pltpu.PrefetchScalarGridSpec(
            num_scalar_prefetch=1,
            grid=(4,),
            in_specs=[whole(a), pl.BlockSpec((rows, width), block)],
            out_specs=[
                chunk_spec(dp_count, chunk, width, dp_first, first_two),
                chunk_spec(dp_count, chunk, width, dp_first, last_two),
            ],
            scratch_shapes=[pltpu.VMEM((depth, rows), LOW)],
        ),
        out_shape=[made, made],
        compiler_params=params(),
        name="weight_grad",
    )(core, a, b)


def add_split_kernel(bits_ref, *refs, parts, merged):
    ins, outs = refs[: 2 * parts], refs[2 * parts :]
    phase = pl.program_id(0)
    for part in range(parts):
        made = (ins[2 * part][...].astype(WIDE) + ins[2 * part + 1][...].astype(WIDE)).astype(LOW)
        send, keep = (outs[0].at[part], outs[1].at[part]) if merged else outs[2 * part : 2 * part + 2]

        @pl.when(phase == 0)
        def _():
            send[...] = made

        @pl.when(phase == 1)
        def _():
            keep[...] = made


def add_split(pairs, bits, merged=False):
    parts = len(pairs)
    shape = pairs[0][0].shape
    half = shape[0] // 2
    steps = 2 if half % 2 == 0 and half > 2 else 1
    block = half // steps
    tail = shape[1:]
    zeros = (0,) * len(tail)

    def source(part):
        def index(phase, i, bits_ref):
            mine = bits_ref[part]
            return (jnp.where(phase == 0, 1 - mine, mine) * steps + i, *zeros)

        return index

    send_at = lambda phase, i: jnp.where(phase == 0, i, steps - 1)
    keep_at = lambda phase, i: jnp.where(phase == 0, 0, i)
    ins = [pl.BlockSpec((block, *tail), source(part)) for part in range(parts) for _ in range(2)]
    if merged:
        outs = [
            pl.BlockSpec((parts, block, *tail), lambda phase, i, r, at=at: (0, at(phase, i), *zeros))
            for at in (send_at, keep_at)
        ]
        out_shape = [jax.ShapeDtypeStruct((parts, half, *tail), LOW)] * 2
    else:
        outs = [
            pl.BlockSpec((block, *tail), lambda phase, i, r, at=at: (at(phase, i), *zeros))
            for _ in range(parts)
            for at in (send_at, keep_at)
        ]
        out_shape = [jax.ShapeDtypeStruct((half, *tail), LOW)] * (2 * parts)
    return pl.pallas_call(
        functools.partial(add_split_kernel, parts=parts, merged=merged),
        grid_spec=pltpu.PrefetchScalarGridSpec(
            num_scalar_prefetch=1, grid=(2, steps), in_specs=ins, out_specs=outs
        ),
        out_shape=out_shape,
        compiler_params=params(),
        name="add_split",
    )(bits, *[value for pair in pairs for value in pair])


def gelu_pair(z):
    cdf = 0.5 + 0.5 * lax.erf(z * ROOT_HALF)
    return z * cdf, cdf + z * (jnp.exp(z * z * -0.5) * INV_ROOT_TAU)


def head_lanes(group):
    return lax.broadcasted_iota(jnp.int32, (1, group), 1) // HD


def pick(mask, values):
    return jnp.where(mask, values, jnp.zeros_like(values))


def attention_forward_kernel(
    x_ref, w_ref, b_ref, bias_ref, q_ref, k_ref, v_ref, p_ref, o_ref, s_ref, *, tile
):
    rows, group = q_ref.shape
    x = x_ref[...]
    q = ((dot_nn(x, w_ref[0]) + b_ref[0]).astype(LOW) * HD**-0.5).astype(LOW)
    k = dot_nn(x, w_ref[1]).astype(LOW)
    v = (dot_nn(x, w_ref[2]) + b_ref[1]).astype(LOW)
    q_ref[...] = q
    k_ref[...] = k
    v_ref[...] = v
    lanes = head_lanes(group)
    total = None
    for head in range(group // HD):
        mask = lanes == head
        s_ref[head] = dot_nt(pick(mask, q), k)
        for start in range(0, rows, tile):
            at = slice(start, start + tile)
            s = s_ref[head, at] + bias_ref[at]
            e = jnp.exp(s - jnp.max(s, axis=1, keepdims=True))
            p_ref[head, at] = (e * (1.0 / jnp.sum(e, axis=1, keepdims=True))).astype(LOW)
        part = dot_nn(p_ref[head], pick(mask, v))
        total = part if total is None else total + part
    o_ref[...] = total.astype(LOW)


def attention_forward(x, w, qv_bias, bias, tile=64):
    rows, width = x.shape
    slots, slot_rows, _ = bias.shape
    groups = width // GROUP
    per = GROUP // HD
    row = pl.BlockSpec((slot_rows, GROUP), lambda s, g: (s, g))
    made = jax.ShapeDtypeStruct((rows, width), LOW)
    probs = jax.ShapeDtypeStruct((slots * groups * per, slot_rows, slot_rows), LOW)
    return pl.pallas_call(
        functools.partial(attention_forward_kernel, tile=tile),
        grid=(slots, groups),
        in_specs=[
            pl.BlockSpec((slot_rows, width), lambda s, g: (s, 0)),
            pl.BlockSpec((3, width, GROUP), lambda s, g: (0, 0, g)),
            pl.BlockSpec((2, 1, GROUP), lambda s, g: (0, 0, g)),
            pl.BlockSpec((None, slot_rows, slot_rows), lambda s, g: (s, 0, 0)),
        ],
        out_specs=[row, row, row, pl.BlockSpec((per, slot_rows, slot_rows), lambda s, g: (s * groups + g, 0, 0)), row],
        out_shape=[made, made, made, probs, made],
        scratch_shapes=[pltpu.VMEM((per, slot_rows, slot_rows), WIDE)],
        compiler_params=params(),
        name="attention_forward",
    )(x, w, qv_bias, bias)


def attention_backward_kernel(
    q_ref, k_ref, v_ref, do_ref, p_ref, dq_ref, dk_ref, dv_ref, sums_ref, t_ref, ds_ref, *, tile
):
    rows, group = q_ref.shape
    lanes = head_lanes(group)
    dq = dk = dv = None
    for head in range(group // HD):
        mask = lanes == head
        do = pick(mask, do_ref[...])
        t_ref[head] = dot_nt(do, v_ref[...])
        for start in range(0, rows, tile):
            at = slice(start, start + tile)
            p = p_ref[head, at].astype(WIDE)
            dp = t_ref[head, at]
            share = jnp.sum(p * dp, axis=1, keepdims=True)
            ds_ref[head, at] = (p * (dp - share)).astype(LOW)
        parts = (
            dot_nn(ds_ref[head], pick(mask, k_ref[...])),
            dot_tn(ds_ref[head], pick(mask, q_ref[...])),
            dot_tn(p_ref[head], do),
        )
        dq, dk, dv = parts if dq is None else (dq + parts[0], dk + parts[1], dv + parts[2])
    dq = (dq * HD**-0.5).astype(LOW)
    dv = dv.astype(LOW)
    dq_ref[...] = dq
    dk_ref[...] = dk.astype(LOW)
    dv_ref[...] = dv

    @pl.when(pl.program_id(1) == 0)
    def _():
        sums_ref[...] = jnp.zeros_like(sums_ref)

    sums_ref[0:1] += column_sum(dq.astype(WIDE))
    sums_ref[1:2] += column_sum(dv.astype(WIDE))


def attention_backward(q, k, v, do, p, tile=64):
    rows, width = q.shape
    slot_rows = p.shape[1]
    slots = rows // slot_rows
    groups = width // GROUP
    per = GROUP // HD
    row = pl.BlockSpec((slot_rows, GROUP), lambda g, s: (s, g))
    made = jax.ShapeDtypeStruct((rows, width), LOW)
    return pl.pallas_call(
        functools.partial(attention_backward_kernel, tile=tile),
        grid=(groups, slots),
        in_specs=[row] * 4 + [pl.BlockSpec((per, slot_rows, slot_rows), lambda g, s: (s * groups + g, 0, 0))],
        out_specs=[row] * 3 + [pl.BlockSpec((8, GROUP), lambda g, s: (0, g))],
        out_shape=[made] * 3 + [jax.ShapeDtypeStruct((8, width), WIDE)],
        scratch_shapes=[pltpu.VMEM((per, slot_rows, slot_rows), WIDE), pltpu.VMEM((per, slot_rows, slot_rows), LOW)],
        compiler_params=params(),
        name="attention_backward",
    )(q, k, v, do, p)


def mask_kernel(base_ref, lengths_ref, bias_ref):
    slots, rows, _ = bias_ref.shape
    count = lengths_ref.shape[1]
    across = lax.broadcasted_iota(jnp.int32, (8, rows), 1)
    down = lax.broadcasted_iota(jnp.int32, (rows, 128), 0)
    for slot in range(slots):
        reach = jnp.int32(0)
        seg_across = jnp.zeros((8, rows), jnp.int32)
        seg_down = jnp.zeros((rows, 128), jnp.int32)
        for k in range(count):
            reach = reach + lengths_ref[base_ref[0] + slot, k]
            seg_across += (across >= reach).astype(jnp.int32)
            seg_down += (down >= reach).astype(jnp.int32)
        inside = seg_down[:, 0:1] == seg_across[0:1, :]
        bias_ref[slot] = jnp.where(inside, 0.0, -1e30)


def mask_bias(lengths, base, slots, slot_rows):
    smem = pl.BlockSpec(memory_space=pltpu.SMEM)
    return pl.pallas_call(
        mask_kernel,
        in_specs=[smem, smem],
        out_shape=jax.ShapeDtypeStruct((slots, slot_rows, slot_rows), WIDE),
        compiler_params=params(),
        name="mask_bias",
    )(base, lengths)


def qkv_grads(x, o, dq, dk, dv, da, core, dp_count):
    rows, depth = x.shape
    part = depth // 4
    chunk = depth // dp_count

    def kernel(core_ref, x_ref, o_ref, dq_ref, dk_ref, dv_ref, da_ref, *refs):
        outs, (xt_ref, ot_ref) = refs[:4], refs[4:]
        step = pl.program_id(0)

        @pl.when(step == 0)
        def _():
            xt_ref[...] = x_ref[...].T
            ot_ref[...] = o_ref[...].T

        flip = jnp.where(step < 2, 1 - core_ref[0], core_ref[0])
        wanted = 2 * (step % 2) + flip
        for head in range(4):

            @pl.when(wanted == head)
            def _():
                at = slice(head * part, (head + 1) * part)
                joined = jnp.concatenate([dq_ref[:, at], dk_ref[:, at], dv_ref[:, at]], axis=1)
                first = dot_nn(xt_ref[...], joined)
                second = dot_nn(ot_ref[...], da_ref[:, at])
                made = jnp.concatenate([first, second], axis=1).astype(LOW)
                for where_to, chosen in ((outs[0], step < 2), (outs[1], step >= 2)):

                    @pl.when(chosen)
                    def _():
                        put_chunks(where_to, made[:, : 2 * part], dp_count)

                for where_to, chosen in ((outs[2], step < 2), (outs[3], step >= 2)):

                    @pl.when(chosen)
                    def _():
                        put_chunks(where_to, made[:, 2 * part :], dp_count)

    made = jax.ShapeDtypeStruct((2, 2, dp_count // 2, chunk, 2 * part), LOW)
    specs = [
        chunk_spec(dp_count, chunk, 2 * part, dp_first, at)
        for dp_first in (False, True)
        for at in (first_two, last_two)
    ]
    return pl.pallas_call(
        kernel,
        grid_spec=pltpu.PrefetchScalarGridSpec(
            num_scalar_prefetch=1,
            grid=(4,),
            in_specs=[whole(v) for v in (x, o, dq, dk, dv, da)],
            out_specs=specs,
            scratch_shapes=[pltpu.VMEM((depth, rows), LOW)] * 2,
        ),
        out_shape=[made] * 4,
        compiler_params=params(),
        name="qkv_grads",
    )(core, x, o, dq, dk, dv, da)


def input_grad_kernel(du_ref, dq_ref, dk_ref, dv_ref, w_ref, out_ref):
    total = du_ref[...]
    for which, part in enumerate((dq_ref, dk_ref, dv_ref)):
        total = total + dot_nt(part[...], w_ref[which])
    out_ref[...] = total.astype(out_ref.dtype)


def input_grad(du, dq, dk, dv, w, out_type, tile=256):
    rows, width = du.shape
    return pl.pallas_call(
        input_grad_kernel,
        grid=(rows // tile,),
        in_specs=[rows_spec(tile, width)] * 4 + [whole(w)],
        out_specs=rows_spec(tile, width),
        out_shape=jax.ShapeDtypeStruct((rows, width), out_type),
        compiler_params=params(),
        name="input_grad",
    )(du, dq, dk, dv, w)


def bits_of(axis):
    size = lax.axis_size(axis)
    return [1 << bit for bit in range(size.bit_length() - 1)]


def swap(value, axis, bit):
    size = lax.axis_size(axis)
    return lax.ppermute(value, axis, [(i, i ^ bit) for i in range(size)])


def my_bit(axis, bit):
    return (lax.axis_index(axis) // bit) % 2


def gather_over(value, axis):
    blocks = [value]
    for bit in bits_of(axis):
        blocks = blocks + [swap(block, axis, bit) for block in blocks]
    mine = lax.axis_index(axis)
    stacked = jnp.stack(blocks)
    return [
        lax.dynamic_index_in_dim(stacked, block ^ mine, 0, keepdims=False)
        for block in range(len(blocks))
    ]


def sum_everywhere(value, axes):
    for axis in axes:
        for bit in bits_of(axis):
            value = value + swap(value, axis, bit)
    return value


class Summing:
    def __init__(self, sends, keeps):
        head, dp = bits_of("head"), bits_of("dp")
        self.first = ("head", head[0])
        self.stages = [
            (("head", head[1]), ("dp", dp[0])),
            (("dp", dp[0]), ("head", head[1])),
        ] + [(("dp", bit),) * 2 for bit in dp[1:]]
        self.at = 0
        self.merged = False
        self.kept = list(keeps)
        self.got = [swap(send, *self.first) for send in sends]

    def pairs(self):
        kept, got = self.kept, self.got
        if self.merged:
            kept, got = [kept[0][0], kept[0][1]], [got[0][0], got[0][1]]
        return [
            (k.reshape(-1, *k.shape[-2:]), g.reshape(-1, *g.shape[-2:])) for k, g in zip(kept, got)
        ]

    def step(self, after):
        stage = self.stages[self.at]
        merge = self.at >= 2
        bits = jnp.stack([my_bit(*one) for one in stage]).astype(jnp.int32)
        pairs, _ = lax.optimization_barrier((self.pairs(), after))
        outs = add_split(pairs, bits, merged=merge)
        if merge:
            self.got, self.kept = [swap(outs[0], *stage[0])], [outs[1]]
        else:
            self.got = [swap(outs[0], *stage[0]), swap(outs[2], *stage[1])]
            self.kept = [outs[1], outs[3]]
        self.merged = merge
        self.at += 1
        return outs[-1]

    def finish(self):
        while self.at < len(self.stages):
            self.step(self.kept[0])
        return (self.kept[0].astype(WIDE) + self.got[0].astype(WIDE))[:, 0]


def ordered(after, *values):
    values, _ = lax.optimization_barrier((values, after))
    return values


def on_device(
    tokens,
    seq_lengths,
    qkv_weight,
    qv_bias,
    out_weight,
    out_bias,
    norm1_gain,
    norm1_shift,
    up_weight,
    up_bias,
    down_weight,
    down_bias,
    norm2_gain,
    norm2_shift,
    out_grad,
):
    head_count = lax.axis_size("head")
    dp_count = lax.axis_size("dp")
    head_index = lax.axis_index("head")
    local_rows, width = tokens.shape
    slot_rows = local_rows * head_count // seq_lengths.shape[0]
    slots = local_rows // slot_rows
    layers = qkv_weight.shape[0]
    hidden = up_weight.shape[2]
    first_bias = jnp.concatenate(gather_over(qv_bias, "head"), axis=2)
    full_qkv = [jnp.concatenate(gather_over(qkv_weight[0], "head"), axis=2)]
    for layer in range(1, layers):
        full_qkv.append(lax.all_gather(qkv_weight[layer], "head", axis=2, tiled=True))
    base = (head_index * slots).astype(jnp.int32).reshape(1)
    bias = mask_bias(seq_lengths, base, slots, slot_rows)
    rounded, residual = tokens, tokens
    kept = []
    for layer in range(layers):
        q, k, v, probs, context = attention_forward(
            rounded, full_qkv[layer], first_bias[layer][:, None], bias
        )
        small = jnp.stack(
            [
                out_bias[layer],
                norm1_gain[layer],
                norm1_shift[layer],
                down_bias[layer],
                norm2_gain[layer],
                norm2_shift[layer],
            ]
        )
        last = layer == layers - 1
        u1, hr, gr, slope, u2, *made = ffn_forward(
            context,
            residual,
            out_weight[layer],
            up_weight[layer],
            down_weight[layer],
            up_bias[layer][None],
            small,
            (LOW,) if last else (LOW, WIDE),
            chunk=width,
        )
        kept.append((rounded, q, k, v, probs, context, u1, hr, gr, slope, u2))
        rounded, residual = made[0], made[-1]
    out_state = rounded
    grad_state = out_grad
    core = my_bit("head", bits_of("head")[0]).astype(jnp.int32).reshape(1)
    small_sums = [None] * layers
    hidden_sums = [None] * layers
    ffn_groups, wide_groups = [None] * layers, [None] * layers
    running = []

    def advance(after):
        for group in running:
            if group.at < len(group.stages):
                after = group.step(after)
        return after

    for layer in reversed(range(layers)):
        rounded, q, k, v, probs, context, u1, hr, gr, slope, u2 = kept[layer]
        gains = jnp.stack([norm1_gain[layer], norm2_gain[layer]])
        df, dz, da, do, du, sums, hidden_sums[layer] = ffn_backward(
            grad_state,
            u2,
            u1,
            slope,
            down_weight[layer],
            up_weight[layer],
            out_weight[layer],
            gains,
            chunk=width,
        )
        token = advance(do)
        (dz, hr) = ordered(token, dz, hr)
        up_send, up_keep = weight_grad(hr, dz, core, dp_count, True)
        (df, gr) = ordered(up_keep, df, gr)
        down_send, down_keep = weight_grad(df, gr, core, dp_count, False)
        ffn_groups[layer] = Summing((down_send, up_send), (down_keep, up_keep))
        token = advance(down_keep)
        (do, q) = ordered(token, do, q)
        dq, dk, dv, qv_sums = attention_backward(q, k, v, do, probs)
        running.append(ffn_groups[layer])
        token = advance(dv)
        (dq, rounded) = ordered(token, dq, rounded)
        a_send, a_keep, b_send, b_keep = qkv_grads(rounded, context, dq, dk, dv, da, core, dp_count)
        wide_groups[layer] = Summing((a_send, b_send), (a_keep, b_keep))
        (dq, du) = ordered(b_keep, dq, du)
        grad_state = input_grad(du, dq, dk, dv, full_qkv[layer], WIDE if layer else LOW)
        running.append(wide_groups[layer])
        token = advance(grad_state)
        if layer:
            (grad_state,) = ordered(token, grad_state)
        small_sums[layer] = jnp.concatenate([sums[:6], qv_sums[:2]])
    small_sum, hidden_sum = (
        sum_everywhere(jnp.stack(part), ("head", "dp")) for part in (small_sums, hidden_sums)
    )
    while any(group.at < len(group.stages) for group in running):
        token = advance(token)
    ffn_sums = [group.finish() for group in ffn_groups]
    wide_sums = [group.finish() for group in wide_groups]
    part = width // head_count
    wide = [
        [both[half, :, at * part : (at + 1) * part] for half in range(2) for at in range(2)]
        for both in wide_sums
    ]
    return (
        out_state,
        grad_state,
        jnp.stack([jnp.stack(w[:3]) for w in wide]),
        small_sum[:, 6:8],
        jnp.stack([w[3] for w in wide]),
        small_sum[:, 5],
        small_sum[:, 3],
        small_sum[:, 4],
        jnp.stack([both[1] for both in ffn_sums]),
        hidden_sum[:, 0],
        jnp.stack([both[0].T for both in ffn_sums]),
        small_sum[:, 2],
        small_sum[:, 0],
        small_sum[:, 1],
    )


def solution(mesh):
    in_specs = (
        P(("dp", "head"), None),
        P("dp", None),
        P(None, None, None, "head"),
        P(None, None, "head"),
        P(),
        P(),
        P(),
        P(),
        P(),
        P(),
        P(),
        P(),
        P(),
        P(),
        P(("dp", "head"), None),
    )
    out_specs = (
        P(("dp", "head"), None),
        P(("dp", "head"), None),
        P(None, None, "dp", "head"),
        P(),
        P(None, "dp", "head"),
        P(),
        P(),
        P(),
        P(None, "dp", "head"),
        P(),
        P(None, "head", "dp"),
        P(),
        P(),
        P(),
    )
    return jax.shard_map(
        on_device, mesh=mesh, in_specs=in_specs, out_specs=out_specs, check_vma=False
    )
```

```python
import functools
import math

import jax
import jax.numpy as jnp
from jax import lax
from jax.experimental import pallas as pl
from jax.experimental.pallas import tpu as pltpu
from jax.sharding import PartitionSpec as P

HD = 64
EPSILON = 1e-06
LOW = jnp.bfloat16
WIDE = jnp.float32
VMEM_BYTES = 58 << 20
ROOT_HALF = 0.7071067811865476
INV_ROOT_TAU = 0.3989422804014327
FAR = -1e30


def row_stats(values):
    centre = jnp.mean(values, axis=-1, keepdims=True)
    centred = values - centre
    spread = jnp.mean(centred * centred, axis=-1, keepdims=True)
    inverse = lax.rsqrt(spread + EPSILON)
    return centred * inverse, inverse


def norm_backward(upstream, xhat, inverse, gain):
    scaled = upstream * gain
    first = jnp.mean(scaled, axis=-1, keepdims=True)
    second = jnp.mean(scaled * xhat, axis=-1, keepdims=True)
    return (scaled - first - xhat * second) * inverse


def column_sum(values):
    return jnp.sum(values, axis=0, keepdims=True)


def dot_nn(left, right):
    return jnp.dot(left, right, preferred_element_type=WIDE)


def dot_nt(left, right):
    return lax.dot_general(left, right, (((1,), (1,)), ((), ())), preferred_element_type=WIDE)


def dot_tn(left, right):
    return lax.dot_general(left, right, (((0,), (0,)), ((), ())), preferred_element_type=WIDE)


def gelu_pair(z):
    cdf = 0.5 + 0.5 * lax.erf(z * ROOT_HALF)
    return z * cdf, cdf + z * (jnp.exp(z * z * -0.5) * INV_ROOT_TAU)


def pick(mask, values):
    return jnp.where(mask, values, jnp.zeros_like(values))


def head_masks(width):
    lanes = lax.broadcasted_iota(jnp.int32, (1, width), 1) // HD
    return [lanes == head for head in range(width // HD)]


def params():
    return pltpu.CompilerParams(vmem_limit_bytes=VMEM_BYTES)


def whole(array):
    return pl.BlockSpec(array.shape, lambda *ids: (0,) * array.ndim, pipeline_mode=pl.Buffered(1))


def in_place():
    return pl.BlockSpec(memory_space=pl.ANY)


def in_hbm():
    return pl.BlockSpec(memory_space=pltpu.HBM)


def shape_of(shape, kind):
    return jax.ShapeDtypeStruct(shape, kind)


def cost(flops, out_shape, operands):
    made = out_shape if isinstance(out_shape, (list, tuple)) else [out_shape]
    moved = sum(math.prod(v.shape) * jnp.dtype(v.dtype).itemsize for v in [*made, *operands])
    return pl.CostEstimate(flops=flops, bytes_accessed=moved, transcendentals=0)


def stored(shape, kind):
    return pltpu.HBM(shape, kind)


def call(kernel, name, grid, in_specs, out_specs, out_shape, scratch, scalars, operands, alias=None, flops=0):
    return pl.pallas_call(
        kernel,
        grid_spec=pltpu.PrefetchScalarGridSpec(
            num_scalar_prefetch=len(scalars),
            grid=grid,
            in_specs=in_specs,
            out_specs=out_specs,
            scratch_shapes=scratch,
        ),
        out_shape=out_shape,
        compiler_params=params(),
        input_output_aliases=alias or {},
        cost_estimate=cost(flops, out_shape, operands),
        name=name,
    )(*scalars, *operands)


def mask_kernel(base_ref, lengths_ref, bias_ref):
    slots, rows, _ = bias_ref.shape
    across = lax.broadcasted_iota(jnp.int32, (8, rows), 1)
    down = lax.broadcasted_iota(jnp.int32, (rows, 128), 0)
    for slot in range(slots):
        reach = jnp.int32(0)
        seg_across = jnp.zeros((8, rows), jnp.int32)
        seg_down = jnp.zeros((rows, 128), jnp.int32)
        for k in range(lengths_ref.shape[1]):
            reach = reach + lengths_ref[base_ref[0] + slot, k]
            seg_across += (across >= reach).astype(jnp.int32)
            seg_down += (down >= reach).astype(jnp.int32)
        inside = seg_down[:, 0:1] == seg_across[0:1, :]
        bias_ref[slot] = jnp.where(inside, 0.0, FAR)


def mask_bias(lengths, base, slots, slot_rows):
    smem = pl.BlockSpec(memory_space=pltpu.SMEM)
    return pl.pallas_call(
        mask_kernel,
        in_specs=[smem, smem],
        out_shape=shape_of((slots, slot_rows, slot_rows), WIDE),
        compiler_params=params(),
        name="mask_bias",
    )(base, lengths)


def attention_forward_kernel(
    x_ref, wa_ref, wb_ref, b_ref, bias_ref, *refs, aliased, tile
):
    mixed_ref, p_ref, s_ref = refs[2 * aliased :]
    rows, part = x_ref.shape[0], wa_ref.shape[0] // 3
    x = x_ref[...]
    masks = head_masks(part)

    def work(w_ref):
        q = ((dot_nt(x, w_ref[:part]) + b_ref[0]).astype(LOW) * HD**-0.5).astype(LOW)
        k = dot_nt(x, w_ref[part : 2 * part]).astype(LOW)
        v = (dot_nt(x, w_ref[2 * part :]) + b_ref[1]).astype(LOW)
        mixed_ref[0] = q
        mixed_ref[1] = k
        mixed_ref[2] = v
        total = None
        for head, mask in enumerate(masks):
            s_ref[head] = dot_nt(pick(mask, q), k)
            for start in range(0, rows, tile):
                at = slice(start, start + tile)
                s = s_ref[head, at] + bias_ref[at]
                e = jnp.exp(s - jnp.max(s, axis=1, keepdims=True))
                p_ref[head, at] = (e * (1.0 / jnp.sum(e, axis=1, keepdims=True))).astype(LOW)
            made = dot_nn(p_ref[head], pick(mask, v))
            total = made if total is None else total + made
        mixed_ref[3] = total.astype(LOW)

    for block, w_ref in enumerate((wa_ref, wb_ref)):

        @pl.when(pl.program_id(1) == block)
        def _():
            work(w_ref)


def attention_forward(x, wa, wb, qv_bias, bias, first, before, tile=64):
    rows, width = x.shape
    slots, slot_rows, _ = bias.shape
    part = wa.shape[0] // 3
    heads = part // HD
    aliased = int(before is not None)
    mixed = shape_of((4, 4, rows, part), LOW)
    probs = shape_of((4, slots, heads, slot_rows, slot_rows), LOW)
    return call(
        functools.partial(attention_forward_kernel, aliased=aliased, tile=tile),
        "attention_forward",
        (slots, 2),
        [
            pl.BlockSpec((slot_rows, width), lambda s, b: (s, 0)),
            whole(wa),
            whole(wb),
            pl.BlockSpec((None, 2, 1, part), lambda s, b: (b, 0, 0, 0)),
            pl.BlockSpec((None, slot_rows, slot_rows), lambda s, b: (s, 0, 0)),
        ]
        + [in_place(), in_place()] * aliased,
        [
            pl.BlockSpec((None, 4, slot_rows, part), lambda s, b: (first + b, 0, s, 0)),
            pl.BlockSpec(
                (None, None, heads, slot_rows, slot_rows), lambda s, b: (first + b, s, 0, 0, 0)
            ),
        ],
        [mixed, probs],
        [pltpu.VMEM((heads, slot_rows, slot_rows), WIDE)],
        [],
        [x, wa, wb, qv_bias, bias, *(before or ())],
        alias={5: 0, 6: 1} if aliased else None,
        flops=12 * rows * width * part + 16 * heads * rows * slot_rows * 256,
    )


def row_tiles(rows, tile):
    return [pl.ds(start, tile) for start in range(0, rows, tile)]


def ffn_forward_kernel(own_ref, mixed_hbm, x_hbm, wo_hbm, wu_ref, wd_ref, bu_ref, small_ref,
                       u1_hbm, hr_hbm, gr_hbm, gp_hbm, u2_hbm, low_hbm,
                       o_ref, x_ref, wo_ref, u1_ref, hr_ref, gr_ref, gp_ref, u2_ref, low_ref, in_sems, out_sems, g_sems,
                       *, layer, tile, renorm):
    step, steps = pl.program_id(0), pl.num_programs(0)
    part = o_ref.shape[2]
    tiles = row_tiles(x_ref.shape[0], tile)
    wo_copy = pltpu.make_async_copy(wo_hbm.at[layer], wo_ref, in_sems.at[0, 0])
    loads, first_out, last_out = [], [], []
    for t, at in enumerate(tiles):
        loads.append(
            [
                pltpu.make_async_copy(mixed_hbm.at[:, 3, at], o_ref.at[:, at], in_sems.at[1, t]),
                pltpu.make_async_copy(x_hbm.at[at], x_ref.at[at], in_sems.at[2, t]),
            ]
        )
        first_out.append(
            [
                pltpu.make_async_copy(u1_ref.at[at], u1_hbm.at[at], out_sems.at[0, t]),
                pltpu.make_async_copy(hr_ref.at[at], hr_hbm.at[at], out_sems.at[1, t]),
            ]
        )
        last_out.append(
            [
                pltpu.make_async_copy(u2_ref.at[at], u2_hbm.at[at], out_sems.at[2, t]),
                pltpu.make_async_copy(low_ref.at[at], low_hbm.at[at], out_sems.at[3, t]),
            ]
        )

    def g_out(chunk, slot):
        return [
            pltpu.make_async_copy(gr_ref.at[slot], gr_hbm.at[chunk], g_sems.at[0, slot]),
            pltpu.make_async_copy(gp_ref.at[slot], gp_hbm.at[chunk], g_sems.at[1, slot]),
        ]

    @pl.when(step == 0)
    def _():
        wo_copy.start()
        for pair in loads:
            for copy in pair:
                copy.start()
        wo_copy.wait()
        for t, at in enumerate(tiles):
            for copy in loads[t]:
                copy.wait()
            residual = x_ref[at].astype(WIDE)
            if renorm:
                residual = row_stats(residual)[0] * small_ref[6:7] + small_ref[7:8]
            u1 = residual + small_ref[0:1]
            for block in range(4):
                rows = pl.ds(pl.multiple_of((own_ref[0] ^ block) * part, 16), part)
                u1 = u1 + dot_nn(o_ref[block, at], wo_ref[rows, :])
            u1_ref[at] = u1
            normed = row_stats(u1)[0] * small_ref[1:2] + small_ref[2:3]
            hr_ref[at] = normed.astype(LOW)
            u2_ref[at] = normed + small_ref[3:4]
            for copy in first_out[t]:
                copy.start()

    slot = step % 2

    @pl.when(step >= 2)
    def _():
        for copy in g_out(step - 2, slot):
            copy.wait()

    z = dot_nn(hr_ref[...], wu_ref[...]) + bu_ref[...]
    g, slope = gelu_pair(z)
    gr = g.astype(LOW)
    gr_ref[slot] = gr
    gp_ref[slot] = slope.astype(LOW)
    for copy in g_out(step, slot):
        copy.start()
    u2_ref[...] += dot_nn(gr, wd_ref[...])

    @pl.when(step == steps - 1)
    def _():
        for t, at in enumerate(tiles):
            total = u2_ref[at]
            low_ref[at] = (row_stats(total)[0] * small_ref[4:5] + small_ref[5:6]).astype(LOW)
            for copy in last_out[t]:
                copy.start()
        for copy in [*g_out(step - 1, 1 - slot), *g_out(step, slot)]:
            copy.wait()
        for pair in first_out + last_out:
            for copy in pair:
                copy.wait()


def ffn_forward(own, mixed, x, wo, wu, wd, bu, small, layer, renorm, tile=512):
    _, _, rows, part = mixed.shape
    width, hidden = wu.shape[1:]
    chunks = hidden // width
    fixed = lambda v: pl.BlockSpec(v.shape, lambda i, o: (0,) * v.ndim)
    sems = lambda *shape: pltpu.SemaphoreType.DMA(shape)
    return call(
        functools.partial(ffn_forward_kernel, layer=layer, tile=tile, renorm=renorm),
        "ffn_forward",
        (chunks,),
        [
            in_place(),
            in_place(),
            in_place(),
            pl.BlockSpec((None, width, width), lambda i, o: (layer, 0, i)),
            pl.BlockSpec((None, width, width), lambda i, o: (layer, i, 0)),
            pl.BlockSpec((None, 1, width), lambda i, o: (i, 0, 0)),
            fixed(small),
        ],
        [in_place()] * 6,
        [
            shape_of((rows, width), WIDE),
            shape_of((rows, width), LOW),
            shape_of((chunks, rows, width), LOW),
            shape_of((chunks, rows, width), LOW),
            shape_of((rows, width), WIDE),
            shape_of((rows, width), LOW),
        ],
        [
            pltpu.VMEM((4, rows, part), LOW),
            pltpu.VMEM((rows, width), x.dtype),
            pltpu.VMEM((width, width), LOW),
            pltpu.VMEM((rows, width), WIDE),
            pltpu.VMEM((rows, width), LOW),
            pltpu.VMEM((2, rows, width), LOW),
            pltpu.VMEM((2, rows, width), LOW),
            pltpu.VMEM((rows, width), WIDE),
            pltpu.VMEM((rows, width), LOW),
            sems(3, rows // tile),
            sems(4, rows // tile),
            sems(2, 2),
        ],
        [own],
        [mixed, x, wo, wu, wd, bu, small],
        flops=6 * rows * width * (width + 2 * hidden),
    )


def reversed_bits(value, count):
    made = 0
    for bit in range(count):
        made = made | (((value >> bit) & 1) << (count - 1 - bit))
    return made


def each_chunk(made, dp_count):
    rows = made.shape[0] // dp_count
    for dp in range(dp_count):
        yield dp, made[dp * rows : (dp + 1) * rows]


def place(dp, own_dp, dp_count):
    away = dp ^ own_dp
    return away & 1, reversed_bits(away >> 1, dp_count.bit_length() - 2)


def ffn_backward_kernel(own_ref, gx_hbm, u2_hbm, u1_hbm, gp_hbm, hr_hbm, gr_hbm, wo_hbm, wu_ref, wd_ref, gain_ref,
                        da_hbm, do_hbm, du_hbm, sums_ref, zsum_ref, send_ref, keep_ref,
                        gx_ref, u2_ref, u1_ref, gp_ref, hr_ref, gr_ref, wo_ref, acc_ref, df_ref, dz_ref, da_ref, do_ref,
                        in_sems, out_sems, g_sems, *, layer, tile, dp_count):
    step, steps = pl.program_id(0), pl.num_programs(0)
    own, own_dp = own_ref[0], own_ref[1]
    part = do_ref.shape[2]
    tiles = row_tiles(gx_ref.shape[0], tile)
    count = len(tiles)
    loads, last_out = [], []
    for t, at in enumerate(tiles):
        loads.append(
            [
                pltpu.make_async_copy(gx_hbm.at[at], gx_ref.at[at], in_sems.at[0, t]),
                pltpu.make_async_copy(u2_hbm.at[at], u2_ref.at[at], in_sems.at[1, t]),
            ]
        )
        last_out.append(
            [
                pltpu.make_async_copy(u2_ref.at[at], du_hbm.at[at], out_sems.at[0, t]),
                pltpu.make_async_copy(da_ref.at[:, at], da_hbm.at[:, at], out_sems.at[1, t]),
                pltpu.make_async_copy(do_ref.at[:, at], do_hbm.at[:, at], out_sems.at[2, t]),
            ]
        )
    hr_copy = pltpu.make_async_copy(hr_hbm, hr_ref, in_sems.at[2, 0])
    u1_copy = pltpu.make_async_copy(u1_hbm, u1_ref, in_sems.at[2, 1])
    wo_copy = pltpu.make_async_copy(wo_hbm.at[layer], wo_ref, in_sems.at[2, 2])

    def streams(at_step):
        slot, head = at_step % 2, own ^ head_order(at_step)
        return (
            pltpu.make_async_copy(gp_hbm.at[head], gp_ref.at[slot], g_sems.at[0, slot]),
            pltpu.make_async_copy(gr_hbm.at[head], gr_ref.at[slot], g_sems.at[1, slot]),
        )

    slot = step % 2
    gp_copy, gr_copy = streams(step)

    @pl.when(step == 0)
    def _():
        for pair in loads:
            for copy in pair:
                copy.start()

        gp_copy.start()
        hr_copy.start()
        gr_copy.start()

    @pl.when(step < steps - 1)
    def _():
        for copy in streams(step + 1):
            copy.start()

    @pl.when(step == 1)
    def _():
        u1_copy.start()
        wo_copy.start()

    @pl.when(step == 0)
    def _():
        sums_ref[...] = jnp.zeros_like(sums_ref)
        for t, at in enumerate(tiles):
            for copy in loads[t]:
                copy.wait()
            gx = gx_ref[at].astype(WIDE)
            xhat, inverse = row_stats(u2_ref[at])
            sums_ref[0:1] += column_sum(gx * xhat)
            sums_ref[1:2] += column_sum(gx)
            gv = norm_backward(gx, xhat, inverse, gain_ref[1:2])
            df = gv.astype(LOW)
            df_ref[at] = df
            sums_ref[2:3] += column_sum(df.astype(WIDE))
            acc_ref[at] = gv

    dg = dot_nt(df_ref[...], wd_ref[...])
    gp_copy.wait()
    dz = (dg * gp_ref[slot].astype(WIDE)).astype(LOW)
    dz_ref[...] = dz
    zsum_ref[...] = column_sum(dz.astype(WIDE))
    acc_ref[...] += dot_nt(dz_ref[...], wu_ref[...])

    @pl.when(step == 0)
    def _():
        hr_copy.wait()

    up = dot_tn(hr_ref[...], dz_ref[...]).astype(LOW)
    gr_copy.wait()
    down = dot_tn(df_ref[...], gr_ref[slot]).astype(LOW)
    for out, wanted in ((send_ref, step < 2), (keep_ref, step >= 2)):

        @pl.when(wanted)
        def _():
            for which, made in enumerate((up, down)):
                for dp, chunk in each_chunk(made, dp_count):
                    out[(which, *place(dp, own_dp, dp_count))] = chunk

    @pl.when(step == steps - 1)
    def _():
        u1_copy.wait()
        wo_copy.wait()
        for t, at in enumerate(tiles):
            total = acc_ref[at]
            xhat, inverse = row_stats(u1_ref[at])
            sums_ref[3:4] += column_sum(total * xhat)
            sums_ref[4:5] += column_sum(total)
            du = norm_backward(total, xhat, inverse, gain_ref[0:1])
            u2_ref[at] = du
            da = du.astype(LOW)
            for block in range(4):
                da_ref[block, at] = da[:, block * part : (block + 1) * part]
            sums_ref[5:6] += column_sum(da.astype(WIDE))
            for block in range(4):
                rows = pl.ds(pl.multiple_of((own ^ block) * part, 16), part)
                do_ref[block, at] = dot_nt(da, wo_ref[rows, :]).astype(LOW)
            for copy in last_out[t]:
                copy.start()
        for several in last_out:
            for copy in several:
                copy.wait()


def head_order(step):
    return jnp.where(step < 2, 1 + 2 * step, 2 * (step - 2))


def ffn_backward(own, gx, u2, u1, gp, hr, gr, wo, wu, wd, gains, layer, dp_count, tile=512):
    rows, width = gx.shape
    chunks = gp.shape[0]
    part = width // 4
    chunk_rows = width // dp_count
    rest = dp_count // 2
    fixed = lambda s: pl.BlockSpec(s.shape, lambda i, o: (0,) * len(s.shape))
    head = lambda i, o: o[0] ^ head_order(i)
    block = (2, None, 2, rest, chunk_rows, width)
    sums = shape_of((8, width), WIDE)
    grads = stored((2, 2, 2, rest, chunk_rows, width), LOW)
    sems = lambda *shape: pltpu.SemaphoreType.DMA(shape)
    low = lambda *shape: pltpu.VMEM(shape, LOW)
    wide = lambda *shape: pltpu.VMEM(shape, WIDE)
    return call(
        functools.partial(ffn_backward_kernel, layer=layer, tile=tile, dp_count=dp_count),
        "ffn_backward",
        (chunks,),
        [in_place()] * 7
        + [
            pl.BlockSpec((None, width, width), lambda i, o: (layer, 0, head(i, o))),
            pl.BlockSpec((None, width, width), lambda i, o: (layer, head(i, o), 0)),
            fixed(gains),
        ],
        [
            in_place(),
            in_place(),
            in_place(),
            fixed(sums),
            pl.BlockSpec((None, 1, width), lambda i, o: (head(i, o), 0, 0)),
            pl.BlockSpec(block, lambda i, o: (0, jnp.minimum(i, 1), 0, 0, 0, 0)),
            pl.BlockSpec(block, lambda i, o: (0, jnp.maximum(i - 2, 0), 0, 0, 0, 0)),
        ],
        [
            shape_of((4, rows, part), LOW),
            shape_of((4, rows, part), LOW),
            shape_of((rows, width), WIDE),
            sums,
            shape_of((chunks, 1, width), WIDE),
            grads,
            grads,
        ],
        [
            pltpu.VMEM((rows, width), gx.dtype),
            wide(rows, width),
            wide(rows, width),
            low(2, rows, width),
            low(rows, width),
            low(2, rows, width),
            low(width, width),
            wide(rows, width),
            low(rows, width),
            low(rows, width),
            low(4, rows, part),
            low(4, rows, part),
            sems(3, max(rows // tile, 3)),
            sems(3, rows // tile),
            sems(2, 2),
        ],
        [own],
        [gx, u2, u1, gp, hr, gr, wo, wu, wd, gains],
        flops=4 * rows * width * (width + 4 * chunks * width),
    )


def split_rows(made, got_ref, own_dp, dp_count, send_ref, keep_ref):
    for dp, chunk in each_chunk(made, dp_count):
        away, rest = place(dp, own_dp, dp_count)
        summed = (chunk + got_ref[away, rest].astype(WIDE)).astype(LOW)

        @pl.when(away == 1)
        def _():
            send_ref[rest] = summed

        @pl.when(away == 0)
        def _():
            keep_ref[rest] = summed


def add_rows(made, got_ref, own_dp, dp_count, out_ref):
    for dp, chunk in each_chunk(made, dp_count):
        at = place(dp, own_dp, dp_count)
        out_ref[at] = (chunk + got_ref[at].astype(WIDE)).astype(LOW)


def core_add_kernel(kept_ref, got_ref, up_send, up_keep, down_send, down_keep):
    step = pl.program_id(0)

    def summed(at):
        return (kept_ref[at].astype(WIDE) + got_ref[at].astype(WIDE)).astype(LOW)

    @pl.when(step < 2)
    def _():
        up_keep[...] = summed(0)
        up_send[...] = summed(1)

    for out, wanted in ((down_send, 2), (down_keep, 3)):

        @pl.when(step == wanted)
        def _():
            out[0] = summed(0)
            out[1] = summed(1)


def core_add(kept, got):
    _, _, _, rest, chunk_rows, width = kept.shape

    def at(i):
        return (i // 2, jnp.where(i < 2, i, 3 - i), 0, 0, 0, 0)

    block = pl.BlockSpec((None, None, 2, rest, chunk_rows, width), at)
    up = pl.BlockSpec((None, rest, chunk_rows, width), lambda i: (jnp.minimum(i, 1), 0, 0, 0))
    down = pl.BlockSpec((2, rest, chunk_rows, width), lambda i: (0, 0, 0, 0))
    made = stored((2, rest, chunk_rows, width), LOW)
    return call(
        core_add_kernel, "core_add", (4,), [block, block], [up, up, down, down], [made] * 4, [], [], [kept, got]
    )


def attention_backward_kernel(own_ref, mixed_ref, do_ref, p_ref, x_ref, o_ref, da_ref, wa_ref, wb_ref, gx_ref, *refs,
                              dp_count, tile, keep):
    if keep:
        got_ref, *refs = refs
    out_ref, sums_ref, *refs = refs
    grads = refs[: 4 if keep else 1]
    t_ref, ds_ref, parts_ref, xt_ref, ot_ref, acc_ref = refs[4 if keep else 1 :]
    slot, block = pl.program_id(0), pl.program_id(1)
    last = pl.num_programs(0) - 1
    own, own_dp = own_ref[0], own_ref[1]
    rows, part = mixed_ref.shape[1:]

    @pl.when((slot == 0) & (block == 0))
    def _():
        xt_ref[...] = x_ref[...].T
        for r in range(4):
            ot_ref[pl.ds(pl.multiple_of((own ^ r) * part, 16), part), :] = o_ref[r].T
        sums_ref[...] = jnp.zeros_like(sums_ref)

    dq = dk = dv = None
    for head, mask in enumerate(head_masks(part)):
        do = pick(mask, do_ref[...])
        t_ref[head] = dot_nt(do, mixed_ref[2])
        for start in range(0, rows, tile):
            at = slice(start, start + tile)
            p = p_ref[head, at].astype(WIDE)
            dp = t_ref[head, at]
            share = jnp.sum(p * dp, axis=1, keepdims=True)
            ds_ref[head, at] = (p * (dp - share)).astype(LOW)
        made = (
            dot_nn(ds_ref[head], pick(mask, mixed_ref[1])),
            dot_tn(ds_ref[head], pick(mask, mixed_ref[0])),
            dot_tn(p_ref[head], do),
        )
        dq, dk, dv = made if dq is None else (dq + made[0], dk + made[1], dv + made[2])
    dq = (dq * HD**-0.5).astype(LOW)
    dk = dk.astype(LOW)
    dv = dv.astype(LOW)
    sums_ref[block, 0:1] += column_sum(dq.astype(WIDE))
    sums_ref[block, 1:2] += column_sum(dv.astype(WIDE))
    joined = jnp.concatenate([dq, dk, dv], axis=1)
    parts_ref[block, pl.ds(pl.multiple_of(slot * rows, rows), rows), :] = joined
    weights = jnp.where(block == 0, wa_ref[...], wb_ref[...])
    passed = dot_nn(joined, weights)

    @pl.when(block == 0)
    def _():
        acc_ref[...] = gx_ref[...] + passed

    @pl.when(block == 1)
    def _():
        out_ref[...] = (acc_ref[...] + passed).astype(out_ref.dtype)

    @pl.when(slot == last)
    def _():
        first = dot_nn(xt_ref[...], parts_ref[block])
        second = dot_nn(ot_ref[...], da_ref[...])
        made = jnp.concatenate([first, second], axis=1)
        if not keep:
            for dp, chunk in each_chunk(made.astype(LOW), dp_count):
                grads[0][place(dp, own_dp, dp_count)] = chunk
            return
        half = made.shape[1] // 2
        a_send, a_keep, b_send, b_keep = grads
        got = [got_ref.at[:, :, :, :half], got_ref.at[:, :, :, half:]]
        for where_to, wanted in ((a_keep, 0), (a_send, 1)):

            @pl.when(block == wanted)
            def _():
                add_rows(made[:, :half], got[0], own_dp, dp_count, where_to)

        split_rows(made[:, half:], got[1], own_dp, dp_count, b_send, b_keep)


def attention_backward(own, mixed, do, probs, x, da, wa, wb, gx, got, dp_count, out_type, tile=64):
    rows, width = x.shape
    part = mixed.shape[3]
    _, slots, heads, slot_rows, _ = probs.shape
    chunk_rows, rest = width // dp_count, dp_count // 2
    keep = got is not None
    away = 0 if keep else 1
    block_of = lambda b: 2 * b + away
    row = pl.BlockSpec((slot_rows, width), lambda s, b, o: (s, 0))
    last = slots - 1
    late = lambda s, b: jnp.where(s == last, b, 0)
    in_specs = [
        pl.BlockSpec((None, 3, slot_rows, part), lambda s, b, o: (block_of(b), 0, s, 0)),
        pl.BlockSpec((None, slot_rows, part), lambda s, b, o: (block_of(b), s, 0)),
        pl.BlockSpec(
            (None, None, heads, slot_rows, slot_rows), lambda s, b, o: (block_of(b), s, 0, 0, 0)
        ),
        whole(x),
        pl.BlockSpec((4, None, rows, part), lambda s, b, o: (0, 3, 0, 0), pipeline_mode=pl.Buffered(1)),
        pl.BlockSpec((None, rows, part), lambda s, b, o: (o[0] ^ block_of(late(s, b)), 0, 0)),
        whole(wa),
        whole(wb),
        row,
    ]
    operands = [mixed, do, probs, x, mixed, da, wa, wb, gx]
    sums = shape_of((2, 8, part), WIDE)
    out_specs = [row, pl.BlockSpec(sums.shape, lambda s, b, o: (0, 0, 0))]
    out_shape = [shape_of((rows, width), out_type), sums]
    whole_block = lambda w: pl.BlockSpec((2, rest, chunk_rows, w), lambda s, b, o: (0, 0, 0, 0))
    if keep:
        in_specs.append(
            pl.BlockSpec(
                (None, 2, rest, chunk_rows, width), lambda s, b, o: (late(s, b), 0, 0, 0, 0)
            )
        )
        operands.append(got)
        half = width // 2
        b_block = pl.BlockSpec(
            (None, rest, chunk_rows, half), lambda s, b, o: (late(s, b), 0, 0, 0)
        )
        out_specs += [whole_block(half)] * 2 + [b_block] * 2
        out_shape += [stored((2, rest, chunk_rows, half), LOW)] * 4
    else:
        out_specs.append(
            pl.BlockSpec(
                (None, 2, rest, chunk_rows, width), lambda s, b, o: (late(s, b), 0, 0, 0, 0)
            )
        )
        out_shape.append(stored((2, 2, rest, chunk_rows, width), LOW))
    return call(
        functools.partial(attention_backward_kernel, dp_count=dp_count, tile=tile, keep=keep),
        "attention_backward",
        (slots, 2),
        in_specs,
        out_specs,
        out_shape,
        [
            pltpu.VMEM((heads, slot_rows, slot_rows), WIDE),
            pltpu.VMEM((heads, slot_rows, slot_rows), LOW),
            pltpu.VMEM((2, rows, 3 * part), LOW),
            pltpu.VMEM((width, rows), LOW),
            pltpu.VMEM((width, rows), LOW),
            pltpu.VMEM((slot_rows, width), WIDE),
        ],
        [own],
        operands,
        flops=36 * heads * rows * slot_rows * 256,
    )


def bits_of(axis):
    size = lax.axis_size(axis)
    return [1 << bit for bit in range(size.bit_length() - 1)]


def swap(value, axis, bit):
    size = lax.axis_size(axis)
    return lax.ppermute(value, axis, [(i, i ^ bit) for i in range(size)])


def add_split_kernel(*refs, merge_in, merge_out):
    inputs = 2 if merge_in else 4
    outputs = 2 if merge_out else 4
    ins, outs = refs[:inputs], refs[inputs : inputs + outputs]
    kept_ref, got_ref, send_ref, keep_ref, in_sems, out_sems = refs[inputs + outputs :]
    half = send_ref.shape[1]
    loads, stores = [], []
    for part in range(2):
        kept, got = (ins[0].at[part], ins[1].at[part]) if merge_in else ins[2 * part : 2 * part + 2]
        send, keep = (
            (outs[0].at[part], outs[1].at[part]) if merge_out else outs[2 * part : 2 * part + 2]
        )
        loads.append(
            [
                pltpu.make_async_copy(kept, kept_ref.at[part], in_sems.at[part, 0]),
                pltpu.make_async_copy(got, got_ref.at[part], in_sems.at[part, 1]),
            ]
        )
        stores.append(
            [
                pltpu.make_async_copy(send_ref.at[part], send, out_sems.at[part, 0]),
                pltpu.make_async_copy(keep_ref.at[part], keep, out_sems.at[part, 1]),
            ]
        )
    for copies in loads:
        for copy in copies:
            copy.start()
    for part in range(2):
        for copy in loads[part]:
            copy.wait()
        for out, at in ((send_ref, slice(half, None)), (keep_ref, slice(None, half))):
            out[part] = (kept_ref[part, at].astype(WIDE) + got_ref[part, at].astype(WIDE)).astype(LOW)
        for copy in stores[part]:
            copy.start()
    for copies in stores:
        for copy in copies:
            copy.wait()


def add_split(ins, merge_in, merge_out):
    size, rows, columns = ins[0].shape[-3:]
    half = (size // 2, rows, columns)
    out_shape = [stored((2, *half), LOW)] * 2 if merge_out else [stored(half, LOW)] * 4
    return pl.pallas_call(
        functools.partial(add_split_kernel, merge_in=merge_in, merge_out=merge_out),
        in_specs=[in_hbm()] * len(ins),
        out_specs=[in_hbm()] * len(out_shape),
        out_shape=out_shape,
        scratch_shapes=[
            pltpu.VMEM((2, size, rows, columns), LOW),
            pltpu.VMEM((2, size, rows, columns), LOW),
            pltpu.VMEM((2, *half), LOW),
            pltpu.VMEM((2, *half), LOW),
            pltpu.SemaphoreType.DMA((2, 2)),
            pltpu.SemaphoreType.DMA((2, 2)),
        ],
        compiler_params=params(),
        cost_estimate=cost(0, out_shape, ins),
        name="add_split",
    )(*ins)


class Summing:
    def __init__(self, a_send, a_keep, b_send, b_keep):
        head, dp = bits_of("head"), bits_of("dp")
        self.stages = [(("dp", dp[0]), ("head", head[1]))] + [(("dp", bit),) for bit in dp[1:]]
        self.at = 0
        self.kept = [a_keep, b_keep]
        self.got = [swap(a_send, "head", head[1]), swap(b_send, "dp", dp[0])]

    def busy(self):
        return self.at < len(self.stages)

    def step(self, after):
        stage = self.stages[self.at]
        merge_in, merge_out = len(self.kept) == 1, len(stage) == 1
        ins = [v for pair in zip(self.kept, self.got) for v in pair]
        lead = 1 if merge_in else 0
        ins = [v.reshape(*v.shape[:lead], -1, *v.shape[-2:]) for v in ins]
        ins, _ = lax.optimization_barrier((ins, after))
        outs = add_split(ins, merge_in, merge_out)
        if merge_out:
            self.got, self.kept = [swap(outs[0], *stage[0])], [outs[1]]
        else:
            self.got = [swap(outs[0], *stage[0]), swap(outs[2], *stage[1])]
            self.kept = [outs[1], outs[3]]
        self.at += 1
        return outs[-1]

    def finish(self):
        kept, got = self.kept[0], self.got[0]
        return (kept.astype(WIDE) + got.astype(WIDE)).reshape(2, *kept.shape[-2:])


def ordered(after, *values):
    values, _ = lax.optimization_barrier((values, after))
    return values


def near_blocks(block):
    low, high = bits_of("head")
    return block, swap(block, "head", low), swap(block, "head", high)


def gathered_pairs(block):
    own, near, far = near_blocks(block)
    return jnp.stack([own, near]), jnp.stack([far, swap(far, "head", bits_of("head")[0])])


def on_device(
    tokens,
    seq_lengths,
    qkv_weight,
    qv_bias,
    out_weight,
    out_bias,
    norm1_gain,
    norm1_shift,
    up_weight,
    up_bias,
    down_weight,
    down_bias,
    norm2_gain,
    norm2_shift,
    out_grad,
):
    head_count, dp_count = lax.axis_size("head"), lax.axis_size("dp")
    head_index, dp_index = lax.axis_index("head"), lax.axis_index("dp")
    own = jnp.stack([head_index, dp_index]).astype(jnp.int32)
    local_rows, width = tokens.shape
    slot_rows = local_rows * head_count // seq_lengths.shape[0]
    slots = local_rows // slot_rows
    layers = qkv_weight.shape[0]
    part = width // head_count
    turned = jnp.swapaxes(qkv_weight, 2, 3).reshape(layers, 3 * part, width)
    near_bias, far_bias = gathered_pairs(qv_bias[:, :, None])
    weights = [near_blocks(turned[0])]
    base = (head_index * slots).astype(jnp.int32).reshape(1)
    bias = mask_bias(seq_lengths, base, slots, slot_rows)
    up_rows = up_bias.reshape(layers, -1, 1, width)
    rounded, residual = tokens, tokens
    kept = []
    for layer in range(layers):
        before = max(layer - 1, 0)
        small = jnp.stack(
            [
                out_bias[layer],
                norm1_gain[layer],
                norm1_shift[layer],
                down_bias[layer],
                norm2_gain[layer],
                norm2_shift[layer],
                norm2_gain[before],
                norm2_shift[before],
            ]
        )
        own_w, near_w, far_w = weights[layer]
        near = attention_forward(rounded, own_w, near_w, near_bias[:, layer], bias, 0, None)
        (far_w, far_b) = ordered(near[0], far_w, far_bias[:, layer])
        both_w = swap(far_w, "head", bits_of("head")[0])
        if layer + 1 < layers:
            (later,) = ordered(near[0], turned[layer + 1])
            weights.append(near_blocks(later))
        mixed, probs = attention_forward(rounded, far_w, both_w, far_b, bias, 2, near)
        w = (own_w, near_w, far_w, both_w)
        weights[layer] = w
        u1, hr, gr, slope, u2, low = ffn_forward(
            own,
            mixed,
            residual,
            out_weight,
            up_weight,
            down_weight,
            up_rows[layer],
            small,
            layer,
            layer > 0,
        )
        kept.append((rounded, mixed, probs, u1, hr, gr, slope, u2))
        rounded, residual = low, u2
    out_state = rounded
    grad_state = out_grad
    small_sums = [None] * layers
    hidden_sums = [None] * layers
    ffn_groups, wide_groups = [None] * layers, [None] * layers
    running = []

    def advance(after, groups=None):
        for group in running if groups is None else groups:
            if group.busy():
                after = group.step(after)
        return after

    for layer in reversed(range(layers)):
        rounded, mixed, probs, u1, hr, gr, slope, u2 = kept[layer]
        w = weights[layer]
        gains = jnp.stack([norm1_gain[layer], norm2_gain[layer]])
        da, do, du, sums, zsums, sent, ffn_kept = ffn_backward(
            own,
            grad_state,
            u2,
            u1,
            slope,
            hr,
            gr,
            out_weight,
            up_weight,
            down_weight,
            gains,
            layer,
            dp_count,
        )
        low_bit = bits_of("head")[0]
        early = bool(running)
        token = advance(do)
        if early:
            (sent,) = ordered(token, sent)
        got = swap(sent, "head", low_bit)

        def sum_ffn(after):
            values = ordered(after, ffn_kept, got)
            up_send, up_keep, down_send, down_keep = core_add(*values)
            ffn_groups[layer] = Summing(down_send, down_keep, up_send, up_keep)
            running.insert(0, ffn_groups[layer])
            return down_keep

        if early:
            token = sum_ffn(token)
        (do, du) = ordered(token, do, du)
        half_grad, away_sums, sent = attention_backward(
            own, mixed, do, probs, rounded, da, w[1], w[3], du, None, dp_count, WIDE
        )
        if early:
            token = advance(half_grad, running[:1])
            (sent,) = ordered(token, sent)
            wide_got = swap(sent, "head", low_bit)
        else:
            wide_got = swap(sent, "head", low_bit)
            token = sum_ffn(half_grad)
        (half_grad, do) = ordered(token, half_grad, do)
        grad_state, own_sums, *parts = attention_backward(
            own,
            mixed,
            do,
            probs,
            rounded,
            da,
            w[0],
            w[2],
            half_grad,
            wide_got,
            dp_count,
            WIDE if layer else LOW,
        )
        wide_groups[layer] = Summing(*parts)
        token = advance(grad_state) if layer else grad_state
        if layer:
            (grad_state,) = ordered(token, grad_state)
        running.append(wide_groups[layer])
        blocks = [own_sums[0], away_sums[0], own_sums[1], away_sums[1]]
        stacked = jnp.stack(blocks)[:, :2]
        qv_sums = jnp.concatenate(
            [
                lax.dynamic_index_in_dim(stacked, head_index ^ head, 0, keepdims=False)
                for head in range(head_count)
            ],
            axis=1,
        )
        small_sums[layer] = jnp.concatenate([sums[:6], qv_sums, zsums[:, 0]])
    small_sum = jnp.stack(small_sums)
    spread = [("head", bits_of("head")[0])] + [("dp", bit) for bit in bits_of("dp")[1:]]
    spread += [("dp", bits_of("dp")[0]), ("head", bits_of("head")[1])]
    while any(group.busy() for group in running) or spread:
        if spread:
            small_sum = small_sum + swap(small_sum, *spread.pop(0))
        token = advance(token)
    ffn_sums = [group.finish() for group in ffn_groups]
    wide_sums = [group.finish() for group in wide_groups]
    wide = [
        [both[half, :, at * part : (at + 1) * part] for half in range(2) for at in range(2)]
        for both in wide_sums
    ]
    return (
        out_state,
        grad_state,
        jnp.stack([jnp.stack(w[:3]) for w in wide]),
        small_sum[:, 6:8],
        jnp.stack([w[3] for w in wide]),
        small_sum[:, 5],
        small_sum[:, 3],
        small_sum[:, 4],
        jnp.stack([both[1] for both in ffn_sums]),
        small_sum[:, 8:].reshape(layers, -1),
        jnp.stack([both[0].T for both in ffn_sums]),
        small_sum[:, 2],
        small_sum[:, 0],
        small_sum[:, 1],
    )


def solution(mesh):
    in_specs = (
        P(("dp", "head"), None),
        P("dp", None),
        P(None, None, None, "head"),
        P(None, None, "head"),
        P(),
        P(),
        P(),
        P(),
        P(),
        P(),
        P(),
        P(),
        P(),
        P(),
        P(("dp", "head"), None),
    )
    out_specs = (
        P(("dp", "head"), None),
        P(("dp", "head"), None),
        P(None, None, "dp", "head"),
        P(),
        P(None, "dp", "head"),
        P(),
        P(),
        P(),
        P(None, "dp", "head"),
        P(),
        P(None, "head", "dp"),
        P(),
        P(),
        P(),
    )
    return jax.shard_map(
        on_device, mesh=mesh, in_specs=in_specs, out_specs=out_specs, check_vma=False
    )
```

```python
import functools
import math

import jax
import jax.numpy as jnp
from jax import lax
from jax.experimental import pallas as pl
from jax.experimental.pallas import tpu as pltpu
from jax.sharding import PartitionSpec as P

HD = 64
EPSILON = 1e-06
LOW = jnp.bfloat16
WIDE = jnp.float32
VMEM_BYTES = 58 << 20
ROOT_HALF = 0.7071067811865476
INV_ROOT_TAU = 0.3989422804014327
FAR = -1e30


def row_stats(values):
    centre = jnp.mean(values, axis=-1, keepdims=True)
    centred = values - centre
    spread = jnp.mean(centred * centred, axis=-1, keepdims=True)
    inverse = lax.rsqrt(spread + EPSILON)
    return centred * inverse, inverse


def norm_backward(upstream, xhat, inverse, gain):
    scaled = upstream * gain
    first = jnp.mean(scaled, axis=-1, keepdims=True)
    second = jnp.mean(scaled * xhat, axis=-1, keepdims=True)
    return (scaled - first - xhat * second) * inverse


def column_sum(values):
    return jnp.sum(values, axis=0, keepdims=True)


def dot_nn(left, right):
    return jnp.dot(left, right, preferred_element_type=WIDE)


def dot_nt(left, right):
    return lax.dot_general(left, right, (((1,), (1,)), ((), ())), preferred_element_type=WIDE)


def dot_tn(left, right):
    return lax.dot_general(left, right, (((0,), (0,)), ((), ())), preferred_element_type=WIDE)


def gelu_pair(z):
    cdf = 0.5 + 0.5 * lax.erf(z * ROOT_HALF)
    return z * cdf, cdf + z * (jnp.exp(z * z * -0.5) * INV_ROOT_TAU)


def pick(mask, values):
    return jnp.where(mask, values, jnp.zeros_like(values))


def head_masks(width):
    lanes = lax.broadcasted_iota(jnp.int32, (1, width), 1) // HD
    return [lanes == head for head in range(width // HD)]


def params():
    return pltpu.CompilerParams(vmem_limit_bytes=VMEM_BYTES)


def whole(array):
    return pl.BlockSpec(array.shape, lambda *ids: (0,) * array.ndim, pipeline_mode=pl.Buffered(1))


def in_place():
    return pl.BlockSpec(memory_space=pl.ANY)


def in_hbm():
    return pl.BlockSpec(memory_space=pltpu.HBM)


def shape_of(shape, kind):
    return jax.ShapeDtypeStruct(shape, kind)


def cost(flops, out_shape, operands):
    made = out_shape if isinstance(out_shape, (list, tuple)) else [out_shape]
    moved = sum(math.prod(v.shape) * jnp.dtype(v.dtype).itemsize for v in [*made, *operands])
    return pl.CostEstimate(flops=flops, bytes_accessed=moved, transcendentals=0)


def stored(shape, kind):
    return pltpu.HBM(shape, kind)


def call(kernel, name, grid, in_specs, out_specs, out_shape, scratch, scalars, operands, alias=None, flops=0, vmem=VMEM_BYTES):
    return pl.pallas_call(
        kernel,
        grid_spec=pltpu.PrefetchScalarGridSpec(
            num_scalar_prefetch=len(scalars),
            grid=grid,
            in_specs=in_specs,
            out_specs=out_specs,
            scratch_shapes=scratch,
        ),
        out_shape=out_shape,
        compiler_params=pltpu.CompilerParams(vmem_limit_bytes=vmem),
        input_output_aliases=alias or {},
        cost_estimate=cost(flops, out_shape, operands),
        name=name,
    )(*scalars, *operands)


def mask_kernel(base_ref, lengths_ref, bias_ref):
    slots, rows, _ = bias_ref.shape
    across = lax.broadcasted_iota(jnp.int32, (8, rows), 1)
    down = lax.broadcasted_iota(jnp.int32, (rows, 128), 0)
    for slot in range(slots):
        reach = jnp.int32(0)
        seg_across = jnp.zeros((8, rows), jnp.int32)
        seg_down = jnp.zeros((rows, 128), jnp.int32)
        for k in range(lengths_ref.shape[1]):
            reach = reach + lengths_ref[base_ref[0] + slot, k]
            seg_across += (across >= reach).astype(jnp.int32)
            seg_down += (down >= reach).astype(jnp.int32)
        inside = seg_down[:, 0:1] == seg_across[0:1, :]
        bias_ref[slot] = jnp.where(inside, 0.0, FAR)


def mask_bias(lengths, base, slots, slot_rows):
    smem = pl.BlockSpec(memory_space=pltpu.SMEM)
    return pl.pallas_call(
        mask_kernel,
        in_specs=[smem, smem],
        out_shape=shape_of((slots, slot_rows, slot_rows), WIDE),
        compiler_params=params(),
        name="mask_bias",
    )(base, lengths)


def attention_forward_kernel(
    x_ref, wa_ref, wb_ref, b_ref, bias_ref, *refs, aliased, tile
):
    mixed_ref, p_ref, s_ref = refs[2 * aliased :]
    rows, part = x_ref.shape[0], wa_ref.shape[0] // 3
    x = x_ref[...]
    masks = head_masks(part)

    def work(w_ref):
        q = ((dot_nt(x, w_ref[:part]) + b_ref[0]).astype(LOW) * HD**-0.5).astype(LOW)
        k = dot_nt(x, w_ref[part : 2 * part]).astype(LOW)
        v = (dot_nt(x, w_ref[2 * part :]) + b_ref[1]).astype(LOW)
        mixed_ref[0] = q
        mixed_ref[1] = k
        mixed_ref[2] = v
        total = None
        for head, mask in enumerate(masks):
            s_ref[head] = dot_nt(pick(mask, q), k)
            for start in range(0, rows, tile):
                at = slice(start, start + tile)
                s = s_ref[head, at] + bias_ref[at]
                e = jnp.exp(s - jnp.max(s, axis=1, keepdims=True))
                p_ref[head, at] = (e * (1.0 / jnp.sum(e, axis=1, keepdims=True))).astype(LOW)
            made = dot_nn(p_ref[head], pick(mask, v))
            total = made if total is None else total + made
        mixed_ref[3] = total.astype(LOW)

    for block, w_ref in enumerate((wa_ref, wb_ref)):

        @pl.when(pl.program_id(1) == block)
        def _():
            work(w_ref)


def attention_forward(x, wa, wb, qv_bias, bias, first, before, tile=64):
    rows, width = x.shape
    slots, slot_rows, _ = bias.shape
    part = wa.shape[0] // 3
    heads = part // HD
    aliased = int(before is not None)
    mixed = shape_of((4, 4, rows, part), LOW)
    probs = shape_of((4, slots, heads, slot_rows, slot_rows), LOW)
    return call(
        functools.partial(attention_forward_kernel, aliased=aliased, tile=tile),
        "attention_forward",
        (slots, 2),
        [
            pl.BlockSpec((slot_rows, width), lambda s, b: (s, 0)),
            whole(wa),
            whole(wb),
            pl.BlockSpec((None, 2, 1, part), lambda s, b: (b, 0, 0, 0)),
            pl.BlockSpec((None, slot_rows, slot_rows), lambda s, b: (s, 0, 0)),
        ]
        + [in_place(), in_place()] * aliased,
        [
            pl.BlockSpec((None, 4, slot_rows, part), lambda s, b: (first + b, 0, s, 0)),
            pl.BlockSpec(
                (None, None, heads, slot_rows, slot_rows), lambda s, b: (first + b, s, 0, 0, 0)
            ),
        ],
        [mixed, probs],
        [pltpu.VMEM((heads, slot_rows, slot_rows), WIDE)],
        [],
        [x, wa, wb, qv_bias, bias, *(before or ())],
        alias={5: 0, 6: 1} if aliased else None,
        flops=12 * rows * width * part + 16 * heads * rows * slot_rows * 256,
    )


def row_tiles(rows, tile):
    return [pl.ds(start, tile) for start in range(0, rows, tile)]


def ffn_forward_kernel(own_ref, mixed_hbm, x_hbm, wo_hbm, wu_ref, wd_ref, bu_ref, small_ref,
                       u1_hbm, hr_hbm, gr_hbm, gp_hbm, u2_hbm, low_hbm,
                       o_ref, x_ref, wo_ref, u1_ref, hr_ref, gr_ref, gp_ref, u2_ref, low_ref, in_sems, out_sems, g_sems,
                       *, layer, tile, renorm):
    step, steps = pl.program_id(0), pl.num_programs(0)
    part = o_ref.shape[2]
    tiles = row_tiles(x_ref.shape[0], tile)
    wo_copy = pltpu.make_async_copy(wo_hbm.at[layer], wo_ref, in_sems.at[0, 0])
    loads, first_out, last_out = [], [], []
    for t, at in enumerate(tiles):
        loads.append(
            [
                pltpu.make_async_copy(mixed_hbm.at[:, 3, at], o_ref.at[:, at], in_sems.at[1, t]),
                pltpu.make_async_copy(x_hbm.at[at], x_ref.at[at], in_sems.at[2, t]),
            ]
        )
        first_out.append(
            [
                pltpu.make_async_copy(u1_ref.at[at], u1_hbm.at[at], out_sems.at[0, t]),
                pltpu.make_async_copy(hr_ref.at[at], hr_hbm.at[at], out_sems.at[1, t]),
            ]
        )
        last_out.append(
            [
                pltpu.make_async_copy(u2_ref.at[at], u2_hbm.at[at], out_sems.at[2, t]),
                pltpu.make_async_copy(low_ref.at[at], low_hbm.at[at], out_sems.at[3, t]),
            ]
        )

    def g_out(chunk, slot):
        return [
            pltpu.make_async_copy(gr_ref.at[slot], gr_hbm.at[chunk], g_sems.at[0, slot]),
            pltpu.make_async_copy(gp_ref.at[slot], gp_hbm.at[chunk], g_sems.at[1, slot]),
        ]

    @pl.when(step == 0)
    def _():
        wo_copy.start()
        for pair in loads:
            for copy in pair:
                copy.start()
        wo_copy.wait()
        for t, at in enumerate(tiles):
            for copy in loads[t]:
                copy.wait()
            residual = x_ref[at].astype(WIDE)
            if renorm:
                residual = row_stats(residual)[0] * small_ref[6:7] + small_ref[7:8]
            u1 = residual + small_ref[0:1]
            for block in range(4):
                rows = pl.ds(pl.multiple_of((own_ref[0] ^ block) * part, 16), part)
                u1 = u1 + dot_nn(o_ref[block, at], wo_ref[rows, :])
            u1_ref[at] = u1
            normed = row_stats(u1)[0] * small_ref[1:2] + small_ref[2:3]
            hr_ref[at] = normed.astype(LOW)
            u2_ref[at] = normed + small_ref[3:4]
            for copy in first_out[t]:
                copy.start()

    slot = step % 2

    @pl.when(step >= 2)
    def _():
        for copy in g_out(step - 2, slot):
            copy.wait()

    z = dot_nn(hr_ref[...], wu_ref[...]) + bu_ref[...]
    g, slope = gelu_pair(z)
    gr = g.astype(LOW)
    gr_ref[slot] = gr
    gp_ref[slot] = slope.astype(LOW)
    for copy in g_out(step, slot):
        copy.start()
    u2_ref[...] += dot_nn(gr, wd_ref[...])

    @pl.when(step == steps - 1)
    def _():
        for t, at in enumerate(tiles):
            total = u2_ref[at]
            low_ref[at] = (row_stats(total)[0] * small_ref[4:5] + small_ref[5:6]).astype(LOW)
            for copy in last_out[t]:
                copy.start()
        for copy in [*g_out(step - 1, 1 - slot), *g_out(step, slot)]:
            copy.wait()
        for pair in first_out + last_out:
            for copy in pair:
                copy.wait()


def ffn_forward(own, mixed, x, wo, wu, wd, bu, small, layer, renorm, tile=512):
    _, _, rows, part = mixed.shape
    width, hidden = wu.shape[1:]
    chunks = hidden // width
    fixed = lambda v: pl.BlockSpec(v.shape, lambda i, o: (0,) * v.ndim)
    sems = lambda *shape: pltpu.SemaphoreType.DMA(shape)
    return call(
        functools.partial(ffn_forward_kernel, layer=layer, tile=tile, renorm=renorm),
        "ffn_forward",
        (chunks,),
        [
            in_place(),
            in_place(),
            in_place(),
            pl.BlockSpec((None, width, width), lambda i, o: (layer, 0, i)),
            pl.BlockSpec((None, width, width), lambda i, o: (layer, i, 0)),
            pl.BlockSpec((None, 1, width), lambda i, o: (i, 0, 0)),
            fixed(small),
        ],
        [in_place()] * 6,
        [
            shape_of((rows, width), WIDE),
            shape_of((rows, width), LOW),
            shape_of((chunks, rows, width), LOW),
            shape_of((chunks, rows, width), LOW),
            shape_of((rows, width), WIDE),
            shape_of((rows, width), LOW),
        ],
        [
            pltpu.VMEM((4, rows, part), LOW),
            pltpu.VMEM((rows, width), x.dtype),
            pltpu.VMEM((width, width), LOW),
            pltpu.VMEM((rows, width), WIDE),
            pltpu.VMEM((rows, width), LOW),
            pltpu.VMEM((2, rows, width), LOW),
            pltpu.VMEM((2, rows, width), LOW),
            pltpu.VMEM((rows, width), WIDE),
            pltpu.VMEM((rows, width), LOW),
            sems(3, rows // tile),
            sems(4, rows // tile),
            sems(2, 2),
        ],
        [own],
        [mixed, x, wo, wu, wd, bu, small],
        flops=6 * rows * width * (width + 2 * hidden),
    )


def reversed_bits(value, count):
    made = 0
    for bit in range(count):
        made = made | (((value >> bit) & 1) << (count - 1 - bit))
    return made


def each_chunk(made, dp_count):
    rows = made.shape[0] // dp_count
    for dp in range(dp_count):
        yield dp, made[dp * rows : (dp + 1) * rows]


def place(dp, own_dp, dp_count):
    away = dp ^ own_dp
    return away & 1, reversed_bits(away >> 1, dp_count.bit_length() - 2)


def ffn_backward_kernel(own_ref, gx_hbm, u2_hbm, u1_hbm, gp_hbm, hr_hbm, gr_hbm, wo_hbm, wu_ref, wd_ref, gain_ref,
                        da_hbm, do_hbm, du_hbm, sums_ref, zsum_ref, send_ref, keep_ref,
                        gx_ref, u2_ref, u1_ref, gp_ref, hr_ref, gr_ref, wo_ref, acc_ref, df_ref, dz_ref, da_ref, do_ref,
                        in_sems, out_sems, g_sems, *, layer, tile, dp_count):
    step, steps = pl.program_id(0), pl.num_programs(0)
    own, own_dp = own_ref[0], own_ref[1]
    part = do_ref.shape[2]
    tiles = row_tiles(gx_ref.shape[0], tile)
    count = len(tiles)
    loads, last_out = [], []
    for t, at in enumerate(tiles):
        loads.append(
            [
                pltpu.make_async_copy(gx_hbm.at[at], gx_ref.at[at], in_sems.at[0, t]),
                pltpu.make_async_copy(u2_hbm.at[at], u2_ref.at[at], in_sems.at[1, t]),
            ]
        )
        last_out.append(
            [
                pltpu.make_async_copy(u2_ref.at[at], du_hbm.at[at], out_sems.at[0, t]),
                pltpu.make_async_copy(da_ref.at[:, at], da_hbm.at[:, at], out_sems.at[1, t]),
                pltpu.make_async_copy(do_ref.at[:, at], do_hbm.at[:, at], out_sems.at[2, t]),
            ]
        )
    hr_copy = pltpu.make_async_copy(hr_hbm, hr_ref, in_sems.at[2, 0])
    u1_copy = pltpu.make_async_copy(u1_hbm, u1_ref, in_sems.at[2, 1])
    wo_copy = pltpu.make_async_copy(wo_hbm.at[layer], wo_ref, in_sems.at[2, 2])

    def streams(at_step):
        slot, head = at_step % 2, own ^ head_order(at_step)
        return (
            pltpu.make_async_copy(gp_hbm.at[head], gp_ref.at[slot], g_sems.at[0, slot]),
            pltpu.make_async_copy(gr_hbm.at[head], gr_ref.at[slot], g_sems.at[1, slot]),
        )

    slot = step % 2
    gp_copy, gr_copy = streams(step)

    @pl.when(step == 0)
    def _():
        for pair in loads:
            for copy in pair:
                copy.start()

        gp_copy.start()
        hr_copy.start()
        gr_copy.start()

    @pl.when(step < steps - 1)
    def _():
        for copy in streams(step + 1):
            copy.start()

    @pl.when(step == 1)
    def _():
        u1_copy.start()
        wo_copy.start()

    @pl.when(step == 0)
    def _():
        sums_ref[...] = jnp.zeros_like(sums_ref)
        for t, at in enumerate(tiles):
            for copy in loads[t]:
                copy.wait()
            gx = gx_ref[at].astype(WIDE)
            xhat, inverse = row_stats(u2_ref[at])
            sums_ref[0:1] += column_sum(gx * xhat)
            sums_ref[1:2] += column_sum(gx)
            gv = norm_backward(gx, xhat, inverse, gain_ref[1:2])
            df = gv.astype(LOW)
            df_ref[at] = df
            sums_ref[2:3] += column_sum(df.astype(WIDE))
            acc_ref[at] = gv

    dg = dot_nt(df_ref[...], wd_ref[...])
    gp_copy.wait()
    dz = (dg * gp_ref[slot].astype(WIDE)).astype(LOW)
    dz_ref[...] = dz
    zsum_ref[...] = column_sum(dz.astype(WIDE))
    acc_ref[...] += dot_nt(dz_ref[...], wu_ref[...])

    @pl.when(step == 0)
    def _():
        hr_copy.wait()

    up = dot_tn(hr_ref[...], dz_ref[...]).astype(LOW)
    gr_copy.wait()
    down = dot_tn(df_ref[...], gr_ref[slot]).astype(LOW)
    for out, wanted in ((send_ref, step < 2), (keep_ref, step >= 2)):

        @pl.when(wanted)
        def _():
            for which, made in enumerate((up, down)):
                for dp, chunk in each_chunk(made, dp_count):
                    out[(which, *place(dp, own_dp, dp_count))] = chunk

    @pl.when(step == steps - 1)
    def _():
        u1_copy.wait()
        wo_copy.wait()
        for t, at in enumerate(tiles):
            total = acc_ref[at]
            xhat, inverse = row_stats(u1_ref[at])
            sums_ref[3:4] += column_sum(total * xhat)
            sums_ref[4:5] += column_sum(total)
            du = norm_backward(total, xhat, inverse, gain_ref[0:1])
            u2_ref[at] = du
            da = du.astype(LOW)
            for block in range(4):
                da_ref[block, at] = da[:, block * part : (block + 1) * part]
            sums_ref[5:6] += column_sum(da.astype(WIDE))
            for block in range(4):
                rows = pl.ds(pl.multiple_of((own ^ block) * part, 16), part)
                do_ref[block, at] = dot_nt(da, wo_ref[rows, :]).astype(LOW)
            for copy in last_out[t]:
                copy.start()
        for several in last_out:
            for copy in several:
                copy.wait()


def head_order(step):
    return jnp.where(step < 2, 1 + 2 * step, 2 * (step - 2))


def ffn_backward(own, gx, u2, u1, gp, hr, gr, wo, wu, wd, gains, layer, dp_count, tile=512):
    rows, width = gx.shape
    chunks = gp.shape[0]
    part = width // 4
    chunk_rows = width // dp_count
    rest = dp_count // 2
    fixed = lambda s: pl.BlockSpec(s.shape, lambda i, o: (0,) * len(s.shape))
    head = lambda i, o: o[0] ^ head_order(i)
    block = (2, None, 2, rest, chunk_rows, width)
    sums = shape_of((8, width), WIDE)
    grads = stored((2, 2, 2, rest, chunk_rows, width), LOW)
    sems = lambda *shape: pltpu.SemaphoreType.DMA(shape)
    low = lambda *shape: pltpu.VMEM(shape, LOW)
    wide = lambda *shape: pltpu.VMEM(shape, WIDE)
    return call(
        functools.partial(ffn_backward_kernel, layer=layer, tile=tile, dp_count=dp_count),
        "ffn_backward",
        (chunks,),
        [in_place()] * 7
        + [
            pl.BlockSpec((None, width, width), lambda i, o: (layer, 0, head(i, o))),
            pl.BlockSpec((None, width, width), lambda i, o: (layer, head(i, o), 0)),
            fixed(gains),
        ],
        [
            in_place(),
            in_place(),
            in_place(),
            fixed(sums),
            pl.BlockSpec((None, 1, width), lambda i, o: (head(i, o), 0, 0)),
            pl.BlockSpec(block, lambda i, o: (0, jnp.minimum(i, 1), 0, 0, 0, 0)),
            pl.BlockSpec(block, lambda i, o: (0, jnp.maximum(i - 2, 0), 0, 0, 0, 0)),
        ],
        [
            shape_of((4, rows, part), LOW),
            shape_of((4, rows, part), LOW),
            shape_of((rows, width), WIDE),
            sums,
            shape_of((chunks, 1, width), WIDE),
            grads,
            grads,
        ],
        [
            pltpu.VMEM((rows, width), gx.dtype),
            wide(rows, width),
            wide(rows, width),
            low(2, rows, width),
            low(rows, width),
            low(2, rows, width),
            low(width, width),
            wide(rows, width),
            low(rows, width),
            low(rows, width),
            low(4, rows, part),
            low(4, rows, part),
            sems(3, max(rows // tile, 3)),
            sems(3, rows // tile),
            sems(2, 2),
        ],
        [own],
        [gx, u2, u1, gp, hr, gr, wo, wu, wd, gains],
        flops=4 * rows * width * (width + 4 * chunks * width),
    )


def split_rows(made, got_ref, own_dp, dp_count, send_ref, keep_ref):
    for dp, chunk in each_chunk(made, dp_count):
        away, rest = place(dp, own_dp, dp_count)
        summed = (chunk + got_ref[away, rest].astype(WIDE)).astype(LOW)

        @pl.when(away == 1)
        def _():
            send_ref[rest] = summed

        @pl.when(away == 0)
        def _():
            keep_ref[rest] = summed


def add_rows(made, got_ref, own_dp, dp_count, out_ref):
    for dp, chunk in each_chunk(made, dp_count):
        at = place(dp, own_dp, dp_count)
        out_ref[at] = (chunk + got_ref[at].astype(WIDE)).astype(LOW)


def core_add_kernel(kept_ref, got_ref, up_send, up_keep, down_send, down_keep):
    step = pl.program_id(0)

    which, away = step // 2, jnp.where(step < 2, step, 3 - step)

    def summed(at):
        return (kept_ref[at].astype(WIDE) + got_ref[which, away, at].astype(WIDE)).astype(LOW)

    @pl.when(step < 2)
    def _():
        up_keep[...] = summed(0)
        up_send[...] = summed(1)

    for out, wanted in ((down_send, 2), (down_keep, 3)):

        @pl.when(step == wanted)
        def _():
            out[0] = summed(0)
            out[1] = summed(1)


def core_add(kept, got):
    _, _, _, rest, chunk_rows, width = kept.shape

    def at(i):
        return (i // 2, jnp.where(i < 2, i, 3 - i), 0, 0, 0, 0)

    block = pl.BlockSpec((None, None, 2, rest, chunk_rows, width), at)
    up = pl.BlockSpec((None, rest, chunk_rows, width), lambda i: (jnp.minimum(i, 1), 0, 0, 0))
    down = pl.BlockSpec((2, rest, chunk_rows, width), lambda i: (0, 0, 0, 0))
    made = stored((2, rest, chunk_rows, width), LOW)
    return call(
        core_add_kernel,
        "core_add",
        (4,),
        [block, pl.BlockSpec(memory_space=pltpu.VMEM)],
        [up, up, down, down],
        [made] * 4,
        [],
        [],
        [kept, got],
        vmem=24 << 20,
    )


def attention_backward_kernel(own_ref, mixed_ref, do_ref, p_ref, x_ref, o_ref, da_ref, wa_ref, wb_ref, gx_ref, *refs,
                              dp_count, tile, keep):
    if keep:
        got_ref, *refs = refs
    out_ref, sums_ref, *refs = refs
    grads = refs[: 4 if keep else 1]
    t_ref, ds_ref, parts_ref, xt_ref, ot_ref, acc_ref = refs[4 if keep else 1 :]
    slot, block = pl.program_id(0), pl.program_id(1)
    last = pl.num_programs(0) - 1
    own, own_dp = own_ref[0], own_ref[1]
    rows, part = mixed_ref.shape[1:]

    @pl.when((slot == 0) & (block == 0))
    def _():
        xt_ref[...] = x_ref[...].T
        for r in range(4):
            ot_ref[pl.ds(pl.multiple_of((own ^ r) * part, 16), part), :] = o_ref[r].T
        sums_ref[...] = jnp.zeros_like(sums_ref)

    dq = dk = dv = None
    for head, mask in enumerate(head_masks(part)):
        do = pick(mask, do_ref[...])
        t_ref[head] = dot_nt(do, mixed_ref[2])
        for start in range(0, rows, tile):
            at = slice(start, start + tile)
            p = p_ref[head, at].astype(WIDE)
            dp = t_ref[head, at]
            share = jnp.sum(p * dp, axis=1, keepdims=True)
            ds_ref[head, at] = (p * (dp - share)).astype(LOW)
        made = (
            dot_nn(ds_ref[head], pick(mask, mixed_ref[1])),
            dot_tn(ds_ref[head], pick(mask, mixed_ref[0])),
            dot_tn(p_ref[head], do),
        )
        dq, dk, dv = made if dq is None else (dq + made[0], dk + made[1], dv + made[2])
    dq = (dq * HD**-0.5).astype(LOW)
    dk = dk.astype(LOW)
    dv = dv.astype(LOW)
    sums_ref[block, 0:1] += column_sum(dq.astype(WIDE))
    sums_ref[block, 1:2] += column_sum(dv.astype(WIDE))
    joined = jnp.concatenate([dq, dk, dv], axis=1)
    parts_ref[block, pl.ds(pl.multiple_of(slot * rows, rows), rows), :] = joined
    weights = jnp.where(block == 0, wa_ref[...], wb_ref[...])
    passed = dot_nn(joined, weights)

    @pl.when(block == 0)
    def _():
        acc_ref[...] = gx_ref[...] + passed

    @pl.when(block == 1)
    def _():
        out_ref[...] = (acc_ref[...] + passed).astype(out_ref.dtype)

    @pl.when(slot == last)
    def _():
        first = dot_nn(xt_ref[...], parts_ref[block])
        second = dot_nn(ot_ref[...], da_ref[...])
        made = jnp.concatenate([first, second], axis=1)
        if not keep:
            for dp, chunk in each_chunk(made.astype(LOW), dp_count):
                grads[0][place(dp, own_dp, dp_count)] = chunk
            return
        half = made.shape[1] // 2
        a_send, a_keep, b_send, b_keep = grads
        got = [got_ref.at[:, :, :, :half], got_ref.at[:, :, :, half:]]
        for where_to, wanted in ((a_keep, 0), (a_send, 1)):

            @pl.when(block == wanted)
            def _():
                add_rows(made[:, :half], got[0], own_dp, dp_count, where_to)

        split_rows(made[:, half:], got[1], own_dp, dp_count, b_send, b_keep)


def attention_backward(own, mixed, do, probs, x, da, wa, wb, gx, got, dp_count, out_type, tile=64):
    rows, width = x.shape
    part = mixed.shape[3]
    _, slots, heads, slot_rows, _ = probs.shape
    chunk_rows, rest = width // dp_count, dp_count // 2
    keep = got is not None
    away = 0 if keep else 1
    block_of = lambda b: 2 * b + away
    row = pl.BlockSpec((slot_rows, width), lambda s, b, o: (s, 0))
    last = slots - 1
    late = lambda s, b: jnp.where(s == last, b, 0)
    in_specs = [
        pl.BlockSpec((None, 3, slot_rows, part), lambda s, b, o: (block_of(b), 0, s, 0)),
        pl.BlockSpec((None, slot_rows, part), lambda s, b, o: (block_of(b), s, 0)),
        pl.BlockSpec(
            (None, None, heads, slot_rows, slot_rows), lambda s, b, o: (block_of(b), s, 0, 0, 0)
        ),
        whole(x),
        pl.BlockSpec((4, None, rows, part), lambda s, b, o: (0, 3, 0, 0), pipeline_mode=pl.Buffered(1)),
        pl.BlockSpec((None, rows, part), lambda s, b, o: (o[0] ^ block_of(late(s, b)), 0, 0)),
        whole(wa),
        whole(wb),
        row,
    ]
    operands = [mixed, do, probs, x, mixed, da, wa, wb, gx]
    sums = shape_of((2, 8, part), WIDE)
    out_specs = [row, pl.BlockSpec(sums.shape, lambda s, b, o: (0, 0, 0))]
    out_shape = [shape_of((rows, width), out_type), sums]
    whole_block = lambda w: pl.BlockSpec((2, rest, chunk_rows, w), lambda s, b, o: (0, 0, 0, 0))
    if keep:
        in_specs.append(
            pl.BlockSpec(
                (None, 2, rest, chunk_rows, width), lambda s, b, o: (late(s, b), 0, 0, 0, 0)
            )
        )
        operands.append(got)
        half = width // 2
        b_block = pl.BlockSpec(
            (None, rest, chunk_rows, half), lambda s, b, o: (late(s, b), 0, 0, 0)
        )
        out_specs += [whole_block(half)] * 2 + [b_block] * 2
        out_shape += [stored((2, rest, chunk_rows, half), LOW)] * 4
    else:
        out_specs.append(
            pl.BlockSpec(
                (None, 2, rest, chunk_rows, width), lambda s, b, o: (late(s, b), 0, 0, 0, 0)
            )
        )
        out_shape.append(stored((2, 2, rest, chunk_rows, width), LOW))
    return call(
        functools.partial(attention_backward_kernel, dp_count=dp_count, tile=tile, keep=keep),
        "attention_backward",
        (slots, 2),
        in_specs,
        out_specs,
        out_shape,
        [
            pltpu.VMEM((heads, slot_rows, slot_rows), WIDE),
            pltpu.VMEM((heads, slot_rows, slot_rows), LOW),
            pltpu.VMEM((2, rows, 3 * part), LOW),
            pltpu.VMEM((width, rows), LOW),
            pltpu.VMEM((width, rows), LOW),
            pltpu.VMEM((slot_rows, width), WIDE),
        ],
        [own],
        operands,
        flops=36 * heads * rows * slot_rows * 256,
    )


def bits_of(axis):
    size = lax.axis_size(axis)
    return [1 << bit for bit in range(size.bit_length() - 1)]


def swap(value, axis, bit):
    size = lax.axis_size(axis)
    return lax.ppermute(value, axis, [(i, i ^ bit) for i in range(size)])


def add_split_kernel(*refs, merge_in, merge_out):
    inputs = 2 if merge_in else 4
    outputs = 2 if merge_out else 4
    ins, outs = refs[:inputs], refs[inputs : inputs + outputs]
    kept_ref, send_ref, keep_ref, in_sems, out_sems = refs[inputs + outputs :]
    half = send_ref.shape[1]
    loads, got, stores = [], [], []
    for part in range(2):
        kept, came = (ins[0].at[part], ins[1].at[part]) if merge_in else ins[2 * part : 2 * part + 2]
        send, keep = (
            (outs[0].at[part], outs[1].at[part]) if merge_out else outs[2 * part : 2 * part + 2]
        )
        got.append(came)
        loads.append(pltpu.make_async_copy(kept, kept_ref.at[part], in_sems.at[part]))
        stores.append(
            [
                pltpu.make_async_copy(send_ref.at[part], send, out_sems.at[part, 0]),
                pltpu.make_async_copy(keep_ref.at[part], keep, out_sems.at[part, 1]),
            ]
        )
    for copy in loads:
        copy.start()
    for part in range(2):
        loads[part].wait()
        for at, (out, copy) in enumerate(zip((send_ref, keep_ref), stores[part])):
            rows = pl.ds(half * (1 - at), half)
            out[part] = (kept_ref[part, rows].astype(WIDE) + got[part][rows].astype(WIDE)).astype(LOW)
            copy.start()
    for copies in stores:
        for copy in copies:
            copy.wait()


def add_split(ins, merge_in, merge_out):
    size, rows, columns = ins[0].shape[-3:]
    half = (size // 2, rows, columns)
    out_shape = [stored((2, *half), LOW)] * 2 if merge_out else [stored(half, LOW)] * 4
    return pl.pallas_call(
        functools.partial(add_split_kernel, merge_in=merge_in, merge_out=merge_out),
        in_specs=[in_hbm(), pl.BlockSpec(memory_space=pltpu.VMEM)] * (len(ins) // 2),
        out_specs=[in_hbm()] * len(out_shape),
        out_shape=out_shape,
        scratch_shapes=[
            pltpu.VMEM((2, size, rows, columns), LOW),
            pltpu.VMEM((2, *half), LOW),
            pltpu.VMEM((2, *half), LOW),
            pltpu.SemaphoreType.DMA((2,)),
            pltpu.SemaphoreType.DMA((2, 2)),
        ],
        compiler_params=pltpu.CompilerParams(vmem_limit_bytes=16 << 20),
        cost_estimate=cost(0, out_shape, ins),
        name="add_split",
    )(*ins)


class Summing:
    def __init__(self, a_send, a_keep, b_send, b_keep):
        head, dp = bits_of("head"), bits_of("dp")
        self.stages = [(("dp", dp[0]), ("head", head[1]))] + [(("dp", bit),) for bit in dp[1:]]
        self.at = 0
        self.kept = [a_keep, b_keep]
        self.got = [swap(a_send, "head", head[1]), swap(b_send, "dp", dp[0])]

    def busy(self):
        return self.at < len(self.stages)

    def step(self, after):
        stage = self.stages[self.at]
        merge_in, merge_out = len(self.kept) == 1, len(stage) == 1
        ins = [v for pair in zip(self.kept, self.got) for v in pair]
        lead = 1 if merge_in else 0
        ins = [v.reshape(*v.shape[:lead], -1, *v.shape[-2:]) for v in ins]
        ins, _ = lax.optimization_barrier((ins, after))
        outs = add_split(ins, merge_in, merge_out)
        if merge_out:
            self.got, self.kept = [swap(outs[0], *stage[0])], [outs[1]]
        else:
            self.got = [swap(outs[0], *stage[0]), swap(outs[2], *stage[1])]
            self.kept = [outs[1], outs[3]]
        self.at += 1
        return outs[-1]


def last_sums_kernel(*refs, layers):
    ins, outs = refs[: 4 * layers + 2], refs[4 * layers + 2 :]
    qkv, qv, out_w, out_b, gain1, shift1, up_w, up_b, down_w, down_b, gain2, shift2 = outs
    part = out_w.shape[2]
    width = down_b.shape[1]
    rows = ins[-2][...] + ins[-1][...]
    for layer in range(layers):
        ffn_kept, ffn_got, wide_kept, wide_got = ins[4 * layer : 4 * layer + 4]
        down_w[layer] = ffn_kept[0, 0].astype(WIDE) + ffn_got[0, 0].astype(WIDE)
        up_w[layer] = ffn_kept[1, 0].astype(WIDE) + ffn_got[1, 0].astype(WIDE)
        for half in range(2):
            both = wide_kept[half, 0].astype(WIDE) + wide_got[half, 0].astype(WIDE)
            for at in range(2):
                which = 2 * half + at
                block = both[:, at * part : (at + 1) * part]
                if which < 3:
                    qkv[layer, which] = block
                else:
                    out_w[layer] = block
        for row, out in enumerate((gain2, shift2, down_b, gain1, shift1, out_b)):
            out[layer : layer + 1] = rows[layer, row : row + 1]
        qv[layer] = rows[layer, 6:8]
        for row in range(up_b.shape[1] // width):
            at = slice(row * width, (row + 1) * width)
            up_b[layer : layer + 1, at] = rows[layer, 8 + row : 9 + row]


def last_sums(groups, small, passing):
    layers, _, width = small.shape
    ins, specs = [], []
    for group in groups:
        ins += [group.kept[0], group.got[0]]
    ins = [v.reshape(2, 1, *v.shape[-2:]) for v in ins] + [small, passing]
    rows, part = ins[0].shape[2], ins[2].shape[3] // 2
    hidden = (small.shape[1] - 8) * width
    shapes = [
        (layers, 3, rows, part),
        (layers, 2, width),
        (layers, rows, part),
        (layers, width),
        (layers, width),
        (layers, width),
        (layers, rows, width),
        (layers, hidden),
        (layers, rows, width),
        (layers, width),
        (layers, width),
        (layers, width),
    ]
    spec = lambda shape: pl.BlockSpec(shape, lambda i: (0,) * len(shape))
    specs = [spec(v.shape) for v in ins]
    return call(
        functools.partial(last_sums_kernel, layers=layers),
        "last_sums",
        (1,),
        specs,
        [spec(shape) for shape in shapes],
        [shape_of(shape, WIDE) for shape in shapes],
        [],
        [],
        ins,
        vmem=24 << 20,
    )


def ordered(after, *values):
    values, _ = lax.optimization_barrier((values, after))
    return values


def near_blocks(block):
    low, high = bits_of("head")
    return block, swap(block, "head", low), swap(block, "head", high)


def gathered_pairs(block):
    own, near, far = near_blocks(block)
    return jnp.stack([own, near]), jnp.stack([far, swap(far, "head", bits_of("head")[0])])


def on_device(
    tokens,
    seq_lengths,
    qkv_weight,
    qv_bias,
    out_weight,
    out_bias,
    norm1_gain,
    norm1_shift,
    up_weight,
    up_bias,
    down_weight,
    down_bias,
    norm2_gain,
    norm2_shift,
    out_grad,
):
    head_count, dp_count = lax.axis_size("head"), lax.axis_size("dp")
    head_index, dp_index = lax.axis_index("head"), lax.axis_index("dp")
    own = jnp.stack([head_index, dp_index]).astype(jnp.int32)
    local_rows, width = tokens.shape
    slot_rows = local_rows * head_count // seq_lengths.shape[0]
    slots = local_rows // slot_rows
    layers = qkv_weight.shape[0]
    part = width // head_count
    turned = jnp.swapaxes(qkv_weight, 2, 3).reshape(layers, 3 * part, width)
    near_bias, far_bias = gathered_pairs(qv_bias[:, :, None])
    weights = [near_blocks(turned[0])]
    base = (head_index * slots).astype(jnp.int32).reshape(1)
    bias = mask_bias(seq_lengths, base, slots, slot_rows)
    up_rows = up_bias.reshape(layers, -1, 1, width)
    rounded, residual = tokens, tokens
    kept = []
    for layer in range(layers):
        before = max(layer - 1, 0)
        small = jnp.stack(
            [
                out_bias[layer],
                norm1_gain[layer],
                norm1_shift[layer],
                down_bias[layer],
                norm2_gain[layer],
                norm2_shift[layer],
                norm2_gain[before],
                norm2_shift[before],
            ]
        )
        own_w, near_w, far_w = weights[layer]
        near = attention_forward(rounded, own_w, near_w, near_bias[:, layer], bias, 0, None)
        (far_w, far_b) = ordered(near[0], far_w, far_bias[:, layer])
        both_w = swap(far_w, "head", bits_of("head")[0])
        if layer + 1 < layers:
            (later,) = ordered(near[0], turned[layer + 1])
            weights.append(near_blocks(later))
        mixed, probs = attention_forward(rounded, far_w, both_w, far_b, bias, 2, near)
        w = (own_w, near_w, far_w, both_w)
        weights[layer] = w
        u1, hr, gr, slope, u2, low = ffn_forward(
            own,
            mixed,
            residual,
            out_weight,
            up_weight,
            down_weight,
            up_rows[layer],
            small,
            layer,
            layer > 0,
        )
        kept.append((rounded, mixed, probs, u1, hr, gr, slope, u2))
        rounded, residual = low, u2
    out_state = rounded
    grad_state = out_grad
    small_sums = [None] * layers
    hidden_sums = [None] * layers
    ffn_groups, wide_groups = [None] * layers, [None] * layers
    running = []

    def advance(after, groups=None):
        for group in running if groups is None else groups:
            if group.busy():
                after = group.step(after)
        return after

    for layer in reversed(range(layers)):
        rounded, mixed, probs, u1, hr, gr, slope, u2 = kept[layer]
        w = weights[layer]
        gains = jnp.stack([norm1_gain[layer], norm2_gain[layer]])
        da, do, du, sums, zsums, sent, ffn_kept = ffn_backward(
            own,
            grad_state,
            u2,
            u1,
            slope,
            hr,
            gr,
            out_weight,
            up_weight,
            down_weight,
            gains,
            layer,
            dp_count,
        )
        low_bit = bits_of("head")[0]
        early = bool(running)
        token = advance(do)
        if early:
            (sent,) = ordered(token, sent)
        got = swap(sent, "head", low_bit)

        def sum_ffn(after):
            values = ordered(after, ffn_kept, got)
            up_send, up_keep, down_send, down_keep = core_add(*values)
            ffn_groups[layer] = Summing(down_send, down_keep, up_send, up_keep)
            running.insert(0, ffn_groups[layer])
            return down_keep

        if early:
            token = sum_ffn(token)
        (do, du) = ordered(token, do, du)
        half_grad, away_sums, sent = attention_backward(
            own, mixed, do, probs, rounded, da, w[1], w[3], du, None, dp_count, WIDE
        )
        if early:
            token = advance(half_grad)
            (sent,) = ordered(token, sent)
            wide_got = swap(sent, "head", low_bit)
        else:
            wide_got = swap(sent, "head", low_bit)
            token = sum_ffn(half_grad)
        (half_grad, do) = ordered(token, half_grad, do)
        grad_state, own_sums, *parts = attention_backward(
            own,
            mixed,
            do,
            probs,
            rounded,
            da,
            w[0],
            w[2],
            half_grad,
            wide_got,
            dp_count,
            WIDE if layer else LOW,
        )
        wide_groups[layer] = Summing(*parts)
        token = advance(grad_state) if layer else grad_state
        if layer:
            (grad_state,) = ordered(token, grad_state)
        running.append(wide_groups[layer])
        blocks = [own_sums[0], away_sums[0], own_sums[1], away_sums[1]]
        stacked = jnp.stack(blocks)[:, :2]
        qv_sums = jnp.concatenate(
            [
                lax.dynamic_index_in_dim(stacked, head_index ^ head, 0, keepdims=False)
                for head in range(head_count)
            ],
            axis=1,
        )
        small_sums[layer] = jnp.concatenate([sums[:6], qv_sums, zsums[:, 0]])
    small_sum = jnp.stack(small_sums)
    spread = [("head", bits_of("head")[0])] + [("dp", bit) for bit in bits_of("dp")[1:]]
    spread += [("dp", bits_of("dp")[0]), ("head", bits_of("head")[1])]
    passing = swap(small_sum, *spread.pop(0))
    while any(group.busy() for group in running) or spread:
        token = advance(token)
        if spread:
            (small_sum, passing) = ordered(token, small_sum, passing)
            small_sum = small_sum + passing
            token = small_sum
            passing = swap(small_sum, *spread.pop(0))
    groups = [group for pair in zip(ffn_groups, wide_groups) for group in pair]
    qkv, qv, out_w, out_b, gain1, shift1, up_w, up_b, down_w, down_b, gain2, shift2 = last_sums(
        groups, small_sum, passing
    )
    return (
        out_state,
        grad_state,
        qkv,
        qv,
        out_w,
        out_b,
        gain1,
        shift1,
        up_w,
        up_b,
        jnp.swapaxes(down_w, 1, 2),
        down_b,
        gain2,
        shift2,
    )


def solution(mesh):
    in_specs = (
        P(("dp", "head"), None),
        P("dp", None),
        P(None, None, None, "head"),
        P(None, None, "head"),
        P(),
        P(),
        P(),
        P(),
        P(),
        P(),
        P(),
        P(),
        P(),
        P(),
        P(("dp", "head"), None),
    )
    out_specs = (
        P(("dp", "head"), None),
        P(("dp", "head"), None),
        P(None, None, "dp", "head"),
        P(),
        P(None, "dp", "head"),
        P(),
        P(),
        P(),
        P(None, "dp", "head"),
        P(),
        P(None, "head", "dp"),
        P(),
        P(),
        P(),
    )
    return jax.shard_map(
        on_device, mesh=mesh, in_specs=in_specs, out_specs=out_specs, check_vma=False
    )
```

```python
import functools
import math

import jax
import jax.numpy as jnp
from jax import lax
from jax.experimental import pallas as pl
from jax.experimental.pallas import tpu as pltpu
from jax.sharding import PartitionSpec as P

HD = 64
EPSILON = 1e-06
LOW = jnp.bfloat16
WIDE = jnp.float32
VMEM_BYTES = 58 << 20
ROOT_HALF = 0.7071067811865476
INV_ROOT_TAU = 0.3989422804014327
FAR = -1e30


def row_stats(values):
    centre = jnp.mean(values, axis=-1, keepdims=True)
    centred = values - centre
    spread = jnp.mean(centred * centred, axis=-1, keepdims=True)
    inverse = lax.rsqrt(spread + EPSILON)
    return centred * inverse, inverse


def norm_backward(upstream, xhat, inverse, gain):
    scaled = upstream * gain
    first = jnp.mean(scaled, axis=-1, keepdims=True)
    second = jnp.mean(scaled * xhat, axis=-1, keepdims=True)
    return (scaled - first - xhat * second) * inverse


def column_sum(values):
    return jnp.sum(values, axis=0, keepdims=True)


def dot_nn(left, right):
    return jnp.dot(left, right, preferred_element_type=WIDE)


def dot_nt(left, right):
    return lax.dot_general(left, right, (((1,), (1,)), ((), ())), preferred_element_type=WIDE)


def dot_tn(left, right):
    return lax.dot_general(left, right, (((0,), (0,)), ((), ())), preferred_element_type=WIDE)


def gelu_pair(z):
    cdf = 0.5 + 0.5 * lax.erf(z * ROOT_HALF)
    return z * cdf, cdf + z * (jnp.exp(z * z * -0.5) * INV_ROOT_TAU)


def pick(mask, values):
    return jnp.where(mask, values, jnp.zeros_like(values))


def head_masks(width):
    lanes = lax.broadcasted_iota(jnp.int32, (1, width), 1) // HD
    return [lanes == head for head in range(width // HD)]


def params():
    return pltpu.CompilerParams(vmem_limit_bytes=VMEM_BYTES)


def whole(array):
    return pl.BlockSpec(array.shape, lambda *ids: (0,) * array.ndim, pipeline_mode=pl.Buffered(1))


def in_place():
    return pl.BlockSpec(memory_space=pl.ANY)


def in_hbm():
    return pl.BlockSpec(memory_space=pltpu.HBM)


def shape_of(shape, kind):
    return jax.ShapeDtypeStruct(shape, kind)


def cost(flops, out_shape, operands):
    if not flops:
        return pl.CostEstimate(flops=0, bytes_accessed=0, transcendentals=0)
    made = out_shape if isinstance(out_shape, (list, tuple)) else [out_shape]
    moved = sum(math.prod(v.shape) * jnp.dtype(v.dtype).itemsize for v in [*made, *operands])
    return pl.CostEstimate(flops=flops, bytes_accessed=moved, transcendentals=0)


def stored(shape, kind):
    return pltpu.HBM(shape, kind)


def call(kernel, name, grid, in_specs, out_specs, out_shape, scratch, scalars, operands, alias=None, flops=0, vmem=VMEM_BYTES):
    return pl.pallas_call(
        kernel,
        grid_spec=pltpu.PrefetchScalarGridSpec(
            num_scalar_prefetch=len(scalars),
            grid=grid,
            in_specs=in_specs,
            out_specs=out_specs,
            scratch_shapes=scratch,
        ),
        out_shape=out_shape,
        compiler_params=pltpu.CompilerParams(vmem_limit_bytes=vmem),
        input_output_aliases=alias or {},
        cost_estimate=cost(flops, out_shape, operands),
        name=name,
    )(*scalars, *operands)


def mask_kernel(base_ref, lengths_ref, bias_ref):
    slots, rows, _ = bias_ref.shape
    across = lax.broadcasted_iota(jnp.int32, (8, rows), 1)
    down = lax.broadcasted_iota(jnp.int32, (rows, 128), 0)
    for slot in range(slots):
        reach = jnp.int32(0)
        seg_across = jnp.zeros((8, rows), jnp.int32)
        seg_down = jnp.zeros((rows, 128), jnp.int32)
        for k in range(lengths_ref.shape[1]):
            reach = reach + lengths_ref[base_ref[0] + slot, k]
            seg_across += (across >= reach).astype(jnp.int32)
            seg_down += (down >= reach).astype(jnp.int32)
        inside = seg_down[:, 0:1] == seg_across[0:1, :]
        bias_ref[slot] = jnp.where(inside, 0.0, FAR)


def mask_bias(lengths, base, slots, slot_rows):
    smem = pl.BlockSpec(memory_space=pltpu.SMEM)
    return pl.pallas_call(
        mask_kernel,
        in_specs=[smem, smem],
        out_shape=shape_of((slots, slot_rows, slot_rows), WIDE),
        compiler_params=params(),
        name="mask_bias",
    )(base, lengths)


def attention_forward_kernel(x_ref, b_ref, bias_ref, *refs, blocks, aliased, tile):
    sources = refs[:blocks]
    mixed_ref, p_ref, s_ref, w_ref, sems = refs[blocks + 2 * aliased :]
    rows, part = x_ref.shape[0], w_ref.shape[1] // 3
    slot, block = pl.program_id(0), pl.program_id(1)
    copies = [pltpu.make_async_copy(w, w_ref.at[b], sems.at[b]) for b, w in enumerate(sources)]

    @pl.when((slot == 0) & (block == 0))
    def _():
        for copy in copies:
            copy.start()

    for b, copy in enumerate(copies):

        @pl.when((slot == 0) & (block == b))
        def _():
            copy.wait()

    x = x_ref[...]
    q = ((dot_nt(x, w_ref[block, :part]) + b_ref[0]).astype(LOW) * HD**-0.5).astype(LOW)
    k = dot_nt(x, w_ref[block, part : 2 * part]).astype(LOW)
    v = (dot_nt(x, w_ref[block, 2 * part :]) + b_ref[1]).astype(LOW)
    mixed_ref[0] = q
    mixed_ref[1] = k
    mixed_ref[2] = v
    total = None
    for head, mask in enumerate(head_masks(part)):
        s_ref[head] = dot_nt(pick(mask, q), k)
        for start in range(0, rows, tile):
            at = slice(start, start + tile)
            s = s_ref[head, at] + bias_ref[at]
            e = jnp.exp(s - jnp.max(s, axis=1, keepdims=True))
            p_ref[head, at] = (e * (1.0 / jnp.sum(e, axis=1, keepdims=True))).astype(LOW)
        made = dot_nn(p_ref[head], pick(mask, v))
        total = made if total is None else total + made
    mixed_ref[3] = total.astype(LOW)


def attention_forward(x, sources, qv_bias, bias, first, before, tile=64):
    rows, width = x.shape
    slots, slot_rows, _ = bias.shape
    blocks = len(sources)
    part = sources[0].shape[0] // 3
    heads = part // HD
    aliased = int(before is not None)
    mixed = shape_of((4, 4, rows, part), LOW)
    probs = shape_of((4, slots, heads, slot_rows, slot_rows), LOW)
    return call(
        functools.partial(attention_forward_kernel, blocks=blocks, aliased=aliased, tile=tile),
        "attention_forward",
        (slots, blocks),
        [
            pl.BlockSpec((slot_rows, width), lambda s, b: (s, 0)),
            pl.BlockSpec((None, 2, 1, part), lambda s, b: (b, 0, 0, 0)),
            pl.BlockSpec((None, slot_rows, slot_rows), lambda s, b: (s, 0, 0)),
        ]
        + [in_place()] * (blocks + 2 * aliased),
        [
            pl.BlockSpec((None, 4, slot_rows, part), lambda s, b: (first + b, 0, s, 0)),
            pl.BlockSpec(
                (None, None, heads, slot_rows, slot_rows), lambda s, b: (first + b, s, 0, 0, 0)
            ),
        ],
        [mixed, probs],
        [
            pltpu.VMEM((heads, slot_rows, slot_rows), WIDE),
            pltpu.VMEM((blocks, 3 * part, width), LOW),
            pltpu.SemaphoreType.DMA((blocks,)),
        ],
        [],
        [x, qv_bias, bias, *sources, *(before or ())],
        alias={3 + blocks: 0, 4 + blocks: 1} if aliased else None,
        flops=blocks * (6 * rows * width * part + 8 * heads * rows * slot_rows * 256),
    )


def row_tiles(rows, tile):
    return [pl.ds(start, tile) for start in range(0, rows, tile)]


def ffn_forward_kernel(own_ref, mixed_hbm, x_hbm, wo_hbm, wu_ref, wd_ref, bu_ref, small_ref,
                       u1_hbm, hr_hbm, gr_hbm, gp_hbm, u2_hbm, low_hbm,
                       o_ref, x_ref, wo_ref, u1_ref, hr_ref, gr_ref, gp_ref, u2_ref, low_ref, in_sems, out_sems, g_sems,
                       *, layer, tile, renorm):
    step, steps = pl.program_id(0), pl.num_programs(0)
    part = o_ref.shape[2]
    tiles = row_tiles(x_ref.shape[0], tile)
    wo_copy = pltpu.make_async_copy(wo_hbm.at[layer], wo_ref, in_sems.at[0, 0])
    loads, first_out, last_out = [], [], []
    for t, at in enumerate(tiles):
        loads.append(
            [
                pltpu.make_async_copy(mixed_hbm.at[:, 3, at], o_ref.at[:, at], in_sems.at[1, t]),
                pltpu.make_async_copy(x_hbm.at[at], x_ref.at[at], in_sems.at[2, t]),
            ]
        )
        first_out.append(
            [
                pltpu.make_async_copy(u1_ref.at[at], u1_hbm.at[at], out_sems.at[0, t]),
                pltpu.make_async_copy(hr_ref.at[at], hr_hbm.at[at], out_sems.at[1, t]),
            ]
        )
        last_out.append(
            [
                pltpu.make_async_copy(u2_ref.at[at], u2_hbm.at[at], out_sems.at[2, t]),
                pltpu.make_async_copy(low_ref.at[at], low_hbm.at[at], out_sems.at[3, t]),
            ]
        )

    def g_out(chunk, slot):
        return [
            pltpu.make_async_copy(gr_ref.at[slot], gr_hbm.at[chunk], g_sems.at[0, slot]),
            pltpu.make_async_copy(gp_ref.at[slot], gp_hbm.at[chunk], g_sems.at[1, slot]),
        ]

    @pl.when(step == 0)
    def _():
        wo_copy.start()
        for pair in loads:
            for copy in pair:
                copy.start()
        wo_copy.wait()
        for t, at in enumerate(tiles):
            for copy in loads[t]:
                copy.wait()
            residual = x_ref[at].astype(WIDE)
            if renorm:
                residual = row_stats(residual)[0] * small_ref[6:7] + small_ref[7:8]
            u1 = residual + small_ref[0:1]
            for block in range(4):
                rows = pl.ds(pl.multiple_of((own_ref[0] ^ block) * part, 16), part)
                u1 = u1 + dot_nn(o_ref[block, at], wo_ref[rows, :])
            u1_ref[at] = u1
            normed = row_stats(u1)[0] * small_ref[1:2] + small_ref[2:3]
            hr_ref[at] = normed.astype(LOW)
            u2_ref[at] = normed + small_ref[3:4]
            for copy in first_out[t]:
                copy.start()

    slot = step % 2

    @pl.when(step >= 2)
    def _():
        for copy in g_out(step - 2, slot):
            copy.wait()

    z = dot_nn(hr_ref[...], wu_ref[...]) + bu_ref[...]
    g, slope = gelu_pair(z)
    gr = g.astype(LOW)
    gr_ref[slot] = gr
    gp_ref[slot] = slope.astype(LOW)
    for copy in g_out(step, slot):
        copy.start()
    u2_ref[...] += dot_nn(gr, wd_ref[...])

    @pl.when(step == steps - 1)
    def _():
        for t, at in enumerate(tiles):
            total = u2_ref[at]
            low_ref[at] = (row_stats(total)[0] * small_ref[4:5] + small_ref[5:6]).astype(LOW)
            for copy in last_out[t]:
                copy.start()
        for copy in [*g_out(step - 1, 1 - slot), *g_out(step, slot)]:
            copy.wait()
        for pair in first_out + last_out:
            for copy in pair:
                copy.wait()


def ffn_forward(own, mixed, x, wo, wu, wd, bu, small, layer, renorm, tile=512):
    _, _, rows, part = mixed.shape
    width, hidden = wu.shape[1:]
    chunks = hidden // width
    fixed = lambda v: pl.BlockSpec(v.shape, lambda i, o: (0,) * v.ndim)
    sems = lambda *shape: pltpu.SemaphoreType.DMA(shape)
    return call(
        functools.partial(ffn_forward_kernel, layer=layer, tile=tile, renorm=renorm),
        "ffn_forward",
        (chunks,),
        [
            in_place(),
            in_place(),
            in_place(),
            pl.BlockSpec((None, width, width), lambda i, o: (layer, 0, i)),
            pl.BlockSpec((None, width, width), lambda i, o: (layer, i, 0)),
            pl.BlockSpec((None, 1, width), lambda i, o: (i, 0, 0)),
            fixed(small),
        ],
        [in_place()] * 6,
        [
            shape_of((rows, width), WIDE),
            shape_of((rows, width), LOW),
            shape_of((chunks, rows, width), LOW),
            shape_of((chunks, rows, width), LOW),
            shape_of((rows, width), WIDE),
            shape_of((rows, width), LOW),
        ],
        [
            pltpu.VMEM((4, rows, part), LOW),
            pltpu.VMEM((rows, width), x.dtype),
            pltpu.VMEM((width, width), LOW),
            pltpu.VMEM((rows, width), WIDE),
            pltpu.VMEM((rows, width), LOW),
            pltpu.VMEM((2, rows, width), LOW),
            pltpu.VMEM((2, rows, width), LOW),
            pltpu.VMEM((rows, width), WIDE),
            pltpu.VMEM((rows, width), LOW),
            sems(3, rows // tile),
            sems(4, rows // tile),
            sems(2, 2),
        ],
        [own],
        [mixed, x, wo, wu, wd, bu, small],
        flops=6 * rows * width * (width + 2 * hidden),
    )


def reversed_bits(value, count):
    made = 0
    for bit in range(count):
        made = made | (((value >> bit) & 1) << (count - 1 - bit))
    return made


def each_chunk(made, dp_count):
    rows = made.shape[0] // dp_count
    for dp in range(dp_count):
        yield dp, made[dp * rows : (dp + 1) * rows]


def place(dp, own_dp, dp_count):
    away = dp ^ own_dp
    return away & 1, reversed_bits(away >> 1, dp_count.bit_length() - 2)


def ffn_backward_kernel(own_ref, gx_hbm, u2_hbm, u1_hbm, gp_hbm, hr_hbm, gr_hbm, wo_hbm, wu_ref, wd_ref, gain_ref,
                        da_hbm, do_hbm, du_hbm, sums_ref, zsum_ref, send_ref, keep_ref,
                        gx_ref, u2_ref, u1_ref, gp_ref, hr_ref, gr_ref, wo_ref, acc_ref, df_ref, dz_ref, da_ref, do_ref,
                        in_sems, out_sems, g_sems, *, layer, tile, dp_count):
    step, steps = pl.program_id(0), pl.num_programs(0)
    own, own_dp = own_ref[0], own_ref[1]
    part = do_ref.shape[2]
    tiles = row_tiles(gx_ref.shape[0], tile)
    count = len(tiles)
    loads, last_out = [], []
    for t, at in enumerate(tiles):
        loads.append(
            [
                pltpu.make_async_copy(gx_hbm.at[at], gx_ref.at[at], in_sems.at[0, t]),
                pltpu.make_async_copy(u2_hbm.at[at], u2_ref.at[at], in_sems.at[1, t]),
            ]
        )
        last_out.append(
            [
                pltpu.make_async_copy(u2_ref.at[at], du_hbm.at[at], out_sems.at[0, t]),
                pltpu.make_async_copy(da_ref.at[:, at], da_hbm.at[:, at], out_sems.at[1, t]),
                pltpu.make_async_copy(do_ref.at[:, at], do_hbm.at[:, at], out_sems.at[2, t]),
            ]
        )
    hr_copy = pltpu.make_async_copy(hr_hbm, hr_ref, in_sems.at[2, 0])
    u1_copy = pltpu.make_async_copy(u1_hbm, u1_ref, in_sems.at[2, 1])
    wo_copy = pltpu.make_async_copy(wo_hbm.at[layer], wo_ref, in_sems.at[2, 2])

    def streams(at_step):
        slot, head = at_step % 2, own ^ head_order(at_step)
        return (
            pltpu.make_async_copy(gp_hbm.at[head], gp_ref.at[slot], g_sems.at[0, slot]),
            pltpu.make_async_copy(gr_hbm.at[head], gr_ref.at[slot], g_sems.at[1, slot]),
        )

    slot = step % 2
    gp_copy, gr_copy = streams(step)

    @pl.when(step == 0)
    def _():
        for pair in loads:
            for copy in pair:
                copy.start()

        gp_copy.start()
        hr_copy.start()
        gr_copy.start()

    @pl.when(step < steps - 1)
    def _():
        for copy in streams(step + 1):
            copy.start()

    @pl.when(step == 1)
    def _():
        u1_copy.start()
        wo_copy.start()

    @pl.when(step == 0)
    def _():
        sums_ref[...] = jnp.zeros_like(sums_ref)
        for t, at in enumerate(tiles):
            for copy in loads[t]:
                copy.wait()
            gx = gx_ref[at].astype(WIDE)
            xhat, inverse = row_stats(u2_ref[at])
            sums_ref[0:1] += column_sum(gx * xhat)
            sums_ref[1:2] += column_sum(gx)
            gv = norm_backward(gx, xhat, inverse, gain_ref[1:2])
            df = gv.astype(LOW)
            df_ref[at] = df
            sums_ref[2:3] += column_sum(df.astype(WIDE))
            acc_ref[at] = gv

    dg = dot_nt(df_ref[...], wd_ref[...])
    gp_copy.wait()
    dz = (dg * gp_ref[slot].astype(WIDE)).astype(LOW)
    dz_ref[...] = dz
    zsum_ref[...] = column_sum(dz.astype(WIDE))
    acc_ref[...] += dot_nt(dz_ref[...], wu_ref[...])

    @pl.when(step == 0)
    def _():
        hr_copy.wait()

    up = dot_tn(hr_ref[...], dz_ref[...]).astype(LOW)
    gr_copy.wait()
    down = dot_tn(df_ref[...], gr_ref[slot]).astype(LOW)
    for out, wanted in ((send_ref, step < 2), (keep_ref, step >= 2)):

        @pl.when(wanted)
        def _():
            for which, made in enumerate((up, down)):
                for dp, chunk in each_chunk(made, dp_count):
                    out[(which, *place(dp, own_dp, dp_count))] = chunk

    @pl.when(step == steps - 1)
    def _():
        u1_copy.wait()
        wo_copy.wait()
        for t, at in enumerate(tiles):
            total = acc_ref[at]
            xhat, inverse = row_stats(u1_ref[at])
            sums_ref[3:4] += column_sum(total * xhat)
            sums_ref[4:5] += column_sum(total)
            du = norm_backward(total, xhat, inverse, gain_ref[0:1])
            u2_ref[at] = du
            da = du.astype(LOW)
            for block in range(4):
                da_ref[block, at] = da[:, block * part : (block + 1) * part]
            sums_ref[5:6] += column_sum(da.astype(WIDE))
            for block in range(4):
                rows = pl.ds(pl.multiple_of((own ^ block) * part, 16), part)
                do_ref[block, at] = dot_nt(da, wo_ref[rows, :]).astype(LOW)
            for copy in last_out[t]:
                copy.start()
        for several in last_out:
            for copy in several:
                copy.wait()


def head_order(step):
    return jnp.where(step < 2, 1 + 2 * step, 2 * (step - 2))


def ffn_backward(own, gx, u2, u1, gp, hr, gr, wo, wu, wd, gains, layer, dp_count, tile=512):
    rows, width = gx.shape
    chunks = gp.shape[0]
    part = width // 4
    chunk_rows = width // dp_count
    rest = dp_count // 2
    fixed = lambda s: pl.BlockSpec(s.shape, lambda i, o: (0,) * len(s.shape))
    head = lambda i, o: o[0] ^ head_order(i)
    block = (2, None, 2, rest, chunk_rows, width)
    sums = shape_of((8, width), WIDE)
    grads = stored((2, 2, 2, rest, chunk_rows, width), LOW)
    sems = lambda *shape: pltpu.SemaphoreType.DMA(shape)
    low = lambda *shape: pltpu.VMEM(shape, LOW)
    wide = lambda *shape: pltpu.VMEM(shape, WIDE)
    return call(
        functools.partial(ffn_backward_kernel, layer=layer, tile=tile, dp_count=dp_count),
        "ffn_backward",
        (chunks,),
        [in_place()] * 7
        + [
            pl.BlockSpec((None, width, width), lambda i, o: (layer, 0, head(i, o))),
            pl.BlockSpec((None, width, width), lambda i, o: (layer, head(i, o), 0)),
            fixed(gains),
        ],
        [
            in_place(),
            in_place(),
            in_place(),
            fixed(sums),
            pl.BlockSpec((None, 1, width), lambda i, o: (head(i, o), 0, 0)),
            pl.BlockSpec(block, lambda i, o: (0, jnp.minimum(i, 1), 0, 0, 0, 0)),
            pl.BlockSpec(block, lambda i, o: (0, jnp.maximum(i - 2, 0), 0, 0, 0, 0)),
        ],
        [
            shape_of((4, rows, part), LOW),
            shape_of((4, rows, part), LOW),
            shape_of((rows, width), WIDE),
            sums,
            shape_of((chunks, 1, width), WIDE),
            grads,
            grads,
        ],
        [
            pltpu.VMEM((rows, width), gx.dtype),
            wide(rows, width),
            wide(rows, width),
            low(2, rows, width),
            low(rows, width),
            low(2, rows, width),
            low(width, width),
            wide(rows, width),
            low(rows, width),
            low(rows, width),
            low(4, rows, part),
            low(4, rows, part),
            sems(3, max(rows // tile, 3)),
            sems(3, rows // tile),
            sems(2, 2),
        ],
        [own],
        [gx, u2, u1, gp, hr, gr, wo, wu, wd, gains],
        flops=4 * rows * width * (width + 4 * chunks * width),
    )


def split_rows(made, got_ref, own_dp, dp_count, send_ref, keep_ref):
    for dp, chunk in each_chunk(made, dp_count):
        away, rest = place(dp, own_dp, dp_count)
        summed = (chunk + got_ref[away, rest].astype(WIDE)).astype(LOW)

        @pl.when(away == 1)
        def _():
            send_ref[rest] = summed

        @pl.when(away == 0)
        def _():
            keep_ref[rest] = summed


def add_rows(made, got_ref, own_dp, dp_count, out_ref):
    for dp, chunk in each_chunk(made, dp_count):
        at = place(dp, own_dp, dp_count)
        out_ref[at] = (chunk + got_ref[at].astype(WIDE)).astype(LOW)


def core_add_kernel(kept_ref, got_ref, up_send, up_keep, down_send, down_keep):
    step = pl.program_id(0)

    which, away = step // 2, jnp.where(step < 2, step, 3 - step)

    def summed(at):
        return (kept_ref[at].astype(WIDE) + got_ref[which, away, at].astype(WIDE)).astype(LOW)

    @pl.when(step < 2)
    def _():
        up_keep[...] = summed(0)
        up_send[...] = summed(1)

    for out, wanted in ((down_send, 2), (down_keep, 3)):

        @pl.when(step == wanted)
        def _():
            out[0] = summed(0)
            out[1] = summed(1)


def core_add(kept, got):
    _, _, _, rest, chunk_rows, width = kept.shape

    def at(i):
        return (i // 2, jnp.where(i < 2, i, 3 - i), 0, 0, 0, 0)

    block = pl.BlockSpec((None, None, 2, rest, chunk_rows, width), at)
    up = pl.BlockSpec((None, rest, chunk_rows, width), lambda i: (jnp.minimum(i, 1), 0, 0, 0))
    down = pl.BlockSpec((2, rest, chunk_rows, width), lambda i: (0, 0, 0, 0))
    made = stored((2, rest, chunk_rows, width), LOW)
    return call(
        core_add_kernel,
        "core_add",
        (4,),
        [block, pl.BlockSpec(memory_space=pltpu.VMEM)],
        [up, up, down, down],
        [made] * 4,
        [],
        [],
        [kept, got],
        vmem=24 << 20,
    )


def attention_backward_kernel(own_ref, mixed_ref, do_ref, p_ref, x_ref, o_ref, da_ref, wa_ref, wb_ref, gx_ref, *refs,
                              dp_count, tile, keep):
    if keep:
        got_ref, *refs = refs
    out_ref, sums_ref, *refs = refs
    grads = refs[: 4 if keep else 1]
    t_ref, ds_ref, parts_ref, xt_ref, ot_ref, acc_ref = refs[4 if keep else 1 :]
    slot, block = pl.program_id(0), pl.program_id(1)
    last = pl.num_programs(0) - 1
    own, own_dp = own_ref[0], own_ref[1]
    rows, part = mixed_ref.shape[1:]

    @pl.when((slot == 0) & (block == 0))
    def _():
        xt_ref[...] = x_ref[...].T
        for r in range(4):
            ot_ref[pl.ds(pl.multiple_of((own ^ r) * part, 16), part), :] = o_ref[r].T
        sums_ref[...] = jnp.zeros_like(sums_ref)

    dq = dk = dv = None
    for head, mask in enumerate(head_masks(part)):
        do = pick(mask, do_ref[...])
        t_ref[head] = dot_nt(do, mixed_ref[2])
        for start in range(0, rows, tile):
            at = slice(start, start + tile)
            p = p_ref[head, at].astype(WIDE)
            dp = t_ref[head, at]
            share = jnp.sum(p * dp, axis=1, keepdims=True)
            ds_ref[head, at] = (p * (dp - share)).astype(LOW)
        made = (
            dot_nn(ds_ref[head], pick(mask, mixed_ref[1])),
            dot_tn(ds_ref[head], pick(mask, mixed_ref[0])),
            dot_tn(p_ref[head], do),
        )
        dq, dk, dv = made if dq is None else (dq + made[0], dk + made[1], dv + made[2])
    dq = (dq * HD**-0.5).astype(LOW)
    dk = dk.astype(LOW)
    dv = dv.astype(LOW)
    sums_ref[block, 0:1] += column_sum(dq.astype(WIDE))
    sums_ref[block, 1:2] += column_sum(dv.astype(WIDE))
    joined = jnp.concatenate([dq, dk, dv], axis=1)
    parts_ref[block, pl.ds(pl.multiple_of(slot * rows, rows), rows), :] = joined
    weights = jnp.where(block == 0, wa_ref[...], wb_ref[...])
    passed = dot_nn(joined, weights)

    @pl.when(block == 0)
    def _():
        acc_ref[...] = gx_ref[...] + passed

    @pl.when(block == 1)
    def _():
        out_ref[...] = (acc_ref[...] + passed).astype(out_ref.dtype)

    @pl.when(slot == last)
    def _():
        first = dot_nn(xt_ref[...], parts_ref[block])
        second = dot_nn(ot_ref[...], da_ref[...])
        made = jnp.concatenate([first, second], axis=1)
        if not keep:
            for dp, chunk in each_chunk(made.astype(LOW), dp_count):
                grads[0][place(dp, own_dp, dp_count)] = chunk
            return
        half = made.shape[1] // 2
        a_send, a_keep, b_send, b_keep = grads
        got = [got_ref.at[:, :, :, :half], got_ref.at[:, :, :, half:]]
        for where_to, wanted in ((a_keep, 0), (a_send, 1)):

            @pl.when(block == wanted)
            def _():
                add_rows(made[:, :half], got[0], own_dp, dp_count, where_to)

        split_rows(made[:, half:], got[1], own_dp, dp_count, b_send, b_keep)


def attention_backward(own, mixed, do, probs, x, da, wa, wb, gx, got, dp_count, out_type, tile=64):
    rows, width = x.shape
    part = mixed.shape[3]
    _, slots, heads, slot_rows, _ = probs.shape
    chunk_rows, rest = width // dp_count, dp_count // 2
    keep = got is not None
    away = 0 if keep else 1
    block_of = lambda b: 2 * b + away
    row = pl.BlockSpec((slot_rows, width), lambda s, b, o: (s, 0))
    last = slots - 1
    late = lambda s, b: jnp.where(s == last, b, 0)
    in_specs = [
        pl.BlockSpec((None, 3, slot_rows, part), lambda s, b, o: (block_of(b), 0, s, 0)),
        pl.BlockSpec((None, slot_rows, part), lambda s, b, o: (block_of(b), s, 0)),
        pl.BlockSpec(
            (None, None, heads, slot_rows, slot_rows), lambda s, b, o: (block_of(b), s, 0, 0, 0)
        ),
        whole(x),
        pl.BlockSpec((4, None, rows, part), lambda s, b, o: (0, 3, 0, 0), pipeline_mode=pl.Buffered(1)),
        pl.BlockSpec((None, rows, part), lambda s, b, o: (o[0] ^ block_of(late(s, b)), 0, 0)),
        whole(wa),
        whole(wb),
        row,
    ]
    operands = [mixed, do, probs, x, mixed, da, wa, wb, gx]
    sums = shape_of((2, 8, part), WIDE)
    out_specs = [row, pl.BlockSpec(sums.shape, lambda s, b, o: (0, 0, 0))]
    out_shape = [shape_of((rows, width), out_type), sums]
    whole_block = lambda w: pl.BlockSpec((2, rest, chunk_rows, w), lambda s, b, o: (0, 0, 0, 0))
    if keep:
        in_specs.append(
            pl.BlockSpec(
                (None, 2, rest, chunk_rows, width), lambda s, b, o: (late(s, b), 0, 0, 0, 0)
            )
        )
        operands.append(got)
        half = width // 2
        b_block = pl.BlockSpec(
            (None, rest, chunk_rows, half), lambda s, b, o: (late(s, b), 0, 0, 0)
        )
        out_specs += [whole_block(half)] * 2 + [b_block] * 2
        out_shape += [stored((2, rest, chunk_rows, half), LOW)] * 4
    else:
        out_specs.append(
            pl.BlockSpec(
                (None, 2, rest, chunk_rows, width), lambda s, b, o: (late(s, b), 0, 0, 0, 0)
            )
        )
        out_shape.append(stored((2, 2, rest, chunk_rows, width), LOW))
    return call(
        functools.partial(attention_backward_kernel, dp_count=dp_count, tile=tile, keep=keep),
        "attention_backward",
        (slots, 2),
        in_specs,
        out_specs,
        out_shape,
        [
            pltpu.VMEM((heads, slot_rows, slot_rows), WIDE),
            pltpu.VMEM((heads, slot_rows, slot_rows), LOW),
            pltpu.VMEM((2, rows, 3 * part), LOW),
            pltpu.VMEM((width, rows), LOW),
            pltpu.VMEM((width, rows), LOW),
            pltpu.VMEM((slot_rows, width), WIDE),
        ],
        [own],
        operands,
        flops=36 * heads * rows * slot_rows * 256,
    )


def bits_of(axis):
    size = lax.axis_size(axis)
    return [1 << bit for bit in range(size.bit_length() - 1)]


def swap(value, axis, bit):
    size = lax.axis_size(axis)
    return lax.ppermute(value, axis, [(i, i ^ bit) for i in range(size)])


def add_split_kernel(*refs, merge_in, merge_out, extra):
    inputs = 2 if merge_in else 4
    outputs = 2 if merge_out else 4
    ins, refs = refs[:inputs], refs[extra:]
    outs = refs[inputs : inputs + outputs]
    kept_ref, send_ref, keep_ref, in_sems, out_sems = refs[inputs + outputs :]
    half = send_ref.shape[1]
    loads, got, stores = [], [], []
    for part in range(2):
        kept, came = (ins[0].at[part], ins[1].at[part]) if merge_in else ins[2 * part : 2 * part + 2]
        send, keep = (
            (outs[0].at[part], outs[1].at[part]) if merge_out else outs[2 * part : 2 * part + 2]
        )
        got.append(came)
        loads.append(pltpu.make_async_copy(kept, kept_ref.at[part], in_sems.at[part]))
        stores.append(
            [
                pltpu.make_async_copy(send_ref.at[part], send, out_sems.at[part, 0]),
                pltpu.make_async_copy(keep_ref.at[part], keep, out_sems.at[part, 1]),
            ]
        )
    for copy in loads:
        copy.start()
    for part in range(2):
        loads[part].wait()
        for at, (out, copy) in enumerate(zip((send_ref, keep_ref), stores[part])):
            rows = pl.ds(half * (1 - at), half)
            out[part] = (kept_ref[part, rows].astype(WIDE) + got[part][rows].astype(WIDE)).astype(LOW)
            copy.start()
    for copies in stores:
        for copy in copies:
            copy.wait()


def add_split(ins, merge_in, merge_out, arrived):
    size, rows, columns = ins[0].shape[-3:]
    half = (size // 2, rows, columns)
    out_shape = [stored((2, *half), LOW)] * 2 if merge_out else [stored(half, LOW)] * 4
    return pl.pallas_call(
        functools.partial(
            add_split_kernel, merge_in=merge_in, merge_out=merge_out, extra=len(arrived)
        ),
        in_specs=[in_hbm(), pl.BlockSpec(memory_space=pltpu.VMEM)] * (len(ins) // 2)
        + [in_place()] * len(arrived),
        out_specs=[in_hbm()] * len(out_shape),
        out_shape=out_shape,
        scratch_shapes=[
            pltpu.VMEM((2, size, rows, columns), LOW),
            pltpu.VMEM((2, *half), LOW),
            pltpu.VMEM((2, *half), LOW),
            pltpu.SemaphoreType.DMA((2,)),
            pltpu.SemaphoreType.DMA((2, 2)),
        ],
        compiler_params=pltpu.CompilerParams(vmem_limit_bytes=16 << 20),
        cost_estimate=pl.CostEstimate(flops=0, bytes_accessed=0, transcendentals=0),
        name="add_split",
    )(*ins, *arrived)


class Summing:
    def __init__(self, a_send, a_keep, b_send, b_keep):
        head, dp = bits_of("head"), bits_of("dp")
        self.stages = [(("dp", dp[0]), ("head", head[1]))] + [(("dp", bit),) for bit in dp[1:]]
        self.at = 0
        self.settled = False
        self.kept = [a_keep, b_keep]
        self.got = [swap(a_send, "head", head[1]), swap(b_send, "dp", dp[0])]

    def busy(self):
        return self.at < len(self.stages)

    def step(self, after, arrived=()):
        stage = self.stages[self.at]
        merge_in, merge_out = len(self.kept) == 1, len(stage) == 1
        ins = [v for pair in zip(self.kept, self.got) for v in pair]
        lead = 1 if merge_in else 0
        ins = [v.reshape(*v.shape[:lead], -1, *v.shape[-2:]) for v in ins]
        ins, _ = lax.optimization_barrier((ins, after))
        outs = add_split(ins, merge_in, merge_out, arrived)
        if merge_out:
            self.got, self.kept = [swap(outs[0], *stage[0])], [outs[1]]
        else:
            self.got = [swap(outs[0], *stage[0]), swap(outs[2], *stage[1])]
            self.kept = [outs[1], outs[3]]
        self.at += 1
        return outs[-1]


def last_sums_kernel(*refs, layers):
    ins, outs = refs[: 4 * layers + 2], refs[4 * layers + 2 :]
    qkv, qv, out_w, out_b, gain1, shift1, up_w, up_b, down_w, down_b, gain2, shift2 = outs
    part = out_w.shape[2]
    width = down_b.shape[1]
    rows = ins[-2][...] + ins[-1][...]
    for layer in range(layers):
        ffn_kept, ffn_got, wide_kept, wide_got = ins[4 * layer : 4 * layer + 4]
        down_w[layer] = ffn_kept[0, 0].astype(WIDE) + ffn_got[0, 0].astype(WIDE)
        up_w[layer] = ffn_kept[1, 0].astype(WIDE) + ffn_got[1, 0].astype(WIDE)
        for half in range(2):
            both = wide_kept[half, 0].astype(WIDE) + wide_got[half, 0].astype(WIDE)
            for at in range(2):
                which = 2 * half + at
                block = both[:, at * part : (at + 1) * part]
                if which < 3:
                    qkv[layer, which] = block
                else:
                    out_w[layer] = block
        for row, out in enumerate((gain2, shift2, down_b, gain1, shift1, out_b)):
            out[layer : layer + 1] = rows[layer, row : row + 1]
        qv[layer] = rows[layer, 6:8]
        for row in range(up_b.shape[1] // width):
            at = slice(row * width, (row + 1) * width)
            up_b[layer : layer + 1, at] = rows[layer, 8 + row : 9 + row]


def last_sums(groups, small, passing):
    layers, _, width = small.shape
    ins, specs = [], []
    for group in groups:
        ins += [group.kept[0], group.got[0]]
    ins = [v.reshape(2, 1, *v.shape[-2:]) for v in ins] + [small, passing]
    rows, part = ins[0].shape[2], ins[2].shape[3] // 2
    hidden = (small.shape[1] - 8) * width
    shapes = [
        (layers, 3, rows, part),
        (layers, 2, width),
        (layers, rows, part),
        (layers, width),
        (layers, width),
        (layers, width),
        (layers, rows, width),
        (layers, hidden),
        (layers, rows, width),
        (layers, width),
        (layers, width),
        (layers, width),
    ]
    spec = lambda shape: pl.BlockSpec(shape, lambda i: (0,) * len(shape))
    specs = [spec(v.shape) for v in ins]
    return call(
        functools.partial(last_sums_kernel, layers=layers),
        "last_sums",
        (1,),
        specs,
        [spec(shape) for shape in shapes],
        [shape_of(shape, WIDE) for shape in shapes],
        [],
        [],
        ins,
        vmem=24 << 20,
    )


def ordered(after, *values):
    values, _ = lax.optimization_barrier((values, after))
    return values


def near_blocks(block, after):
    low, high = bits_of("head")
    near = swap(block, "head", low)
    (later,) = ordered((after, near), block)
    return block, near, swap(later, "head", high)


def gathered_pairs(block, after):
    own, near, far = near_blocks(block, after)
    return jnp.stack([own, near]), jnp.stack([far, swap(far, "head", bits_of("head")[0])])


def on_device(
    tokens,
    seq_lengths,
    qkv_weight,
    qv_bias,
    out_weight,
    out_bias,
    norm1_gain,
    norm1_shift,
    up_weight,
    up_bias,
    down_weight,
    down_bias,
    norm2_gain,
    norm2_shift,
    out_grad,
):
    head_count, dp_count = lax.axis_size("head"), lax.axis_size("dp")
    head_index, dp_index = lax.axis_index("head"), lax.axis_index("dp")
    own = jnp.stack([head_index, dp_index]).astype(jnp.int32)
    local_rows, width = tokens.shape
    slot_rows = local_rows * head_count // seq_lengths.shape[0]
    slots = local_rows // slot_rows
    layers = qkv_weight.shape[0]
    part = width // head_count
    turned = jnp.swapaxes(qkv_weight, 2, 3).reshape(layers, 3 * part, width)
    base = (head_index * slots).astype(jnp.int32).reshape(1)
    bias = mask_bias(seq_lengths, base, slots, slot_rows)
    weights = [near_blocks(turned[0], base)]
    near_bias, far_bias = gathered_pairs(qv_bias[:, :, None], base)
    up_rows = up_bias.reshape(layers, -1, 1, width)
    rounded, residual = tokens, tokens
    kept = []
    for layer in range(layers):
        before = max(layer - 1, 0)
        small = jnp.stack(
            [
                out_bias[layer],
                norm1_gain[layer],
                norm1_shift[layer],
                down_bias[layer],
                norm2_gain[layer],
                norm2_shift[layer],
                norm2_gain[before],
                norm2_shift[before],
            ]
        )
        own_w, near_w, far_w = weights[layer]
        if layer == 0:
            near = attention_forward(rounded, (own_w, near_w), near_bias[:, layer], bias, 0, None)
            (far_w, far_b) = ordered(near[0], far_w, far_bias[:, layer])
            both_w = swap(far_w, "head", bits_of("head")[0])
            for other in range(1, layers):
                (later,) = ordered(near[0], turned[other])
                weights.append(near_blocks(later, near[0]))
            mixed, probs = attention_forward(rounded, (far_w, both_w), far_b, bias, 2, near)
            (far_ws,) = ordered(mixed, [w[2] for w in weights[1:]])
            both_ws = [swap(w, "head", bits_of("head")[0]) for w in far_ws]
        else:
            both_w = both_ws[layer - 1]
            all_bias = jnp.concatenate([near_bias[:, layer], far_bias[:, layer]])
            mixed, probs = attention_forward(
                rounded, (own_w, near_w, far_w, both_w), all_bias, bias, 0, None
            )
        weights[layer] = w = (own_w, near_w, far_w, both_w)
        u1, hr, gr, slope, u2, low = ffn_forward(
            own,
            mixed,
            residual,
            out_weight,
            up_weight,
            down_weight,
            up_rows[layer],
            small,
            layer,
            layer > 0,
        )
        kept.append((rounded, mixed, probs, u1, hr, gr, slope, u2))
        rounded, residual = low, u2
    out_state = rounded
    grad_state = out_grad
    small_sums = [None] * layers
    hidden_sums = [None] * layers
    ffn_groups, wide_groups = [None] * layers, [None] * layers
    running = []

    def advance(after):
        arrived = []
        for group in running:
            if not group.busy() and not group.settled:
                arrived += group.got
                group.settled = True
        for group in running:
            if group.busy():
                after = group.step(after, arrived)
                arrived = []
        return after

    for layer in reversed(range(layers)):
        rounded, mixed, probs, u1, hr, gr, slope, u2 = kept[layer]
        w = weights[layer]
        gains = jnp.stack([norm1_gain[layer], norm2_gain[layer]])
        da, do, du, sums, zsums, sent, ffn_kept = ffn_backward(
            own,
            grad_state,
            u2,
            u1,
            slope,
            hr,
            gr,
            out_weight,
            up_weight,
            down_weight,
            gains,
            layer,
            dp_count,
        )
        low_bit = bits_of("head")[0]
        early = bool(running)
        token = advance(do)
        if early:
            (sent,) = ordered(token, sent)
        got = swap(sent, "head", low_bit)

        def sum_ffn(after):
            values = ordered(after, ffn_kept, got)
            up_send, up_keep, down_send, down_keep = core_add(*values)
            ffn_groups[layer] = Summing(down_send, down_keep, up_send, up_keep)
            running.insert(0, ffn_groups[layer])
            return down_keep

        if early:
            token = sum_ffn(token)
        (do, du) = ordered(token, do, du)
        half_grad, away_sums, sent = attention_backward(
            own, mixed, do, probs, rounded, da, w[1], w[3], du, None, dp_count, WIDE
        )
        if early:
            token = advance(half_grad)
            (sent,) = ordered(token, sent)
            wide_got = swap(sent, "head", low_bit)
        else:
            wide_got = swap(sent, "head", low_bit)
            token = sum_ffn(half_grad)
        (half_grad, do) = ordered(token, half_grad, do)
        grad_state, own_sums, *parts = attention_backward(
            own,
            mixed,
            do,
            probs,
            rounded,
            da,
            w[0],
            w[2],
            half_grad,
            wide_got,
            dp_count,
            WIDE if layer else LOW,
        )
        wide_groups[layer] = Summing(*parts)
        token = advance(grad_state) if layer else grad_state
        if layer:
            (grad_state,) = ordered(token, grad_state)
        running.append(wide_groups[layer])
        blocks = [own_sums[0], away_sums[0], own_sums[1], away_sums[1]]
        stacked = jnp.stack(blocks)[:, :2]
        qv_sums = jnp.concatenate(
            [
                lax.dynamic_index_in_dim(stacked, head_index ^ head, 0, keepdims=False)
                for head in range(head_count)
            ],
            axis=1,
        )
        small_sums[layer] = jnp.concatenate([sums[:6], qv_sums, zsums[:, 0]])
    small_sum = jnp.stack(small_sums)
    near, far = bits_of("head")
    waiting = [[("head", near)], [("dp", 1)], [("head", far)], [("dp", 2 * k) for k in range(1, dp_count // 2)]]
    passing = [swap(small_sum, *one) for one in waiting.pop(0)]
    while any(not group.settled for group in running) or waiting:
        if any(group.busy() for group in running):
            token = advance(token)
        elif not waiting:
            break
        if waiting:
            small_sum, passing = ordered(token, small_sum, passing)
            small_sum = sum(passing, small_sum)
            token = small_sum
            passing = [swap(small_sum, *one) for one in waiting.pop(0)]
    small_sum, passing = sum(passing[:-1], small_sum), passing[-1]
    groups = [group for pair in zip(ffn_groups, wide_groups) for group in pair]
    qkv, qv, out_w, out_b, gain1, shift1, up_w, up_b, down_w, down_b, gain2, shift2 = last_sums(
        groups, small_sum, passing
    )
    return (
        out_state,
        grad_state,
        qkv,
        qv,
        out_w,
        out_b,
        gain1,
        shift1,
        up_w,
        up_b,
        jnp.swapaxes(down_w, 1, 2),
        down_b,
        gain2,
        shift2,
    )


def solution(mesh):
    in_specs = (
        P(("dp", "head"), None),
        P("dp", None),
        P(None, None, None, "head"),
        P(None, None, "head"),
        P(),
        P(),
        P(),
        P(),
        P(),
        P(),
        P(),
        P(),
        P(),
        P(),
        P(("dp", "head"), None),
    )
    out_specs = (
        P(("dp", "head"), None),
        P(("dp", "head"), None),
        P(None, None, "dp", "head"),
        P(),
        P(None, "dp", "head"),
        P(),
        P(),
        P(),
        P(None, "dp", "head"),
        P(),
        P(None, "head", "dp"),
        P(),
        P(),
        P(),
    )
    return jax.shard_map(
        on_device, mesh=mesh, in_specs=in_specs, out_specs=out_specs, check_vma=False
    )
```

```python
import functools
import math

import jax
import jax.numpy as jnp
from jax import lax
from jax.experimental import pallas as pl
from jax.experimental.pallas import tpu as pltpu
from jax.sharding import PartitionSpec as P

HD = 64
EPSILON = 1e-06
LOW = jnp.bfloat16
WIDE = jnp.float32
VMEM_BYTES = 58 << 20
ROOT_HALF = 0.7071067811865476
INV_ROOT_TAU = 0.3989422804014327
FAR = -1e30


def row_stats(values):
    centre = jnp.mean(values, axis=-1, keepdims=True)
    centred = values - centre
    spread = jnp.mean(centred * centred, axis=-1, keepdims=True)
    inverse = lax.rsqrt(spread + EPSILON)
    return centred * inverse, inverse


def norm_backward(upstream, xhat, inverse, gain):
    scaled = upstream * gain
    first = jnp.mean(scaled, axis=-1, keepdims=True)
    second = jnp.mean(scaled * xhat, axis=-1, keepdims=True)
    return (scaled - first - xhat * second) * inverse


def column_sum(values):
    return jnp.sum(values, axis=0, keepdims=True)


def dot_nn(left, right):
    return jnp.dot(left, right, preferred_element_type=WIDE)


def dot_nt(left, right):
    return lax.dot_general(left, right, (((1,), (1,)), ((), ())), preferred_element_type=WIDE)


def dot_tn(left, right):
    return lax.dot_general(left, right, (((0,), (0,)), ((), ())), preferred_element_type=WIDE)


def gelu_pair(z):
    cdf = 0.5 + 0.5 * lax.erf(z * ROOT_HALF)
    return z * cdf, cdf + z * (jnp.exp(z * z * -0.5) * INV_ROOT_TAU)


def pick(mask, values):
    return jnp.where(mask, values, jnp.zeros_like(values))


def head_masks(width):
    lanes = lax.broadcasted_iota(jnp.int32, (1, width), 1) // HD
    return [lanes == head for head in range(width // HD)]


def params():
    return pltpu.CompilerParams(vmem_limit_bytes=VMEM_BYTES)


def whole(array):
    return pl.BlockSpec(array.shape, lambda *ids: (0,) * array.ndim, pipeline_mode=pl.Buffered(1))


def in_place():
    return pl.BlockSpec(memory_space=pl.ANY)


def in_hbm():
    return pl.BlockSpec(memory_space=pltpu.HBM)


def shape_of(shape, kind):
    return jax.ShapeDtypeStruct(shape, kind)


def cost(flops, out_shape, operands):
    if not flops:
        return pl.CostEstimate(flops=0, bytes_accessed=0, transcendentals=0)
    made = out_shape if isinstance(out_shape, (list, tuple)) else [out_shape]
    moved = sum(math.prod(v.shape) * jnp.dtype(v.dtype).itemsize for v in [*made, *operands])
    return pl.CostEstimate(flops=flops, bytes_accessed=moved, transcendentals=0)


def stored(shape, kind):
    return pltpu.HBM(shape, kind)


def call(kernel, name, grid, in_specs, out_specs, out_shape, scratch, scalars, operands, alias=None, flops=0, vmem=VMEM_BYTES):
    return pl.pallas_call(
        kernel,
        grid_spec=pltpu.PrefetchScalarGridSpec(
            num_scalar_prefetch=len(scalars),
            grid=grid,
            in_specs=in_specs,
            out_specs=out_specs,
            scratch_shapes=scratch,
        ),
        out_shape=out_shape,
        compiler_params=pltpu.CompilerParams(vmem_limit_bytes=vmem),
        input_output_aliases=alias or {},
        cost_estimate=cost(flops, out_shape, operands),
        name=name,
    )(*scalars, *operands)


def mask_kernel(base_ref, lengths_ref, bias_ref):
    slots, rows, _ = bias_ref.shape
    across = lax.broadcasted_iota(jnp.int32, (8, rows), 1)
    down = lax.broadcasted_iota(jnp.int32, (rows, 128), 0)
    for slot in range(slots):
        reach = jnp.int32(0)
        seg_across = jnp.zeros((8, rows), jnp.int32)
        seg_down = jnp.zeros((rows, 128), jnp.int32)
        for k in range(lengths_ref.shape[1]):
            reach = reach + lengths_ref[base_ref[0] + slot, k]
            seg_across += (across >= reach).astype(jnp.int32)
            seg_down += (down >= reach).astype(jnp.int32)
        inside = seg_down[:, 0:1] == seg_across[0:1, :]
        bias_ref[slot] = jnp.where(inside, 0.0, FAR)


def mask_bias(lengths, base, slots, slot_rows):
    smem = pl.BlockSpec(memory_space=pltpu.SMEM)
    return pl.pallas_call(
        mask_kernel,
        in_specs=[smem, smem],
        out_shape=shape_of((slots, slot_rows, slot_rows), WIDE),
        compiler_params=params(),
        name="mask_bias",
    )(base, lengths)


def attention_forward_kernel(x_ref, b_ref, bias_ref, *refs, blocks, aliased, tile):
    sources = refs[:blocks]
    mixed_ref, p_ref, s_ref, w_ref, sems = refs[blocks + 2 * aliased :]
    rows, part = x_ref.shape[0], w_ref.shape[1] // 3
    slot, block = pl.program_id(0), pl.program_id(1)
    copies = [pltpu.make_async_copy(w, w_ref.at[b], sems.at[b]) for b, w in enumerate(sources)]

    @pl.when((slot == 0) & (block == 0))
    def _():
        for copy in copies:
            copy.start()

    for b, copy in enumerate(copies):

        @pl.when((slot == 0) & (block == b))
        def _():
            copy.wait()

    x = x_ref[...]
    q = ((dot_nt(x, w_ref[block, :part]) + b_ref[0]).astype(LOW) * HD**-0.5).astype(LOW)
    k = dot_nt(x, w_ref[block, part : 2 * part]).astype(LOW)
    v = (dot_nt(x, w_ref[block, 2 * part :]) + b_ref[1]).astype(LOW)
    mixed_ref[0] = q
    mixed_ref[1] = k
    mixed_ref[2] = v
    total = None
    for head, mask in enumerate(head_masks(part)):
        s_ref[head] = dot_nt(pick(mask, q), k)
        for start in range(0, rows, tile):
            at = slice(start, start + tile)
            s = s_ref[head, at] + bias_ref[at]
            e = jnp.exp(s - jnp.max(s, axis=1, keepdims=True))
            p_ref[head, at] = (e * (1.0 / jnp.sum(e, axis=1, keepdims=True))).astype(LOW)
        made = dot_nn(p_ref[head], pick(mask, v))
        total = made if total is None else total + made
    mixed_ref[3] = total.astype(LOW)


def attention_forward(x, sources, qv_bias, bias, first, before, tile=64):
    rows, width = x.shape
    slots, slot_rows, _ = bias.shape
    blocks = len(sources)
    part = sources[0].shape[0] // 3
    heads = part // HD
    aliased = int(before is not None)
    mixed = shape_of((4, 4, rows, part), LOW)
    probs = shape_of((4, slots, heads, slot_rows, slot_rows), LOW)
    return call(
        functools.partial(attention_forward_kernel, blocks=blocks, aliased=aliased, tile=tile),
        "attention_forward",
        (slots, blocks),
        [
            pl.BlockSpec((slot_rows, width), lambda s, b: (s, 0)),
            pl.BlockSpec((None, 2, 1, part), lambda s, b: (b, 0, 0, 0)),
            pl.BlockSpec((None, slot_rows, slot_rows), lambda s, b: (s, 0, 0)),
        ]
        + [in_place()] * (blocks + 2 * aliased),
        [
            pl.BlockSpec((None, 4, slot_rows, part), lambda s, b: (first + b, 0, s, 0)),
            pl.BlockSpec(
                (None, None, heads, slot_rows, slot_rows), lambda s, b: (first + b, s, 0, 0, 0)
            ),
        ],
        [mixed, probs],
        [
            pltpu.VMEM((heads, slot_rows, slot_rows), WIDE),
            pltpu.VMEM((blocks, 3 * part, width), LOW),
            pltpu.SemaphoreType.DMA((blocks,)),
        ],
        [],
        [x, qv_bias, bias, *sources, *(before or ())],
        alias={3 + blocks: 0, 4 + blocks: 1} if aliased else None,
        flops=blocks * (6 * rows * width * part + 8 * heads * rows * slot_rows * 256),
    )


def row_tiles(rows, tile):
    return [pl.ds(start, tile) for start in range(0, rows, tile)]


def ffn_forward_kernel(own_ref, mixed_hbm, x_hbm, wo_hbm, wu_ref, wd_ref, bu_ref, small_ref,
                       u1_hbm, hr_hbm, gr_hbm, gp_hbm, u2_hbm, low_hbm,
                       o_ref, x_ref, wo_ref, u1_ref, hr_ref, gr_ref, gp_ref, u2_ref, low_ref, in_sems, out_sems, g_sems,
                       *, layer, tile, renorm):
    step, steps = pl.program_id(0), pl.num_programs(0)
    part = o_ref.shape[2]
    tiles = row_tiles(x_ref.shape[0], tile)
    wo_copy = pltpu.make_async_copy(wo_hbm.at[layer], wo_ref, in_sems.at[0, 0])
    loads, first_out, last_out = [], [], []
    for t, at in enumerate(tiles):
        loads.append(
            [
                pltpu.make_async_copy(mixed_hbm.at[:, 3, at], o_ref.at[:, at], in_sems.at[1, t]),
                pltpu.make_async_copy(x_hbm.at[at], x_ref.at[at], in_sems.at[2, t]),
            ]
        )
        first_out.append(
            [
                pltpu.make_async_copy(u1_ref.at[at], u1_hbm.at[at], out_sems.at[0, t]),
                pltpu.make_async_copy(hr_ref.at[at], hr_hbm.at[at], out_sems.at[1, t]),
            ]
        )
        last_out.append(
            [
                pltpu.make_async_copy(u2_ref.at[at], u2_hbm.at[at], out_sems.at[2, t]),
                pltpu.make_async_copy(low_ref.at[at], low_hbm.at[at], out_sems.at[3, t]),
            ]
        )

    def g_out(chunk, slot):
        return [
            pltpu.make_async_copy(gr_ref.at[slot], gr_hbm.at[chunk], g_sems.at[0, slot]),
            pltpu.make_async_copy(gp_ref.at[slot], gp_hbm.at[chunk], g_sems.at[1, slot]),
        ]

    @pl.when(step == 0)
    def _():
        wo_copy.start()
        for pair in loads:
            for copy in pair:
                copy.start()
        wo_copy.wait()
        for t, at in enumerate(tiles):
            for copy in loads[t]:
                copy.wait()
            residual = x_ref[at].astype(WIDE)
            if renorm:
                residual = row_stats(residual)[0] * small_ref[6:7] + small_ref[7:8]
            u1 = residual + small_ref[0:1]
            for block in range(4):
                rows = pl.ds(pl.multiple_of((own_ref[0] ^ block) * part, 16), part)
                u1 = u1 + dot_nn(o_ref[block, at], wo_ref[rows, :])
            u1_ref[at] = u1
            normed = row_stats(u1)[0] * small_ref[1:2] + small_ref[2:3]
            hr_ref[at] = normed.astype(LOW)
            u2_ref[at] = normed + small_ref[3:4]
            for copy in first_out[t]:
                copy.start()

    slot = step % 2

    @pl.when(step >= 2)
    def _():
        for copy in g_out(step - 2, slot):
            copy.wait()

    z = dot_nn(hr_ref[...], wu_ref[...]) + bu_ref[...]
    g, slope = gelu_pair(z)
    gr = g.astype(LOW)
    gr_ref[slot] = gr
    gp_ref[slot] = slope.astype(LOW)
    for copy in g_out(step, slot):
        copy.start()
    u2_ref[...] += dot_nn(gr, wd_ref[...])

    @pl.when(step == steps - 1)
    def _():
        for t, at in enumerate(tiles):
            total = u2_ref[at]
            low_ref[at] = (row_stats(total)[0] * small_ref[4:5] + small_ref[5:6]).astype(LOW)
            for copy in last_out[t]:
                copy.start()
        for copy in [*g_out(step - 1, 1 - slot), *g_out(step, slot)]:
            copy.wait()
        for pair in first_out + last_out:
            for copy in pair:
                copy.wait()


def ffn_forward(own, mixed, x, wo, wu, wd, bu, small, layer, renorm, tile=512):
    _, _, rows, part = mixed.shape
    width, hidden = wu.shape[1:]
    chunks = hidden // width
    fixed = lambda v: pl.BlockSpec(v.shape, lambda i, o: (0,) * v.ndim)
    sems = lambda *shape: pltpu.SemaphoreType.DMA(shape)
    return call(
        functools.partial(ffn_forward_kernel, layer=layer, tile=tile, renorm=renorm),
        "ffn_forward",
        (chunks,),
        [
            in_place(),
            in_place(),
            in_place(),
            pl.BlockSpec((None, width, width), lambda i, o: (layer, 0, i)),
            pl.BlockSpec((None, width, width), lambda i, o: (layer, i, 0)),
            pl.BlockSpec((None, 1, width), lambda i, o: (i, 0, 0)),
            fixed(small),
        ],
        [in_place()] * 6,
        [
            shape_of((rows, width), WIDE),
            shape_of((rows, width), LOW),
            shape_of((chunks, rows, width), LOW),
            shape_of((chunks, rows, width), LOW),
            shape_of((rows, width), WIDE),
            shape_of((rows, width), LOW),
        ],
        [
            pltpu.VMEM((4, rows, part), LOW),
            pltpu.VMEM((rows, width), x.dtype),
            pltpu.VMEM((width, width), LOW),
            pltpu.VMEM((rows, width), WIDE),
            pltpu.VMEM((rows, width), LOW),
            pltpu.VMEM((2, rows, width), LOW),
            pltpu.VMEM((2, rows, width), LOW),
            pltpu.VMEM((rows, width), WIDE),
            pltpu.VMEM((rows, width), LOW),
            sems(3, rows // tile),
            sems(4, rows // tile),
            sems(2, 2),
        ],
        [own],
        [mixed, x, wo, wu, wd, bu, small],
        flops=6 * rows * width * (width + 2 * hidden),
    )


def reversed_bits(value, count):
    made = 0
    for bit in range(count):
        made = made | (((value >> bit) & 1) << (count - 1 - bit))
    return made


def row_halves(depth):
    return [(half, slice(half * depth // 2, (half + 1) * depth // 2)) for half in range(2)]


def each_chunk(made, count, half):
    rows = made.shape[0] // count
    for dp in range(count):
        yield half * count + dp, made[dp * rows : (dp + 1) * rows]


def place(dp, own_dp, dp_count):
    away = dp ^ own_dp
    return away & 1, reversed_bits(away >> 1, dp_count.bit_length() - 2)


def ffn_backward_kernel(own_ref, gx_hbm, u2_hbm, u1_hbm, gp_hbm, hr_hbm, gr_hbm, wo_hbm, wu_ref, wd_ref, gain_ref,
                        da_hbm, do_hbm, du_hbm, sums_ref, zsum_ref, send_ref, keep_ref,
                        gx_ref, u2_ref, u1_ref, gp_ref, hr_ref, gr_ref, wo_ref, acc_ref, df_ref, dz_ref, da_ref, do_ref,
                        in_sems, out_sems, g_sems, *, layer, tile, dp_count):
    step, steps = pl.program_id(0), pl.num_programs(0)
    own, own_dp = own_ref[0], own_ref[1]
    part = do_ref.shape[2]
    tiles = row_tiles(gx_ref.shape[0], tile)
    count = len(tiles)
    loads, last_out = [], []
    for t, at in enumerate(tiles):
        loads.append(
            [
                pltpu.make_async_copy(gx_hbm.at[at], gx_ref.at[at], in_sems.at[0, t]),
                pltpu.make_async_copy(u2_hbm.at[at], u2_ref.at[at], in_sems.at[1, t]),
            ]
        )
        last_out.append(
            [
                pltpu.make_async_copy(u2_ref.at[at], du_hbm.at[at], out_sems.at[0, t]),
                pltpu.make_async_copy(da_ref.at[:, at], da_hbm.at[:, at], out_sems.at[1, t]),
                pltpu.make_async_copy(do_ref.at[:, at], do_hbm.at[:, at], out_sems.at[2, t]),
            ]
        )
    hr_copy = pltpu.make_async_copy(hr_hbm, hr_ref, in_sems.at[2, 0])
    u1_copy = pltpu.make_async_copy(u1_hbm, u1_ref, in_sems.at[2, 1])
    wo_copy = pltpu.make_async_copy(wo_hbm.at[layer], wo_ref, in_sems.at[2, 2])

    def streams(at_step):
        slot, head = at_step % 2, own ^ head_order(at_step)
        return (
            pltpu.make_async_copy(gp_hbm.at[head], gp_ref.at[slot], g_sems.at[0, slot]),
            pltpu.make_async_copy(gr_hbm.at[head], gr_ref.at[slot], g_sems.at[1, slot]),
        )

    slot = step % 2
    gp_copy, gr_copy = streams(step)

    @pl.when(step == 0)
    def _():
        for pair in loads:
            for copy in pair:
                copy.start()

        gp_copy.start()
        hr_copy.start()
        gr_copy.start()

    @pl.when(step < steps - 1)
    def _():
        for copy in streams(step + 1):
            copy.start()

    @pl.when(step == 1)
    def _():
        u1_copy.start()
        wo_copy.start()

    @pl.when(step == 0)
    def _():
        sums_ref[...] = jnp.zeros_like(sums_ref)
        for t, at in enumerate(tiles):
            for copy in loads[t]:
                copy.wait()
            gx = gx_ref[at].astype(WIDE)
            xhat, inverse = row_stats(u2_ref[at])
            sums_ref[0:1] += column_sum(gx * xhat)
            sums_ref[1:2] += column_sum(gx)
            gv = norm_backward(gx, xhat, inverse, gain_ref[1:2])
            df = gv.astype(LOW)
            df_ref[at] = df
            sums_ref[2:3] += column_sum(df.astype(WIDE))
            acc_ref[at] = gv

    gp_copy.wait()
    zsum = jnp.zeros(zsum_ref.shape, WIDE)
    for start in range(0, dz_ref.shape[0], 256):
        at = slice(start, start + 256)
        dg = dot_nt(df_ref[at], wd_ref[...])
        dz = (dg * gp_ref[slot, at].astype(WIDE)).astype(LOW)
        dz_ref[at] = dz
        zsum = zsum + column_sum(dz.astype(WIDE))
        acc_ref[at] += dot_nt(dz, wu_ref[...])
    zsum_ref[...] = zsum

    @pl.when(step == 0)
    def _():
        hr_copy.wait()

    gr_copy.wait()
    for out, wanted in ((send_ref, step < 2), (keep_ref, step >= 2)):

        @pl.when(wanted)
        def _():
            for which, (a, b) in enumerate(((hr_ref, dz_ref[...]), (df_ref, gr_ref[slot]))):
                for first, rows in row_halves(hr_ref.shape[1]):
                    made = dot_tn(a[:, rows], b).astype(LOW)
                    for dp, chunk in each_chunk(made, dp_count // 2, first):
                        out[(which, *place(dp, own_dp, dp_count))] = chunk

    @pl.when(step == steps - 1)
    def _():
        u1_copy.wait()
        wo_copy.wait()
        for t, at in enumerate(tiles):
            total = acc_ref[at]
            xhat, inverse = row_stats(u1_ref[at])
            sums_ref[3:4] += column_sum(total * xhat)
            sums_ref[4:5] += column_sum(total)
            du = norm_backward(total, xhat, inverse, gain_ref[0:1])
            u2_ref[at] = du
            da = du.astype(LOW)
            for block in range(4):
                da_ref[block, at] = da[:, block * part : (block + 1) * part]
            sums_ref[5:6] += column_sum(da.astype(WIDE))
            for block in range(4):
                rows = pl.ds(pl.multiple_of((own ^ block) * part, 16), part)
                do_ref[block, at] = dot_nt(da, wo_ref[rows, :]).astype(LOW)
            for copy in last_out[t]:
                copy.start()
        for several in last_out:
            for copy in several:
                copy.wait()


def head_order(step):
    return jnp.where(step < 2, 1 + 2 * step, 2 * (step - 2))


def ffn_backward(own, gx, u2, u1, gp, hr, gr, wo, wu, wd, gains, layer, dp_count, tile=512):
    rows, width = gx.shape
    chunks = gp.shape[0]
    part = width // 4
    chunk_rows = width // dp_count
    rest = dp_count // 2
    fixed = lambda s: pl.BlockSpec(s.shape, lambda i, o: (0,) * len(s.shape))
    head = lambda i, o: o[0] ^ head_order(i)
    block = (2, None, 2, rest, chunk_rows, width)
    sums = shape_of((8, width), WIDE)
    grads = stored((2, 2, 2, rest, chunk_rows, width), LOW)
    sems = lambda *shape: pltpu.SemaphoreType.DMA(shape)
    low = lambda *shape: pltpu.VMEM(shape, LOW)
    wide = lambda *shape: pltpu.VMEM(shape, WIDE)
    return call(
        functools.partial(ffn_backward_kernel, layer=layer, tile=tile, dp_count=dp_count),
        "ffn_backward",
        (chunks,),
        [in_place()] * 7
        + [
            pl.BlockSpec((None, width, width), lambda i, o: (layer, 0, head(i, o))),
            pl.BlockSpec((None, width, width), lambda i, o: (layer, head(i, o), 0)),
            fixed(gains),
        ],
        [
            in_place(),
            in_place(),
            in_place(),
            fixed(sums),
            pl.BlockSpec((None, 1, width), lambda i, o: (head(i, o), 0, 0)),
            pl.BlockSpec(block, lambda i, o: (0, jnp.minimum(i, 1), 0, 0, 0, 0)),
            pl.BlockSpec(block, lambda i, o: (0, jnp.maximum(i - 2, 0), 0, 0, 0, 0)),
        ],
        [
            shape_of((4, rows, part), LOW),
            shape_of((4, rows, part), LOW),
            shape_of((rows, width), WIDE),
            sums,
            shape_of((chunks, 1, width), WIDE),
            grads,
            grads,
        ],
        [
            pltpu.VMEM((rows, width), gx.dtype),
            wide(rows, width),
            wide(rows, width),
            low(2, rows, width),
            low(rows, width),
            low(2, rows, width),
            low(width, width),
            wide(rows, width),
            low(rows, width),
            low(rows, width),
            low(4, rows, part),
            low(4, rows, part),
            sems(3, max(rows // tile, 3)),
            sems(3, rows // tile),
            sems(2, 2),
        ],
        [own],
        [gx, u2, u1, gp, hr, gr, wo, wu, wd, gains],
        flops=4 * rows * width * (width + 4 * chunks * width),
    )


def split_rows(made, half, got_ref, own_dp, dp_count, send_ref, keep_ref):
    for dp, chunk in each_chunk(made, dp_count // 2, half):
        away, rest = place(dp, own_dp, dp_count)
        summed = (chunk + got_ref[away, rest].astype(WIDE)).astype(LOW)

        @pl.when(away == 1)
        def _():
            send_ref[rest] = summed

        @pl.when(away == 0)
        def _():
            keep_ref[rest] = summed


def add_rows(made, half, got_ref, own_dp, dp_count, out_ref):
    for dp, chunk in each_chunk(made, dp_count // 2, half):
        at = place(dp, own_dp, dp_count)
        out_ref[at] = (chunk + got_ref[at].astype(WIDE)).astype(LOW)


def core_add_kernel(kept_ref, got_ref, up_send, up_keep, down_send, down_keep):
    step = pl.program_id(0)

    which, away = step // 2, jnp.where(step < 2, step, 3 - step)

    def summed(at):
        return (kept_ref[at].astype(WIDE) + got_ref[which, away, at].astype(WIDE)).astype(LOW)

    @pl.when(step < 2)
    def _():
        up_keep[...] = summed(0)
        up_send[...] = summed(1)

    for out, wanted in ((down_send, 2), (down_keep, 3)):

        @pl.when(step == wanted)
        def _():
            out[0] = summed(0)
            out[1] = summed(1)


def core_add(kept, got):
    _, _, _, rest, chunk_rows, width = kept.shape

    def at(i):
        return (i // 2, jnp.where(i < 2, i, 3 - i), 0, 0, 0, 0)

    block = pl.BlockSpec((None, None, 2, rest, chunk_rows, width), at)
    up = pl.BlockSpec((None, rest, chunk_rows, width), lambda i: (jnp.minimum(i, 1), 0, 0, 0))
    down = pl.BlockSpec((2, rest, chunk_rows, width), lambda i: (0, 0, 0, 0))
    made = stored((2, rest, chunk_rows, width), LOW)
    return call(
        core_add_kernel,
        "core_add",
        (4,),
        [block, pl.BlockSpec(memory_space=pltpu.VMEM)],
        [up, up, down, down],
        [made] * 4,
        [],
        [],
        [kept, got],
        vmem=24 << 20,
    )


def attention_backward_kernel(own_ref, mixed_ref, do_ref, p_ref, x_ref, o_ref, da_ref, wa_ref, wb_ref, gx_ref, *refs,
                              dp_count, tile, keep):
    if keep:
        got_ref, *refs = refs
    out_ref, sums_ref, *refs = refs
    grads = refs[: 4 if keep else 1]
    t_ref, ds_ref, parts_ref, xt_ref, ot_ref, acc_ref = refs[4 if keep else 1 :]
    slot, block = pl.program_id(0), pl.program_id(1)
    last = pl.num_programs(0) - 1
    own, own_dp = own_ref[0], own_ref[1]
    rows, part = mixed_ref.shape[1:]

    @pl.when((slot == 0) & (block == 0))
    def _():
        xt_ref[...] = x_ref[...].T
        for r in range(4):
            ot_ref[pl.ds(pl.multiple_of((own ^ r) * part, 16), part), :] = o_ref[r].T
        sums_ref[...] = jnp.zeros_like(sums_ref)

    dq = dk = dv = None
    for head, mask in enumerate(head_masks(part)):
        do = pick(mask, do_ref[...])
        t_ref[head] = dot_nt(do, mixed_ref[2])
        for start in range(0, rows, tile):
            at = slice(start, start + tile)
            p = p_ref[head, at].astype(WIDE)
            dp = t_ref[head, at]
            share = jnp.sum(p * dp, axis=1, keepdims=True)
            ds_ref[head, at] = (p * (dp - share)).astype(LOW)
        made = (
            dot_nn(ds_ref[head], pick(mask, mixed_ref[1])),
            dot_tn(ds_ref[head], pick(mask, mixed_ref[0])),
            dot_tn(p_ref[head], do),
        )
        dq, dk, dv = made if dq is None else (dq + made[0], dk + made[1], dv + made[2])
    dq = (dq * HD**-0.5).astype(LOW)
    dk = dk.astype(LOW)
    dv = dv.astype(LOW)
    sums_ref[block, 0:1] += column_sum(dq.astype(WIDE))
    sums_ref[block, 1:2] += column_sum(dv.astype(WIDE))
    joined = jnp.concatenate([dq, dk, dv], axis=1)
    parts_ref[block, pl.ds(pl.multiple_of(slot * rows, rows), rows), :] = joined
    weights = jnp.where(block == 0, wa_ref[...], wb_ref[...])
    passed = dot_nn(joined, weights)

    @pl.when(block == 0)
    def _():
        acc_ref[...] = gx_ref[...] + passed

    @pl.when(block == 1)
    def _():
        out_ref[...] = (acc_ref[...] + passed).astype(out_ref.dtype)

    @pl.when(slot == last)
    def _():
        for half, rows in row_halves(xt_ref.shape[0]):
            first = dot_nn(xt_ref[rows, :], parts_ref[block])
            second = dot_nn(ot_ref[rows, :], da_ref[...])
            made = jnp.concatenate([first, second], axis=1)
            if not keep:
                for dp, chunk in each_chunk(made.astype(LOW), dp_count // 2, half):
                    grads[0][place(dp, own_dp, dp_count)] = chunk
                continue
            cut = made.shape[1] // 2
            a_send, a_keep, b_send, b_keep = grads
            got = [got_ref.at[:, :, :, :cut], got_ref.at[:, :, :, cut:]]
            for where_to, wanted in ((a_keep, 0), (a_send, 1)):

                @pl.when(block == wanted)
                def _():
                    add_rows(made[:, :cut], half, got[0], own_dp, dp_count, where_to)

            split_rows(made[:, cut:], half, got[1], own_dp, dp_count, b_send, b_keep)


def attention_backward(own, mixed, do, probs, x, da, wa, wb, gx, got, dp_count, out_type, tile=64):
    rows, width = x.shape
    part = mixed.shape[3]
    _, slots, heads, slot_rows, _ = probs.shape
    chunk_rows, rest = width // dp_count, dp_count // 2
    keep = got is not None
    away = 0 if keep else 1
    block_of = lambda b: 2 * b + away
    row = pl.BlockSpec((slot_rows, width), lambda s, b, o: (s, 0))
    last = slots - 1
    late = lambda s, b: jnp.where(s == last, b, 0)
    in_specs = [
        pl.BlockSpec((None, 3, slot_rows, part), lambda s, b, o: (block_of(b), 0, s, 0)),
        pl.BlockSpec((None, slot_rows, part), lambda s, b, o: (block_of(b), s, 0)),
        pl.BlockSpec(
            (None, None, heads, slot_rows, slot_rows), lambda s, b, o: (block_of(b), s, 0, 0, 0)
        ),
        whole(x),
        pl.BlockSpec((4, None, rows, part), lambda s, b, o: (0, 3, 0, 0), pipeline_mode=pl.Buffered(1)),
        pl.BlockSpec((None, rows, part), lambda s, b, o: (o[0] ^ block_of(late(s, b)), 0, 0)),
        whole(wa),
        whole(wb),
        row,
    ]
    operands = [mixed, do, probs, x, mixed, da, wa, wb, gx]
    sums = shape_of((2, 8, part), WIDE)
    out_specs = [row, pl.BlockSpec(sums.shape, lambda s, b, o: (0, 0, 0))]
    out_shape = [shape_of((rows, width), out_type), sums]
    whole_block = lambda w: pl.BlockSpec((2, rest, chunk_rows, w), lambda s, b, o: (0, 0, 0, 0))
    if keep:
        in_specs.append(
            pl.BlockSpec(
                (None, 2, rest, chunk_rows, width), lambda s, b, o: (late(s, b), 0, 0, 0, 0)
            )
        )
        operands.append(got)
        half = width // 2
        b_block = pl.BlockSpec(
            (None, rest, chunk_rows, half), lambda s, b, o: (late(s, b), 0, 0, 0)
        )
        out_specs += [whole_block(half)] * 2 + [b_block] * 2
        out_shape += [stored((2, rest, chunk_rows, half), LOW)] * 4
    else:
        out_specs.append(
            pl.BlockSpec(
                (None, 2, rest, chunk_rows, width), lambda s, b, o: (late(s, b), 0, 0, 0, 0)
            )
        )
        out_shape.append(stored((2, 2, rest, chunk_rows, width), LOW))
    return call(
        functools.partial(attention_backward_kernel, dp_count=dp_count, tile=tile, keep=keep),
        "attention_backward",
        (slots, 2),
        in_specs,
        out_specs,
        out_shape,
        [
            pltpu.VMEM((heads, slot_rows, slot_rows), WIDE),
            pltpu.VMEM((heads, slot_rows, slot_rows), LOW),
            pltpu.VMEM((2, rows, 3 * part), LOW),
            pltpu.VMEM((width, rows), LOW),
            pltpu.VMEM((width, rows), LOW),
            pltpu.VMEM((slot_rows, width), WIDE),
        ],
        [own],
        operands,
        flops=36 * heads * rows * slot_rows * 256,
    )


def bits_of(axis):
    size = lax.axis_size(axis)
    return [1 << bit for bit in range(size.bit_length() - 1)]


def swap(value, axis, bit):
    size = lax.axis_size(axis)
    return lax.ppermute(value, axis, [(i, i ^ bit) for i in range(size)])


def add_split_kernel(*refs, merge_in, merge_out, extra):
    inputs = 2 if merge_in else 4
    outputs = 2 if merge_out else 4
    ins, refs = refs[:inputs], refs[extra:]
    outs = refs[inputs : inputs + outputs]
    kept_ref, send_ref, keep_ref, in_sems, out_sems = refs[inputs + outputs :]
    half = send_ref.shape[1]
    loads, got, stores = [], [], []
    for part in range(2):
        kept, came = (ins[0].at[part], ins[1].at[part]) if merge_in else ins[2 * part : 2 * part + 2]
        send, keep = (
            (outs[0].at[part], outs[1].at[part]) if merge_out else outs[2 * part : 2 * part + 2]
        )
        got.append(came)
        loads.append(pltpu.make_async_copy(kept, kept_ref.at[part], in_sems.at[part]))
        stores.append(
            [
                pltpu.make_async_copy(send_ref.at[part], send, out_sems.at[part, 0]),
                pltpu.make_async_copy(keep_ref.at[part], keep, out_sems.at[part, 1]),
            ]
        )
    for copy in loads:
        copy.start()
    for part in range(2):
        loads[part].wait()
        for at, (out, copy) in enumerate(zip((send_ref, keep_ref), stores[part])):
            rows = pl.ds(half * (1 - at), half)
            out[part] = (kept_ref[part, rows].astype(WIDE) + got[part][rows].astype(WIDE)).astype(LOW)
            copy.start()
    for copies in stores:
        for copy in copies:
            copy.wait()


def add_split(ins, merge_in, merge_out, arrived):
    size, rows, columns = ins[0].shape[-3:]
    half = (size // 2, rows, columns)
    out_shape = [stored((2, *half), LOW)] * 2 if merge_out else [stored(half, LOW)] * 4
    return pl.pallas_call(
        functools.partial(
            add_split_kernel, merge_in=merge_in, merge_out=merge_out, extra=len(arrived)
        ),
        in_specs=[in_hbm(), pl.BlockSpec(memory_space=pltpu.VMEM)] * (len(ins) // 2)
        + [in_place()] * len(arrived),
        out_specs=[in_hbm()] * len(out_shape),
        out_shape=out_shape,
        scratch_shapes=[
            pltpu.VMEM((2, size, rows, columns), LOW),
            pltpu.VMEM((2, *half), LOW),
            pltpu.VMEM((2, *half), LOW),
            pltpu.SemaphoreType.DMA((2,)),
            pltpu.SemaphoreType.DMA((2, 2)),
        ],
        compiler_params=pltpu.CompilerParams(vmem_limit_bytes=16 << 20),
        cost_estimate=pl.CostEstimate(flops=0, bytes_accessed=0, transcendentals=0),
        name="add_split",
    )(*ins, *arrived)


class Summing:
    def __init__(self, a_send, a_keep, b_send, b_keep):
        head, dp = bits_of("head"), bits_of("dp")
        self.stages = [(("dp", dp[0]), ("head", head[1]))] + [(("dp", bit),) for bit in dp[1:]]
        self.at = 0
        self.settled = False
        self.kept = [a_keep, b_keep]
        self.got = [swap(a_send, "head", head[1]), swap(b_send, "dp", dp[0])]

    def busy(self):
        return self.at < len(self.stages)

    def step(self, after, arrived=()):
        stage = self.stages[self.at]
        merge_in, merge_out = len(self.kept) == 1, len(stage) == 1
        ins = [v for pair in zip(self.kept, self.got) for v in pair]
        lead = 1 if merge_in else 0
        ins = [v.reshape(*v.shape[:lead], -1, *v.shape[-2:]) for v in ins]
        ins, _ = lax.optimization_barrier((ins, after))
        outs = add_split(ins, merge_in, merge_out, arrived)
        if merge_out:
            self.got, self.kept = [swap(outs[0], *stage[0])], [outs[1]]
        else:
            self.got = [swap(outs[0], *stage[0]), swap(outs[2], *stage[1])]
            self.kept = [outs[1], outs[3]]
        self.at += 1
        return outs[-1]


def last_sums_kernel(*refs, layers):
    ins, outs = refs[: 4 * layers + 2], refs[4 * layers + 2 :]
    qkv, qv, out_w, out_b, gain1, shift1, up_w, up_b, down_w, down_b, gain2, shift2 = outs
    part = out_w.shape[2]
    width = down_b.shape[1]
    rows = ins[-2][...] + ins[-1][...]
    for layer in range(layers):
        ffn_kept, ffn_got, wide_kept, wide_got = ins[4 * layer : 4 * layer + 4]
        down_w[layer] = ffn_kept[0, 0].astype(WIDE) + ffn_got[0, 0].astype(WIDE)
        up_w[layer] = ffn_kept[1, 0].astype(WIDE) + ffn_got[1, 0].astype(WIDE)
        for half in range(2):
            both = wide_kept[half, 0].astype(WIDE) + wide_got[half, 0].astype(WIDE)
            for at in range(2):
                which = 2 * half + at
                block = both[:, at * part : (at + 1) * part]
                if which < 3:
                    qkv[layer, which] = block
                else:
                    out_w[layer] = block
        for row, out in enumerate((gain2, shift2, down_b, gain1, shift1, out_b)):
            out[layer : layer + 1] = rows[layer, row : row + 1]
        qv[layer] = rows[layer, 6:8]
        for row in range(up_b.shape[1] // width):
            at = slice(row * width, (row + 1) * width)
            up_b[layer : layer + 1, at] = rows[layer, 8 + row : 9 + row]


def last_sums(groups, small, passing):
    layers, _, width = small.shape
    ins, specs = [], []
    for group in groups:
        ins += [group.kept[0], group.got[0]]
    ins = [v.reshape(2, 1, *v.shape[-2:]) for v in ins] + [small, passing]
    rows, part = ins[0].shape[2], ins[2].shape[3] // 2
    hidden = (small.shape[1] - 8) * width
    shapes = [
        (layers, 3, rows, part),
        (layers, 2, width),
        (layers, rows, part),
        (layers, width),
        (layers, width),
        (layers, width),
        (layers, rows, width),
        (layers, hidden),
        (layers, rows, width),
        (layers, width),
        (layers, width),
        (layers, width),
    ]
    spec = lambda shape: pl.BlockSpec(shape, lambda i: (0,) * len(shape))
    specs = [spec(v.shape) for v in ins]
    return call(
        functools.partial(last_sums_kernel, layers=layers),
        "last_sums",
        (1,),
        specs,
        [spec(shape) for shape in shapes],
        [shape_of(shape, WIDE) for shape in shapes],
        [],
        [],
        ins,
        vmem=24 << 20,
    )


def ordered(after, *values):
    values, _ = lax.optimization_barrier((values, after))
    return values


def near_blocks(block, after):
    low, high = bits_of("head")
    near = swap(block, "head", low)
    (later,) = ordered((after, near), block)
    return block, near, swap(later, "head", high)


def gathered_pairs(block, after):
    own, near, far = near_blocks(block, after)
    return jnp.stack([own, near]), jnp.stack([far, swap(far, "head", bits_of("head")[0])])


def on_device(
    tokens,
    seq_lengths,
    qkv_weight,
    qv_bias,
    out_weight,
    out_bias,
    norm1_gain,
    norm1_shift,
    up_weight,
    up_bias,
    down_weight,
    down_bias,
    norm2_gain,
    norm2_shift,
    out_grad,
):
    head_count, dp_count = lax.axis_size("head"), lax.axis_size("dp")
    head_index, dp_index = lax.axis_index("head"), lax.axis_index("dp")
    own = jnp.stack([head_index, dp_index]).astype(jnp.int32)
    local_rows, width = tokens.shape
    slot_rows = local_rows * head_count // seq_lengths.shape[0]
    slots = local_rows // slot_rows
    layers = qkv_weight.shape[0]
    part = width // head_count
    turned = jnp.swapaxes(qkv_weight, 2, 3).reshape(layers, 3 * part, width)
    base = (head_index * slots).astype(jnp.int32).reshape(1)
    bias = mask_bias(seq_lengths, base, slots, slot_rows)
    weights = [near_blocks(turned[0], base)]
    near_bias, far_bias = gathered_pairs(qv_bias[:, :, None], base)
    up_rows = up_bias.reshape(layers, -1, 1, width)
    rounded, residual = tokens, tokens
    kept = []
    for layer in range(layers):
        before = max(layer - 1, 0)
        small = jnp.stack(
            [
                out_bias[layer],
                norm1_gain[layer],
                norm1_shift[layer],
                down_bias[layer],
                norm2_gain[layer],
                norm2_shift[layer],
                norm2_gain[before],
                norm2_shift[before],
            ]
        )
        own_w, near_w, far_w = weights[layer]
        if layer == 0:
            near = attention_forward(rounded, (own_w, near_w), near_bias[:, layer], bias, 0, None)
            (far_w, far_b) = ordered(near[0], far_w, far_bias[:, layer])
            both_w = swap(far_w, "head", bits_of("head")[0])
            for other in range(1, layers):
                (later,) = ordered(near[0], turned[other])
                weights.append(near_blocks(later, near[0]))
            mixed, probs = attention_forward(rounded, (far_w, both_w), far_b, bias, 2, near)
            (far_ws,) = ordered(mixed, [w[2] for w in weights[1:]])
            both_ws = [swap(w, "head", bits_of("head")[0]) for w in far_ws]
        else:
            both_w = both_ws[layer - 1]
            all_bias = jnp.concatenate([near_bias[:, layer], far_bias[:, layer]])
            mixed, probs = attention_forward(
                rounded, (own_w, near_w, far_w, both_w), all_bias, bias, 0, None
            )
        weights[layer] = w = (own_w, near_w, far_w, both_w)
        u1, hr, gr, slope, u2, low = ffn_forward(
            own,
            mixed,
            residual,
            out_weight,
            up_weight,
            down_weight,
            up_rows[layer],
            small,
            layer,
            layer > 0,
        )
        kept.append((rounded, mixed, probs, u1, hr, gr, slope, u2))
        rounded, residual = low, u2
    out_state = rounded
    grad_state = out_grad
    small_sums = [None] * layers
    hidden_sums = [None] * layers
    ffn_groups, wide_groups = [None] * layers, [None] * layers
    running = []

    def advance(after):
        arrived = []
        for group in running:
            if not group.busy() and not group.settled:
                arrived += group.got
                group.settled = True
        for group in running:
            if group.busy():
                after = group.step(after, arrived)
                arrived = []
        return after

    for layer in reversed(range(layers)):
        rounded, mixed, probs, u1, hr, gr, slope, u2 = kept[layer]
        w = weights[layer]
        gains = jnp.stack([norm1_gain[layer], norm2_gain[layer]])
        da, do, du, sums, zsums, sent, ffn_kept = ffn_backward(
            own,
            grad_state,
            u2,
            u1,
            slope,
            hr,
            gr,
            out_weight,
            up_weight,
            down_weight,
            gains,
            layer,
            dp_count,
        )
        low_bit = bits_of("head")[0]
        early = bool(running)
        token = advance(do)
        if early:
            (sent,) = ordered(token, sent)
        got = swap(sent, "head", low_bit)

        def sum_ffn(after):
            values = ordered(after, ffn_kept, got)
            up_send, up_keep, down_send, down_keep = core_add(*values)
            ffn_groups[layer] = Summing(down_send, down_keep, up_send, up_keep)
            running.insert(0, ffn_groups[layer])
            return down_keep

        if early:
            token = sum_ffn(token)
        (do, du) = ordered(token, do, du)
        half_grad, away_sums, sent = attention_backward(
            own, mixed, do, probs, rounded, da, w[1], w[3], du, None, dp_count, WIDE
        )
        if early:
            token = advance(half_grad)
            (sent,) = ordered(token, sent)
            wide_got = swap(sent, "head", low_bit)
        else:
            wide_got = swap(sent, "head", low_bit)
            token = sum_ffn(half_grad)
        (half_grad, do) = ordered(token, half_grad, do)
        grad_state, own_sums, *parts = attention_backward(
            own,
            mixed,
            do,
            probs,
            rounded,
            da,
            w[0],
            w[2],
            half_grad,
            wide_got,
            dp_count,
            WIDE if layer else LOW,
        )
        wide_groups[layer] = Summing(*parts)
        token = advance(grad_state) if layer else grad_state
        if layer:
            (grad_state,) = ordered(token, grad_state)
        running.append(wide_groups[layer])
        blocks = [own_sums[0], away_sums[0], own_sums[1], away_sums[1]]
        stacked = jnp.stack(blocks)[:, :2]
        qv_sums = jnp.concatenate(
            [
                lax.dynamic_index_in_dim(stacked, head_index ^ head, 0, keepdims=False)
                for head in range(head_count)
            ],
            axis=1,
        )
        small_sums[layer] = jnp.concatenate([sums[:6], qv_sums, zsums[:, 0]])
    small_sum = jnp.stack(small_sums)
    near, far = bits_of("head")
    waiting = [[("head", near)], [("dp", 1)], [("head", far)], [("dp", 2 * k) for k in range(1, dp_count // 2)]]
    passing = [swap(small_sum, *one) for one in waiting.pop(0)]
    while any(not group.settled for group in running) or waiting:
        if any(group.busy() for group in running):
            token = advance(token)
        elif not waiting:
            break
        if waiting:
            small_sum, passing = ordered(token, small_sum, passing)
            small_sum = sum(passing, small_sum)
            token = small_sum
            passing = [swap(small_sum, *one) for one in waiting.pop(0)]
    small_sum, passing = sum(passing[:-1], small_sum), passing[-1]
    groups = [group for pair in zip(ffn_groups, wide_groups) for group in pair]
    qkv, qv, out_w, out_b, gain1, shift1, up_w, up_b, down_w, down_b, gain2, shift2 = last_sums(
        groups, small_sum, passing
    )
    return (
        out_state,
        grad_state,
        qkv,
        qv,
        out_w,
        out_b,
        gain1,
        shift1,
        up_w,
        up_b,
        jnp.swapaxes(down_w, 1, 2),
        down_b,
        gain2,
        shift2,
    )


def solution(mesh):
    in_specs = (
        P(("dp", "head"), None),
        P("dp", None),
        P(None, None, None, "head"),
        P(None, None, "head"),
        P(),
        P(),
        P(),
        P(),
        P(),
        P(),
        P(),
        P(),
        P(),
        P(),
        P(("dp", "head"), None),
    )
    out_specs = (
        P(("dp", "head"), None),
        P(("dp", "head"), None),
        P(None, None, "dp", "head"),
        P(),
        P(None, "dp", "head"),
        P(),
        P(),
        P(),
        P(None, "dp", "head"),
        P(),
        P(None, "head", "dp"),
        P(),
        P(),
        P(),
    )
    return jax.shard_map(
        on_device, mesh=mesh, in_specs=in_specs, out_specs=out_specs, check_vma=False
    )
```

```python
import functools
import math

import jax
import jax.numpy as jnp
from jax import lax
from jax.experimental import pallas as pl
from jax.experimental.pallas import tpu as pltpu
from jax.sharding import PartitionSpec as P

HD = 64
EPSILON = 1e-06
LOW = jnp.bfloat16
WIDE = jnp.float32
VMEM_BYTES = 58 << 20
ROOT_HALF = 0.7071067811865476
INV_ROOT_TAU = 0.3989422804014327
FAR = -1e30


def row_stats(values):
    centre = jnp.mean(values, axis=-1, keepdims=True)
    centred = values - centre
    spread = jnp.mean(centred * centred, axis=-1, keepdims=True)
    inverse = lax.rsqrt(spread + EPSILON)
    return centred * inverse, inverse


def norm_backward(upstream, xhat, inverse, gain):
    scaled = upstream * gain
    first = jnp.mean(scaled, axis=-1, keepdims=True)
    second = jnp.mean(scaled * xhat, axis=-1, keepdims=True)
    return (scaled - first - xhat * second) * inverse


def column_sum(values):
    return jnp.sum(values, axis=0, keepdims=True)


def dot_nn(left, right):
    return jnp.dot(left, right, preferred_element_type=WIDE)


def dot_nt(left, right):
    return lax.dot_general(left, right, (((1,), (1,)), ((), ())), preferred_element_type=WIDE)


def dot_tn(left, right):
    return lax.dot_general(left, right, (((0,), (0,)), ((), ())), preferred_element_type=WIDE)


def gelu_pair(z):
    cdf = 0.5 + 0.5 * lax.erf(z * ROOT_HALF)
    return z * cdf, cdf + z * (jnp.exp(z * z * -0.5) * INV_ROOT_TAU)


def pick(mask, values):
    return jnp.where(mask, values, jnp.zeros_like(values))


def head_masks(width):
    lanes = lax.broadcasted_iota(jnp.int32, (1, width), 1) // HD
    return [lanes == head for head in range(width // HD)]


def params():
    return pltpu.CompilerParams(vmem_limit_bytes=VMEM_BYTES)


def whole(array):
    return pl.BlockSpec(array.shape, lambda *ids: (0,) * array.ndim, pipeline_mode=pl.Buffered(1))


def in_place():
    return pl.BlockSpec(memory_space=pl.ANY)


def in_vmem():
    return pl.BlockSpec(memory_space=pltpu.VMEM)


def in_hbm():
    return pl.BlockSpec(memory_space=pltpu.HBM)


def shape_of(shape, kind):
    return jax.ShapeDtypeStruct(shape, kind)


def cost(flops, out_shape, operands):
    if not flops:
        return pl.CostEstimate(flops=0, bytes_accessed=0, transcendentals=0)
    made = out_shape if isinstance(out_shape, (list, tuple)) else [out_shape]
    moved = sum(math.prod(v.shape) * jnp.dtype(v.dtype).itemsize for v in [*made, *operands])
    return pl.CostEstimate(flops=flops, bytes_accessed=moved, transcendentals=0)


def stored(shape, kind):
    return pltpu.HBM(shape, kind)


def call(kernel, name, grid, in_specs, out_specs, out_shape, scratch, scalars, operands, alias=None, flops=0, vmem=VMEM_BYTES):
    return pl.pallas_call(
        kernel,
        grid_spec=pltpu.PrefetchScalarGridSpec(
            num_scalar_prefetch=len(scalars),
            grid=grid,
            in_specs=in_specs,
            out_specs=out_specs,
            scratch_shapes=scratch,
        ),
        out_shape=out_shape,
        compiler_params=pltpu.CompilerParams(vmem_limit_bytes=vmem),
        input_output_aliases=alias or {},
        cost_estimate=cost(flops, out_shape, operands),
        name=name,
    )(*scalars, *operands)


def mask_kernel(base_ref, lengths_ref, bias_ref):
    slots, rows, _ = bias_ref.shape
    across = lax.broadcasted_iota(jnp.int32, (8, rows), 1)
    down = lax.broadcasted_iota(jnp.int32, (rows, 128), 0)
    for slot in range(slots):
        reach = jnp.int32(0)
        seg_across = jnp.zeros((8, rows), jnp.int32)
        seg_down = jnp.zeros((rows, 128), jnp.int32)
        for k in range(lengths_ref.shape[1]):
            reach = reach + lengths_ref[base_ref[0] + slot, k]
            seg_across += (across >= reach).astype(jnp.int32)
            seg_down += (down >= reach).astype(jnp.int32)
        inside = seg_down[:, 0:1] == seg_across[0:1, :]
        bias_ref[slot] = jnp.where(inside, 0.0, FAR)


def mask_bias(lengths, base, slots, slot_rows):
    smem = pl.BlockSpec(memory_space=pltpu.SMEM)
    return pl.pallas_call(
        mask_kernel,
        in_specs=[smem, smem],
        out_shape=shape_of((slots, slot_rows, slot_rows), WIDE),
        compiler_params=params(),
        name="mask_bias",
    )(base, lengths)


def attention_forward_kernel(x_ref, b_ref, bias_ref, *refs, blocks, aliased, tile):
    sources = refs[:blocks]
    mixed_ref, p_ref, s_ref, w_ref, sems = refs[blocks + 2 * aliased :]
    rows, part = x_ref.shape[0], w_ref.shape[1] // 3
    slot, block = pl.program_id(0), pl.program_id(1)
    copies = [pltpu.make_async_copy(w, w_ref.at[b], sems.at[b]) for b, w in enumerate(sources)]

    @pl.when((slot == 0) & (block == 0))
    def _():
        for copy in copies:
            copy.start()

    for b, copy in enumerate(copies):

        @pl.when((slot == 0) & (block == b))
        def _():
            copy.wait()

    x = x_ref[...]
    q = ((dot_nt(x, w_ref[block, :part]) + b_ref[0]).astype(LOW) * HD**-0.5).astype(LOW)
    k = dot_nt(x, w_ref[block, part : 2 * part]).astype(LOW)
    v = (dot_nt(x, w_ref[block, 2 * part :]) + b_ref[1]).astype(LOW)
    mixed_ref[0] = q
    mixed_ref[1] = k
    mixed_ref[2] = v
    total = None
    for head, mask in enumerate(head_masks(part)):
        s_ref[head] = dot_nt(pick(mask, q), k)
        for start in range(0, rows, tile):
            at = slice(start, start + tile)
            s = s_ref[head, at] + bias_ref[at]
            e = jnp.exp(s - jnp.max(s, axis=1, keepdims=True))
            p_ref[head, at] = (e * (1.0 / jnp.sum(e, axis=1, keepdims=True))).astype(LOW)
        made = dot_nn(p_ref[head], pick(mask, v))
        total = made if total is None else total + made
    mixed_ref[3] = total.astype(LOW)


def attention_forward(x, sources, qv_bias, bias, first, before, tile=64):
    rows, width = x.shape
    slots, slot_rows, _ = bias.shape
    blocks = len(sources)
    part = sources[0].shape[0] // 3
    heads = part // HD
    aliased = int(before is not None)
    mixed = shape_of((4, 4, rows, part), LOW)
    probs = shape_of((4, slots, heads, slot_rows, slot_rows), LOW)
    return call(
        functools.partial(attention_forward_kernel, blocks=blocks, aliased=aliased, tile=tile),
        "attention_forward",
        (slots, blocks),
        [
            pl.BlockSpec((slot_rows, width), lambda s, b: (s, 0)),
            pl.BlockSpec((None, 2, 1, part), lambda s, b: (b, 0, 0, 0)),
            pl.BlockSpec((None, slot_rows, slot_rows), lambda s, b: (s, 0, 0)),
        ]
        + [in_place()] * (blocks + 2 * aliased),
        [
            pl.BlockSpec((None, 4, slot_rows, part), lambda s, b: (first + b, 0, s, 0)),
            pl.BlockSpec(
                (None, None, heads, slot_rows, slot_rows), lambda s, b: (first + b, s, 0, 0, 0)
            ),
        ],
        [mixed, probs],
        [
            pltpu.VMEM((heads, slot_rows, slot_rows), WIDE),
            pltpu.VMEM((blocks, 3 * part, width), LOW),
            pltpu.SemaphoreType.DMA((blocks,)),
        ],
        [],
        [x, qv_bias, bias, *sources, *(before or ())],
        alias={3 + blocks: 0, 4 + blocks: 1} if aliased else None,
        flops=blocks * (6 * rows * width * part + 8 * heads * rows * slot_rows * 256),
    )


def row_tiles(rows, tile):
    return [pl.ds(start, tile) for start in range(0, rows, tile)]


def ffn_forward_kernel(own_ref, mixed_hbm, x_hbm, wo_hbm, wu_ref, wd_ref, bu_ref, small_ref,
                       u1_hbm, hr_hbm, gr_hbm, gp_hbm, u2_hbm, low_hbm,
                       o_ref, x_ref, wo_ref, u1_ref, hr_ref, gr_ref, gp_ref, u2_ref, low_ref, in_sems, out_sems, g_sems,
                       *, layer, tile, renorm):
    step, steps = pl.program_id(0), pl.num_programs(0)
    part = o_ref.shape[2]
    tiles = row_tiles(x_ref.shape[0], tile)
    wo_copy = pltpu.make_async_copy(wo_hbm.at[layer], wo_ref, in_sems.at[0, 0])
    loads, first_out, last_out = [], [], []
    for t, at in enumerate(tiles):
        loads.append(
            [
                pltpu.make_async_copy(mixed_hbm.at[:, 3, at], o_ref.at[:, at], in_sems.at[1, t]),
                pltpu.make_async_copy(x_hbm.at[at], x_ref.at[at], in_sems.at[2, t]),
            ]
        )
        first_out.append(
            [
                pltpu.make_async_copy(u1_ref.at[at], u1_hbm.at[at], out_sems.at[0, t]),
                pltpu.make_async_copy(hr_ref.at[at], hr_hbm.at[at], out_sems.at[1, t]),
            ]
        )
        last_out.append(
            [
                pltpu.make_async_copy(u2_ref.at[at], u2_hbm.at[at], out_sems.at[2, t]),
                pltpu.make_async_copy(low_ref.at[at], low_hbm.at[at], out_sems.at[3, t]),
            ]
        )

    def g_out(chunk, slot):
        return [
            pltpu.make_async_copy(gr_ref.at[slot], gr_hbm.at[chunk], g_sems.at[0, slot]),
            pltpu.make_async_copy(gp_ref.at[slot], gp_hbm.at[chunk], g_sems.at[1, slot]),
        ]

    @pl.when(step == 0)
    def _():
        wo_copy.start()
        for pair in loads:
            for copy in pair:
                copy.start()
        wo_copy.wait()
        for t, at in enumerate(tiles):
            for copy in loads[t]:
                copy.wait()
            residual = x_ref[at].astype(WIDE)
            if renorm:
                residual = row_stats(residual)[0] * small_ref[6:7] + small_ref[7:8]
            u1 = residual + small_ref[0:1]
            for block in range(4):
                rows = pl.ds(pl.multiple_of((own_ref[0] ^ block) * part, 16), part)
                u1 = u1 + dot_nn(o_ref[block, at], wo_ref[rows, :])
            u1_ref[at] = u1
            normed = row_stats(u1)[0] * small_ref[1:2] + small_ref[2:3]
            hr_ref[at] = normed.astype(LOW)
            u2_ref[at] = normed + small_ref[3:4]
            for copy in first_out[t]:
                copy.start()

    slot = step % 2

    @pl.when(step >= 2)
    def _():
        for copy in g_out(step - 2, slot):
            copy.wait()

    z = dot_nn(hr_ref[...], wu_ref[...]) + bu_ref[...]
    g, slope = gelu_pair(z)
    gr = g.astype(LOW)
    gr_ref[slot] = gr
    gp_ref[slot] = slope.astype(LOW)
    for copy in g_out(step, slot):
        copy.start()
    u2_ref[...] += dot_nn(gr, wd_ref[...])

    @pl.when(step == steps - 1)
    def _():
        for t, at in enumerate(tiles):
            total = u2_ref[at]
            low_ref[at] = (row_stats(total)[0] * small_ref[4:5] + small_ref[5:6]).astype(LOW)
            for copy in last_out[t]:
                copy.start()
        for copy in [*g_out(step - 1, 1 - slot), *g_out(step, slot)]:
            copy.wait()
        for pair in first_out + last_out:
            for copy in pair:
                copy.wait()


def ffn_forward(own, mixed, x, wo, wu, wd, bu, small, layer, renorm, tile=512):
    _, _, rows, part = mixed.shape
    width, hidden = wu.shape[1:]
    chunks = hidden // width
    fixed = lambda v: pl.BlockSpec(v.shape, lambda i, o: (0,) * v.ndim)
    sems = lambda *shape: pltpu.SemaphoreType.DMA(shape)
    return call(
        functools.partial(ffn_forward_kernel, layer=layer, tile=tile, renorm=renorm),
        "ffn_forward",
        (chunks,),
        [
            in_place(),
            in_place(),
            in_place(),
            pl.BlockSpec((None, width, width), lambda i, o: (layer, 0, i)),
            pl.BlockSpec((None, width, width), lambda i, o: (layer, i, 0)),
            pl.BlockSpec((None, 1, width), lambda i, o: (i, 0, 0)),
            fixed(small),
        ],
        [in_place()] * 6,
        [
            shape_of((rows, width), WIDE),
            shape_of((rows, width), LOW),
            shape_of((chunks, rows, width), LOW),
            shape_of((chunks, rows, width), LOW),
            shape_of((rows, width), WIDE),
            shape_of((rows, width), LOW),
        ],
        [
            pltpu.VMEM((4, rows, part), LOW),
            pltpu.VMEM((rows, width), x.dtype),
            pltpu.VMEM((width, width), LOW),
            pltpu.VMEM((rows, width), WIDE),
            pltpu.VMEM((rows, width), LOW),
            pltpu.VMEM((2, rows, width), LOW),
            pltpu.VMEM((2, rows, width), LOW),
            pltpu.VMEM((rows, width), WIDE),
            pltpu.VMEM((rows, width), LOW),
            sems(3, rows // tile),
            sems(4, rows // tile),
            sems(2, 2),
        ],
        [own],
        [mixed, x, wo, wu, wd, bu, small],
        flops=6 * rows * width * (width + 2 * hidden),
    )


def reversed_bits(value, count):
    made = 0
    for bit in range(count):
        made = made | (((value >> bit) & 1) << (count - 1 - bit))
    return made


def row_halves(depth):
    return [(half, slice(half * depth // 2, (half + 1) * depth // 2)) for half in range(2)]


def each_chunk(made, count, half):
    rows = made.shape[0] // count
    for dp in range(count):
        yield half * count + dp, made[dp * rows : (dp + 1) * rows]


def place(dp, own_dp, dp_count):
    away = dp ^ own_dp
    return away & 1, reversed_bits(away >> 1, dp_count.bit_length() - 2)


def ffn_backward_kernel(own_ref, gx_hbm, u2_hbm, u1_hbm, gp_hbm, hr_hbm, gr_hbm, wo_hbm, wu_ref, wd_ref, gain_ref,
                        da_hbm, do_hbm, du_hbm, sums_ref, zsum_ref, send_ref, keep_ref,
                        gx_ref, u2_ref, u1_ref, gp_ref, hr_ref, gr_ref, wo_ref, acc_ref, df_ref, dz_ref, da_ref, do_ref,
                        in_sems, out_sems, g_sems, *, layer, tile, dp_count):
    step, steps = pl.program_id(0), pl.num_programs(0)
    own, own_dp = own_ref[0], own_ref[1]
    part = do_ref.shape[2]
    tiles = row_tiles(gx_ref.shape[0], tile)
    count = len(tiles)
    loads, last_out = [], []
    for t, at in enumerate(tiles):
        loads.append(
            [
                pltpu.make_async_copy(gx_hbm.at[at], gx_ref.at[at], in_sems.at[0, t]),
                pltpu.make_async_copy(u2_hbm.at[at], u2_ref.at[at], in_sems.at[1, t]),
            ]
        )
        last_out.append(
            [
                pltpu.make_async_copy(u2_ref.at[at], du_hbm.at[at], out_sems.at[0, t]),
                pltpu.make_async_copy(da_ref.at[:, at], da_hbm.at[:, at], out_sems.at[1, t]),
                pltpu.make_async_copy(do_ref.at[:, at], do_hbm.at[:, at], out_sems.at[2, t]),
            ]
        )
    hr_copy = pltpu.make_async_copy(hr_hbm, hr_ref, in_sems.at[2, 0])
    u1_copy = pltpu.make_async_copy(u1_hbm, u1_ref, in_sems.at[2, 1])
    wo_copy = pltpu.make_async_copy(wo_hbm.at[layer], wo_ref, in_sems.at[2, 2])

    def streams(at_step):
        slot, head = at_step % 2, own ^ head_order(at_step)
        return (
            pltpu.make_async_copy(gp_hbm.at[head], gp_ref.at[slot], g_sems.at[0, slot]),
            pltpu.make_async_copy(gr_hbm.at[head], gr_ref.at[slot], g_sems.at[1, slot]),
        )

    slot = step % 2
    gp_copy, gr_copy = streams(step)

    @pl.when(step == 0)
    def _():
        for pair in loads:
            for copy in pair:
                copy.start()

        gp_copy.start()
        hr_copy.start()
        gr_copy.start()

    @pl.when(step < steps - 1)
    def _():
        for copy in streams(step + 1):
            copy.start()

    @pl.when(step == 1)
    def _():
        u1_copy.start()
        wo_copy.start()

    @pl.when(step == 0)
    def _():
        sums_ref[...] = jnp.zeros_like(sums_ref)
        for t, at in enumerate(tiles):
            for copy in loads[t]:
                copy.wait()
            gx = gx_ref[at].astype(WIDE)
            xhat, inverse = row_stats(u2_ref[at])
            sums_ref[0:1] += column_sum(gx * xhat)
            sums_ref[1:2] += column_sum(gx)
            gv = norm_backward(gx, xhat, inverse, gain_ref[1:2])
            df = gv.astype(LOW)
            df_ref[at] = df
            sums_ref[2:3] += column_sum(df.astype(WIDE))
            acc_ref[at] = gv

    gp_copy.wait()
    zsum = jnp.zeros(zsum_ref.shape, WIDE)
    for start in range(0, dz_ref.shape[0], 256):
        at = slice(start, start + 256)
        dg = dot_nt(df_ref[at], wd_ref[...])
        dz = (dg * gp_ref[slot, at].astype(WIDE)).astype(LOW)
        dz_ref[at] = dz
        zsum = zsum + column_sum(dz.astype(WIDE))
        acc_ref[at] += dot_nt(dz, wu_ref[...])
    zsum_ref[...] = zsum

    @pl.when(step == 0)
    def _():
        hr_copy.wait()

    gr_copy.wait()
    for out, wanted in ((send_ref, step < 2), (keep_ref, step >= 2)):

        @pl.when(wanted)
        def _():
            for which, (a, b) in enumerate(((hr_ref, dz_ref[...]), (df_ref, gr_ref[slot]))):
                for first, rows in row_halves(hr_ref.shape[1]):
                    made = dot_tn(a[:, rows], b).astype(LOW)
                    for dp, chunk in each_chunk(made, dp_count // 2, first):
                        out[(which, *place(dp, own_dp, dp_count))] = chunk

    @pl.when(step == steps - 1)
    def _():
        u1_copy.wait()
        wo_copy.wait()
        for t, at in enumerate(tiles):
            total = acc_ref[at]
            xhat, inverse = row_stats(u1_ref[at])
            sums_ref[3:4] += column_sum(total * xhat)
            sums_ref[4:5] += column_sum(total)
            du = norm_backward(total, xhat, inverse, gain_ref[0:1])
            u2_ref[at] = du
            da = du.astype(LOW)
            for block in range(4):
                da_ref[block, at] = da[:, block * part : (block + 1) * part]
            sums_ref[5:6] += column_sum(da.astype(WIDE))
            for block in range(4):
                rows = pl.ds(pl.multiple_of((own ^ block) * part, 16), part)
                do_ref[block, at] = dot_nt(da, wo_ref[rows, :]).astype(LOW)
            for copy in last_out[t]:
                copy.start()
        for several in last_out:
            for copy in several:
                copy.wait()


def head_order(step):
    return jnp.where(step < 2, 1 + 2 * step, 2 * (step - 2))


def ffn_backward(own, gx, u2, u1, gp, hr, gr, wo, wu, wd, gains, layer, dp_count, tile=512):
    rows, width = gx.shape
    chunks = gp.shape[0]
    part = width // 4
    chunk_rows = width // dp_count
    rest = dp_count // 2
    fixed = lambda s: pl.BlockSpec(s.shape, lambda i, o: (0,) * len(s.shape))
    head = lambda i, o: o[0] ^ head_order(i)
    block = (2, None, 2, rest, chunk_rows, width)
    sums = shape_of((8, width), WIDE)
    grads = stored((2, 2, 2, rest, chunk_rows, width), LOW)
    sems = lambda *shape: pltpu.SemaphoreType.DMA(shape)
    low = lambda *shape: pltpu.VMEM(shape, LOW)
    wide = lambda *shape: pltpu.VMEM(shape, WIDE)
    return call(
        functools.partial(ffn_backward_kernel, layer=layer, tile=tile, dp_count=dp_count),
        "ffn_backward",
        (chunks,),
        [in_place()] * 7
        + [
            pl.BlockSpec((None, width, width), lambda i, o: (layer, 0, head(i, o))),
            pl.BlockSpec((None, width, width), lambda i, o: (layer, head(i, o), 0)),
            fixed(gains),
        ],
        [
            in_place(),
            in_place(),
            in_place(),
            fixed(sums),
            pl.BlockSpec((None, 1, width), lambda i, o: (head(i, o), 0, 0)),
            pl.BlockSpec(block, lambda i, o: (0, jnp.minimum(i, 1), 0, 0, 0, 0)),
            pl.BlockSpec(block, lambda i, o: (0, jnp.maximum(i - 2, 0), 0, 0, 0, 0)),
        ],
        [
            shape_of((4, rows, part), LOW),
            shape_of((4, rows, part), LOW),
            shape_of((rows, width), WIDE),
            sums,
            shape_of((chunks, 1, width), WIDE),
            grads,
            grads,
        ],
        [
            pltpu.VMEM((rows, width), gx.dtype),
            wide(rows, width),
            wide(rows, width),
            low(2, rows, width),
            low(rows, width),
            low(2, rows, width),
            low(width, width),
            wide(rows, width),
            low(rows, width),
            low(rows, width),
            low(4, rows, part),
            low(4, rows, part),
            sems(3, max(rows // tile, 3)),
            sems(3, rows // tile),
            sems(2, 2),
        ],
        [own],
        [gx, u2, u1, gp, hr, gr, wo, wu, wd, gains],
        flops=4 * rows * width * (width + 4 * chunks * width),
    )


def split_rows(made, half, got_ref, own_dp, dp_count, send_ref, keep_ref):
    for dp, chunk in each_chunk(made, dp_count // 2, half):
        away, rest = place(dp, own_dp, dp_count)
        summed = (chunk + got_ref[away, rest].astype(WIDE)).astype(LOW)

        @pl.when(away == 1)
        def _():
            send_ref[rest] = summed

        @pl.when(away == 0)
        def _():
            keep_ref[rest] = summed


def add_rows(made, half, got_ref, own_dp, dp_count, out_ref):
    for dp, chunk in each_chunk(made, dp_count // 2, half):
        at = place(dp, own_dp, dp_count)
        out_ref[at] = (chunk + got_ref[at].astype(WIDE)).astype(LOW)


def core_add_kernel(kept_ref, got_ref, up_send, up_keep, down_send, down_keep):
    step = pl.program_id(0)

    which, away = step // 2, jnp.where(step < 2, step, 3 - step)

    def summed(at):
        return (kept_ref[at].astype(WIDE) + got_ref[which, away, at].astype(WIDE)).astype(LOW)

    @pl.when(step < 2)
    def _():
        up_keep[...] = summed(0)
        up_send[...] = summed(1)

    for out, wanted in ((down_send, 2), (down_keep, 3)):

        @pl.when(step == wanted)
        def _():
            out[0] = summed(0)
            out[1] = summed(1)


def core_add(kept, got):
    _, _, _, rest, chunk_rows, width = kept.shape

    def at(i):
        return (i // 2, jnp.where(i < 2, i, 3 - i), 0, 0, 0, 0)

    block = pl.BlockSpec((None, None, 2, rest, chunk_rows, width), at)
    up = pl.BlockSpec((None, rest, chunk_rows, width), lambda i: (jnp.minimum(i, 1), 0, 0, 0))
    down = pl.BlockSpec((2, rest, chunk_rows, width), lambda i: (0, 0, 0, 0))
    made = stored((2, rest, chunk_rows, width), LOW)
    return call(
        core_add_kernel,
        "core_add",
        (4,),
        [block, pl.BlockSpec(memory_space=pltpu.VMEM)],
        [up, up, down, down],
        [made] * 4,
        [],
        [],
        [kept, got],
        vmem=24 << 20,
    )


def attention_backward_kernel(own_ref, mixed_ref, do_ref, p_ref, x_ref, o_ref, da_ref, wa_ref, wb_ref, gx_ref, *refs,
                              dp_count, tile, keep):
    if keep:
        got_ref, *refs = refs
    out_ref, sums_ref, *refs = refs
    grads = refs[: 4 if keep else 1]
    t_ref, ds_ref, parts_ref, xt_ref, ot_ref, acc_ref = refs[4 if keep else 1 :]
    slot, block = pl.program_id(0), pl.program_id(1)
    last = pl.num_programs(0) - 1
    own, own_dp = own_ref[0], own_ref[1]
    rows, part = mixed_ref.shape[1:]

    @pl.when((slot == 0) & (block == 0))
    def _():
        xt_ref[...] = x_ref[...].T
        for r in range(4):
            ot_ref[pl.ds(pl.multiple_of((own ^ r) * part, 16), part), :] = o_ref[r].T
        sums_ref[...] = jnp.zeros_like(sums_ref)

    dq = dk = dv = None
    for head, mask in enumerate(head_masks(part)):
        do = pick(mask, do_ref[...])
        t_ref[head] = dot_nt(do, mixed_ref[2])
        for start in range(0, rows, tile):
            at = slice(start, start + tile)
            p = p_ref[head, at].astype(WIDE)
            dp = t_ref[head, at]
            share = jnp.sum(p * dp, axis=1, keepdims=True)
            ds_ref[head, at] = (p * (dp - share)).astype(LOW)
        made = (
            dot_nn(ds_ref[head], pick(mask, mixed_ref[1])),
            dot_tn(ds_ref[head], pick(mask, mixed_ref[0])),
            dot_tn(p_ref[head], do),
        )
        dq, dk, dv = made if dq is None else (dq + made[0], dk + made[1], dv + made[2])
    dq = (dq * HD**-0.5).astype(LOW)
    dk = dk.astype(LOW)
    dv = dv.astype(LOW)
    sums_ref[block, 0:1] += column_sum(dq.astype(WIDE))
    sums_ref[block, 1:2] += column_sum(dv.astype(WIDE))
    joined = jnp.concatenate([dq, dk, dv], axis=1)
    parts_ref[block, pl.ds(pl.multiple_of(slot * rows, rows), rows), :] = joined
    weights = jnp.where(block == 0, wa_ref[...], wb_ref[...])
    passed = dot_nn(joined, weights)

    @pl.when(block == 0)
    def _():
        acc_ref[...] = gx_ref[...] + passed

    @pl.when(block == 1)
    def _():
        out_ref[...] = (acc_ref[...] + passed).astype(out_ref.dtype)

    @pl.when(slot == last)
    def _():
        for half, rows in row_halves(xt_ref.shape[0]):
            first = dot_nn(xt_ref[rows, :], parts_ref[block])
            second = dot_nn(ot_ref[rows, :], da_ref[...])
            made = jnp.concatenate([first, second], axis=1)
            if not keep:
                for dp, chunk in each_chunk(made.astype(LOW), dp_count // 2, half):
                    grads[0][place(dp, own_dp, dp_count)] = chunk
                continue
            cut = made.shape[1] // 2
            a_send, a_keep, b_send, b_keep = grads
            got = [got_ref.at[:, :, :, :cut], got_ref.at[:, :, :, cut:]]
            for where_to, wanted in ((a_keep, 0), (a_send, 1)):

                @pl.when(block == wanted)
                def _():
                    add_rows(made[:, :cut], half, got[0], own_dp, dp_count, where_to)

            split_rows(made[:, cut:], half, got[1], own_dp, dp_count, b_send, b_keep)


def attention_backward(own, mixed, do, probs, x, da, wa, wb, gx, got, dp_count, out_type, tile=64):
    rows, width = x.shape
    part = mixed.shape[3]
    _, slots, heads, slot_rows, _ = probs.shape
    chunk_rows, rest = width // dp_count, dp_count // 2
    keep = got is not None
    away = 0 if keep else 1
    block_of = lambda b: 2 * b + away
    row = pl.BlockSpec((slot_rows, width), lambda s, b, o: (s, 0))
    last = slots - 1
    late = lambda s, b: jnp.where(s == last, b, 0)
    in_specs = [
        pl.BlockSpec((None, 3, slot_rows, part), lambda s, b, o: (block_of(b), 0, s, 0)),
        pl.BlockSpec((None, slot_rows, part), lambda s, b, o: (block_of(b), s, 0)),
        pl.BlockSpec(
            (None, None, heads, slot_rows, slot_rows), lambda s, b, o: (block_of(b), s, 0, 0, 0)
        ),
        whole(x),
        pl.BlockSpec((4, None, rows, part), lambda s, b, o: (0, 3, 0, 0), pipeline_mode=pl.Buffered(1)),
        pl.BlockSpec((None, rows, part), lambda s, b, o: (o[0] ^ block_of(late(s, b)), 0, 0)),
        whole(wa),
        whole(wb),
        row,
    ]
    operands = [mixed, do, probs, x, mixed, da, wa, wb, gx]
    sums = shape_of((2, 8, part), WIDE)
    out_specs = [row, pl.BlockSpec(sums.shape, lambda s, b, o: (0, 0, 0))]
    out_shape = [shape_of((rows, width), out_type), sums]
    whole_block = lambda w: pl.BlockSpec((2, rest, chunk_rows, w), lambda s, b, o: (0, 0, 0, 0))
    if keep:
        in_specs.append(
            pl.BlockSpec(
                (None, 2, rest, chunk_rows, width), lambda s, b, o: (late(s, b), 0, 0, 0, 0)
            )
        )
        operands.append(got)
        half = width // 2
        b_block = pl.BlockSpec(
            (None, rest, chunk_rows, half), lambda s, b, o: (late(s, b), 0, 0, 0)
        )
        out_specs += [whole_block(half)] * 2 + [b_block] * 2
        out_shape += [stored((2, rest, chunk_rows, half), LOW)] * 4
    else:
        out_specs.append(
            pl.BlockSpec(
                (None, 2, rest, chunk_rows, width), lambda s, b, o: (late(s, b), 0, 0, 0, 0)
            )
        )
        out_shape.append(stored((2, 2, rest, chunk_rows, width), LOW))
    return call(
        functools.partial(attention_backward_kernel, dp_count=dp_count, tile=tile, keep=keep),
        "attention_backward",
        (slots, 2),
        in_specs,
        out_specs,
        out_shape,
        [
            pltpu.VMEM((heads, slot_rows, slot_rows), WIDE),
            pltpu.VMEM((heads, slot_rows, slot_rows), LOW),
            pltpu.VMEM((2, rows, 3 * part), LOW),
            pltpu.VMEM((width, rows), LOW),
            pltpu.VMEM((width, rows), LOW),
            pltpu.VMEM((slot_rows, width), WIDE),
        ],
        [own],
        operands,
        flops=36 * heads * rows * slot_rows * 256,
    )


def bits_of(axis):
    size = lax.axis_size(axis)
    return [1 << bit for bit in range(size.bit_length() - 1)]


def swap(value, axis, bit):
    size = lax.axis_size(axis)
    return lax.ppermute(value, axis, [(i, i ^ bit) for i in range(size)])


def add_split_kernel(*refs, merge_in, merge_out, extra, late):
    inputs = 2 if merge_in else 4
    outputs = 2 if merge_out else 4
    ins, refs = refs[:inputs], refs[extra:]
    outs = refs[inputs : inputs + outputs]
    kept_ref, send_ref, keep_ref, in_sems, out_sems = refs[inputs + outputs :]
    half = send_ref.shape[1]
    own, loads, got, stores = [], [], [], []
    for part in range(2):
        kept, came = (ins[0].at[part], ins[1].at[part]) if merge_in else ins[2 * part : 2 * part + 2]
        send, keep = (
            (outs[0].at[part], outs[1].at[part]) if merge_out else outs[2 * part : 2 * part + 2]
        )
        got.append(came)
        if late:
            own.append(kept)
        else:
            own.append(kept_ref.at[part])
            loads.append(pltpu.make_async_copy(kept, kept_ref.at[part], in_sems.at[part]))
        stores.append(
            [
                pltpu.make_async_copy(send_ref.at[part], send, out_sems.at[part, 0]),
                pltpu.make_async_copy(keep_ref.at[part], keep, out_sems.at[part, 1]),
            ]
        )
    for copy in loads:
        copy.start()
    for part in range(2):
        if loads:
            loads[part].wait()
        for at, (out, copy) in enumerate(zip((send_ref, keep_ref), stores[part])):
            rows = pl.ds(half * (1 - at), half)
            out[part] = (own[part][rows].astype(WIDE) + got[part][rows].astype(WIDE)).astype(LOW)
            copy.start()
    for copies in stores:
        for copy in copies:
            copy.wait()


def add_split(ins, merge_in, merge_out, arrived, late):
    size, rows, columns = ins[0].shape[-3:]
    half = (size // 2, rows, columns)
    out_shape = [stored((2, *half), LOW)] * 2 if merge_out else [stored(half, LOW)] * 4
    return pl.pallas_call(
        functools.partial(
            add_split_kernel,
            merge_in=merge_in,
            merge_out=merge_out,
            extra=len(arrived),
            late=late,
        ),
        in_specs=[in_vmem() if late else in_hbm(), in_vmem()] * (len(ins) // 2)
        + [in_place()] * len(arrived),
        out_specs=[in_hbm()] * len(out_shape),
        out_shape=out_shape,
        scratch_shapes=[
            pltpu.VMEM((2, size, rows, columns), LOW),
            pltpu.VMEM((2, *half), LOW),
            pltpu.VMEM((2, *half), LOW),
            pltpu.SemaphoreType.DMA((2,)),
            pltpu.SemaphoreType.DMA((2, 2)),
        ],
        compiler_params=pltpu.CompilerParams(vmem_limit_bytes=16 << 20),
        cost_estimate=pl.CostEstimate(flops=0, bytes_accessed=0, transcendentals=0),
        name="add_split",
    )(*ins, *arrived)


class Summing:
    def __init__(self, a_send, a_keep, b_send, b_keep):
        head, dp = bits_of("head"), bits_of("dp")
        self.stages = [(("dp", dp[0]), ("head", head[1]))] + [(("dp", bit),) for bit in dp[1:]]
        self.at = 0
        self.settled = False
        self.kept = [a_keep, b_keep]
        self.got = [swap(a_send, "head", head[1]), swap(b_send, "dp", dp[0])]

    def busy(self):
        return self.at < len(self.stages)

    def step(self, after, arrived=(), late=False):
        stage = self.stages[self.at]
        merge_in, merge_out = len(self.kept) == 1, len(stage) == 1
        ins = [v for pair in zip(self.kept, self.got) for v in pair]
        lead = 1 if merge_in else 0
        ins = [v.reshape(*v.shape[:lead], -1, *v.shape[-2:]) for v in ins]
        ins, _ = lax.optimization_barrier((ins, after))
        outs = add_split(ins, merge_in, merge_out, arrived, late)
        if merge_out:
            self.got, self.kept = [swap(outs[0], *stage[0])], [outs[1]]
        else:
            self.got = [swap(outs[0], *stage[0]), swap(outs[2], *stage[1])]
            self.kept = [outs[1], outs[3]]
        self.at += 1
        return outs[-1]


def last_sums_kernel(*refs, layers):
    ins, outs = refs[: 4 * layers + 2], refs[4 * layers + 2 :]
    qkv, qv, out_w, out_b, gain1, shift1, up_w, up_b, down_w, down_b, gain2, shift2 = outs
    part = out_w.shape[2]
    width = down_b.shape[1]
    rows = ins[-2][...] + ins[-1][...]
    for layer in range(layers):
        ffn_kept, ffn_got, wide_kept, wide_got = ins[4 * layer : 4 * layer + 4]
        down_w[layer] = ffn_kept[0, 0].astype(WIDE) + ffn_got[0, 0].astype(WIDE)
        up_w[layer] = ffn_kept[1, 0].astype(WIDE) + ffn_got[1, 0].astype(WIDE)
        for half in range(2):
            both = wide_kept[half, 0].astype(WIDE) + wide_got[half, 0].astype(WIDE)
            for at in range(2):
                which = 2 * half + at
                block = both[:, at * part : (at + 1) * part]
                if which < 3:
                    qkv[layer, which] = block
                else:
                    out_w[layer] = block
        for row, out in enumerate((gain2, shift2, down_b, gain1, shift1, out_b)):
            out[layer : layer + 1] = rows[layer, row : row + 1]
        qv[layer] = rows[layer, 6:8]
        for row in range(up_b.shape[1] // width):
            at = slice(row * width, (row + 1) * width)
            up_b[layer : layer + 1, at] = rows[layer, 8 + row : 9 + row]


def last_sums(groups, small, passing):
    layers, _, width = small.shape
    ins, specs = [], []
    for group in groups:
        ins += [group.kept[0], group.got[0]]
    ins = [v.reshape(2, 1, *v.shape[-2:]) for v in ins] + [small, passing]
    rows, part = ins[0].shape[2], ins[2].shape[3] // 2
    hidden = (small.shape[1] - 8) * width
    shapes = [
        (layers, 3, rows, part),
        (layers, 2, width),
        (layers, rows, part),
        (layers, width),
        (layers, width),
        (layers, width),
        (layers, rows, width),
        (layers, hidden),
        (layers, rows, width),
        (layers, width),
        (layers, width),
        (layers, width),
    ]
    spec = lambda shape: pl.BlockSpec(shape, lambda i: (0,) * len(shape))
    specs = [spec(v.shape) for v in ins]
    return call(
        functools.partial(last_sums_kernel, layers=layers),
        "last_sums",
        (1,),
        specs,
        [spec(shape) for shape in shapes],
        [shape_of(shape, WIDE) for shape in shapes],
        [],
        [],
        ins,
        vmem=24 << 20,
    )


def ordered(after, *values):
    values, _ = lax.optimization_barrier((values, after))
    return values


def near_blocks(block, after):
    low, high = bits_of("head")
    near = swap(block, "head", low)
    (later,) = ordered((after, near), block)
    return block, near, swap(later, "head", high)


def gathered_pairs(block, after):
    own, near, far = near_blocks(block, after)
    return jnp.stack([own, near]), jnp.stack([far, swap(far, "head", bits_of("head")[0])])


def on_device(
    tokens,
    seq_lengths,
    qkv_weight,
    qv_bias,
    out_weight,
    out_bias,
    norm1_gain,
    norm1_shift,
    up_weight,
    up_bias,
    down_weight,
    down_bias,
    norm2_gain,
    norm2_shift,
    out_grad,
):
    head_count, dp_count = lax.axis_size("head"), lax.axis_size("dp")
    head_index, dp_index = lax.axis_index("head"), lax.axis_index("dp")
    own = jnp.stack([head_index, dp_index]).astype(jnp.int32)
    local_rows, width = tokens.shape
    slot_rows = local_rows * head_count // seq_lengths.shape[0]
    slots = local_rows // slot_rows
    layers = qkv_weight.shape[0]
    part = width // head_count
    turned = jnp.swapaxes(qkv_weight, 2, 3).reshape(layers, 3 * part, width)
    base = (head_index * slots).astype(jnp.int32).reshape(1)
    bias = mask_bias(seq_lengths, base, slots, slot_rows)
    weights = [near_blocks(turned[0], base)]
    near_bias, far_bias = gathered_pairs(qv_bias[:, :, None], base)
    up_rows = up_bias.reshape(layers, -1, 1, width)
    rounded, residual = tokens, tokens
    kept = []
    for layer in range(layers):
        before = max(layer - 1, 0)
        small = jnp.stack(
            [
                out_bias[layer],
                norm1_gain[layer],
                norm1_shift[layer],
                down_bias[layer],
                norm2_gain[layer],
                norm2_shift[layer],
                norm2_gain[before],
                norm2_shift[before],
            ]
        )
        own_w, near_w, far_w = weights[layer]
        if layer == 0:
            near = attention_forward(rounded, (own_w, near_w), near_bias[:, layer], bias, 0, None)
            (far_w, far_b) = ordered(near[0], far_w, far_bias[:, layer])
            both_w = swap(far_w, "head", bits_of("head")[0])
            for other in range(1, layers):
                (later,) = ordered(near[0], turned[other])
                weights.append(near_blocks(later, near[0]))
            mixed, probs = attention_forward(rounded, (far_w, both_w), far_b, bias, 2, near)
        else:
            both_w = both_ws[layer - 1]
            all_bias = jnp.concatenate([near_bias[:, layer], far_bias[:, layer]])
            mixed, probs = attention_forward(
                rounded, (own_w, near_w, far_w, both_w), all_bias, bias, 0, None
            )
        weights[layer] = w = (own_w, near_w, far_w, both_w)
        u1, hr, gr, slope, u2, low = ffn_forward(
            own,
            mixed,
            residual,
            out_weight,
            up_weight,
            down_weight,
            up_rows[layer],
            small,
            layer,
            layer > 0,
        )
        kept.append((rounded, mixed, probs, u1, hr, gr, slope, u2))
        rounded, residual = low, u2
        if layer == 0:
            (far_ws,) = ordered(u2, [w[2] for w in weights[1:]])
            both_ws = [swap(w, "head", bits_of("head")[0]) for w in far_ws]
    out_state = rounded
    grad_state = out_grad
    small_sums = [None] * layers
    hidden_sums = [None] * layers
    ffn_groups, wide_groups = [None] * layers, [None] * layers
    running = []

    def advance(after, late=False):
        arrived = []
        for group in running:
            if not group.busy() and not group.settled:
                arrived += group.got
                group.settled = True
        for group in running:
            if group.busy():
                after = group.step(after, arrived, late)
                arrived = []
        return after

    for layer in reversed(range(layers)):
        rounded, mixed, probs, u1, hr, gr, slope, u2 = kept[layer]
        w = weights[layer]
        gains = jnp.stack([norm1_gain[layer], norm2_gain[layer]])
        da, do, du, sums, zsums, sent, ffn_kept = ffn_backward(
            own,
            grad_state,
            u2,
            u1,
            slope,
            hr,
            gr,
            out_weight,
            up_weight,
            down_weight,
            gains,
            layer,
            dp_count,
        )
        low_bit = bits_of("head")[0]
        early = bool(running)
        token = advance(do)
        if early:
            (sent,) = ordered(token, sent)
        got = swap(sent, "head", low_bit)

        def sum_ffn(after):
            values = ordered(after, ffn_kept, got)
            up_send, up_keep, down_send, down_keep = core_add(*values)
            ffn_groups[layer] = Summing(down_send, down_keep, up_send, up_keep)
            running.insert(0, ffn_groups[layer])
            return down_keep

        if early:
            token = sum_ffn(token)
        (do, du) = ordered(token, do, du)
        half_grad, away_sums, sent = attention_backward(
            own, mixed, do, probs, rounded, da, w[1], w[3], du, None, dp_count, WIDE
        )
        if early:
            token = advance(half_grad)
            (sent,) = ordered(token, sent)
            wide_got = swap(sent, "head", low_bit)
        else:
            wide_got = swap(sent, "head", low_bit)
            token = sum_ffn(half_grad)
        (half_grad, do) = ordered(token, half_grad, do)
        grad_state, own_sums, *parts = attention_backward(
            own,
            mixed,
            do,
            probs,
            rounded,
            da,
            w[0],
            w[2],
            half_grad,
            wide_got,
            dp_count,
            WIDE if layer else LOW,
        )
        wide_groups[layer] = Summing(*parts)
        token = advance(grad_state) if layer else grad_state
        if layer:
            (grad_state,) = ordered(token, grad_state)
        running.append(wide_groups[layer])
        blocks = [own_sums[0], away_sums[0], own_sums[1], away_sums[1]]
        stacked = jnp.stack(blocks)[:, :2]
        qv_sums = jnp.concatenate(
            [
                lax.dynamic_index_in_dim(stacked, head_index ^ head, 0, keepdims=False)
                for head in range(head_count)
            ],
            axis=1,
        )
        small_sums[layer] = jnp.concatenate([sums[:6], qv_sums, zsums[:, 0]])
    small_sum = jnp.stack(small_sums)
    near, far = bits_of("head")
    waiting = [[("head", near)], [("dp", 1)], [("head", far)], [("dp", 2 * k) for k in range(1, dp_count // 2)]]
    passing = [swap(small_sum, *one) for one in waiting.pop(0)]
    while any(not group.settled for group in running) or waiting:
        if any(group.busy() for group in running):
            token = advance(token, True)
        elif not waiting:
            break
        if waiting:
            small_sum, passing = ordered(token, small_sum, passing)
            small_sum = sum(passing, small_sum)
            token = small_sum
            passing = [swap(small_sum, *one) for one in waiting.pop(0)]
    small_sum, passing = sum(passing[:-1], small_sum), passing[-1]
    groups = [group for pair in zip(ffn_groups, wide_groups) for group in pair]
    qkv, qv, out_w, out_b, gain1, shift1, up_w, up_b, down_w, down_b, gain2, shift2 = last_sums(
        groups, small_sum, passing
    )
    return (
        out_state,
        grad_state,
        qkv,
        qv,
        out_w,
        out_b,
        gain1,
        shift1,
        up_w,
        up_b,
        jnp.swapaxes(down_w, 1, 2),
        down_b,
        gain2,
        shift2,
    )


def solution(mesh):
    in_specs = (
        P(("dp", "head"), None),
        P("dp", None),
        P(None, None, None, "head"),
        P(None, None, "head"),
        P(),
        P(),
        P(),
        P(),
        P(),
        P(),
        P(),
        P(),
        P(),
        P(),
        P(("dp", "head"), None),
    )
    out_specs = (
        P(("dp", "head"), None),
        P(("dp", "head"), None),
        P(None, None, "dp", "head"),
        P(),
        P(None, "dp", "head"),
        P(),
        P(),
        P(),
        P(None, "dp", "head"),
        P(),
        P(None, "head", "dp"),
        P(),
        P(),
        P(),
    )
    return jax.shard_map(
        on_device, mesh=mesh, in_specs=in_specs, out_specs=out_specs, check_vma=False
    )
```

```python
import functools
import math

import jax
import jax.numpy as jnp
from jax import lax
from jax.experimental import pallas as pl
from jax.experimental.pallas import tpu as pltpu
from jax.sharding import PartitionSpec as P

HD = 64
EPSILON = 1e-06
LOW = jnp.bfloat16
WIDE = jnp.float32
VMEM_BYTES = 58 << 20
ROOT_HALF = 0.7071067811865476
INV_ROOT_TAU = 0.3989422804014327
FAR = -1e30


def row_stats(values):
    centre = jnp.mean(values, axis=-1, keepdims=True)
    centred = values - centre
    spread = jnp.mean(centred * centred, axis=-1, keepdims=True)
    inverse = lax.rsqrt(spread + EPSILON)
    return centred * inverse, inverse


def norm_backward(upstream, xhat, inverse, gain):
    scaled = upstream * gain
    first = jnp.mean(scaled, axis=-1, keepdims=True)
    second = jnp.mean(scaled * xhat, axis=-1, keepdims=True)
    return (scaled - first - xhat * second) * inverse


def column_sum(values):
    return jnp.sum(values, axis=0, keepdims=True)


def dot_nn(left, right):
    return jnp.dot(left, right, preferred_element_type=WIDE)


def dot_nt(left, right):
    return lax.dot_general(left, right, (((1,), (1,)), ((), ())), preferred_element_type=WIDE)


def dot_tn(left, right):
    return lax.dot_general(left, right, (((0,), (0,)), ((), ())), preferred_element_type=WIDE)


def gelu_pair(z):
    cdf = 0.5 + 0.5 * lax.erf(z * ROOT_HALF)
    return z * cdf, cdf + z * (jnp.exp(z * z * -0.5) * INV_ROOT_TAU)


def pick(mask, values):
    return jnp.where(mask, values, jnp.zeros_like(values))


def head_masks(width):
    lanes = lax.broadcasted_iota(jnp.int32, (1, width), 1) // HD
    return [lanes == head for head in range(width // HD)]


def params():
    return pltpu.CompilerParams(vmem_limit_bytes=VMEM_BYTES)


def whole(array):
    return pl.BlockSpec(array.shape, lambda *ids: (0,) * array.ndim, pipeline_mode=pl.Buffered(1))


def in_place():
    return pl.BlockSpec(memory_space=pl.ANY)


def in_vmem():
    return pl.BlockSpec(memory_space=pltpu.VMEM)


def in_hbm():
    return pl.BlockSpec(memory_space=pltpu.HBM)


def shape_of(shape, kind):
    return jax.ShapeDtypeStruct(shape, kind)


def cost(flops, out_shape, operands):
    if not flops:
        return pl.CostEstimate(flops=0, bytes_accessed=0, transcendentals=0)
    made = out_shape if isinstance(out_shape, (list, tuple)) else [out_shape]
    moved = sum(math.prod(v.shape) * jnp.dtype(v.dtype).itemsize for v in [*made, *operands])
    return pl.CostEstimate(flops=flops, bytes_accessed=moved, transcendentals=0)


def stored(shape, kind):
    return pltpu.HBM(shape, kind)


def call(kernel, name, grid, in_specs, out_specs, out_shape, scratch, scalars, operands, alias=None, flops=0, vmem=VMEM_BYTES):
    return pl.pallas_call(
        kernel,
        grid_spec=pltpu.PrefetchScalarGridSpec(
            num_scalar_prefetch=len(scalars),
            grid=grid,
            in_specs=in_specs,
            out_specs=out_specs,
            scratch_shapes=scratch,
        ),
        out_shape=out_shape,
        compiler_params=pltpu.CompilerParams(vmem_limit_bytes=vmem),
        input_output_aliases=alias or {},
        cost_estimate=cost(flops, out_shape, operands),
        name=name,
    )(*scalars, *operands)


def mask_kernel(base_ref, lengths_ref, bias_ref):
    slots, rows, _ = bias_ref.shape
    across = lax.broadcasted_iota(jnp.int32, (8, rows), 1)
    down = lax.broadcasted_iota(jnp.int32, (rows, 128), 0)
    for slot in range(slots):
        reach = jnp.int32(0)
        seg_across = jnp.zeros((8, rows), jnp.int32)
        seg_down = jnp.zeros((rows, 128), jnp.int32)
        for k in range(lengths_ref.shape[1]):
            reach = reach + lengths_ref[base_ref[0] + slot, k]
            seg_across += (across >= reach).astype(jnp.int32)
            seg_down += (down >= reach).astype(jnp.int32)
        inside = seg_down[:, 0:1] == seg_across[0:1, :]
        bias_ref[slot] = jnp.where(inside, 0.0, FAR)


def mask_bias(lengths, base, slots, slot_rows):
    smem = pl.BlockSpec(memory_space=pltpu.SMEM)
    return pl.pallas_call(
        mask_kernel,
        in_specs=[smem, smem],
        out_shape=shape_of((slots, slot_rows, slot_rows), WIDE),
        compiler_params=params(),
        name="mask_bias",
    )(base, lengths)


def attention_forward_kernel(x_ref, b_ref, bias_ref, *refs, blocks, aliased, tile):
    sources = refs[:blocks]
    mixed_ref, p_ref, s_ref, w_ref, sems = refs[blocks + 2 * aliased :]
    rows, part = x_ref.shape[0], w_ref.shape[1] // 3
    slot, block = pl.program_id(0), pl.program_id(1)
    copies = [pltpu.make_async_copy(w, w_ref.at[b], sems.at[b]) for b, w in enumerate(sources)]

    @pl.when((slot == 0) & (block == 0))
    def _():
        for copy in copies:
            copy.start()

    for b, copy in enumerate(copies):

        @pl.when((slot == 0) & (block == b))
        def _():
            copy.wait()

    x = x_ref[...]
    q = ((dot_nt(x, w_ref[block, :part]) + b_ref[0]).astype(LOW) * HD**-0.5).astype(LOW)
    k = dot_nt(x, w_ref[block, part : 2 * part]).astype(LOW)
    v = (dot_nt(x, w_ref[block, 2 * part :]) + b_ref[1]).astype(LOW)
    mixed_ref[0] = q
    mixed_ref[1] = k
    mixed_ref[2] = v
    total = None
    for head, mask in enumerate(head_masks(part)):
        s_ref[head] = dot_nt(pick(mask, q), k)
        for start in range(0, rows, tile):
            at = slice(start, start + tile)
            s = s_ref[head, at] + bias_ref[at]
            e = jnp.exp(s - jnp.max(s, axis=1, keepdims=True))
            p_ref[head, at] = (e * (1.0 / jnp.sum(e, axis=1, keepdims=True))).astype(LOW)
        made = dot_nn(p_ref[head], pick(mask, v))
        total = made if total is None else total + made
    mixed_ref[3] = total.astype(LOW)


def attention_forward(x, sources, qv_bias, bias, first, before, tile=64):
    rows, width = x.shape
    slots, slot_rows, _ = bias.shape
    blocks = len(sources)
    part = sources[0].shape[0] // 3
    heads = part // HD
    aliased = int(before is not None)
    mixed = shape_of((4, 4, rows, part), LOW)
    probs = shape_of((4, slots, heads, slot_rows, slot_rows), LOW)
    return call(
        functools.partial(attention_forward_kernel, blocks=blocks, aliased=aliased, tile=tile),
        "attention_forward",
        (slots, blocks),
        [
            pl.BlockSpec((slot_rows, width), lambda s, b: (s, 0)),
            pl.BlockSpec((None, 2, 1, part), lambda s, b: (b, 0, 0, 0)),
            pl.BlockSpec((None, slot_rows, slot_rows), lambda s, b: (s, 0, 0)),
        ]
        + [in_place()] * (blocks + 2 * aliased),
        [
            pl.BlockSpec((None, 4, slot_rows, part), lambda s, b: (first + b, 0, s, 0)),
            pl.BlockSpec(
                (None, None, heads, slot_rows, slot_rows), lambda s, b: (first + b, s, 0, 0, 0)
            ),
        ],
        [mixed, probs],
        [
            pltpu.VMEM((heads, slot_rows, slot_rows), WIDE),
            pltpu.VMEM((blocks, 3 * part, width), LOW),
            pltpu.SemaphoreType.DMA((blocks,)),
        ],
        [],
        [x, qv_bias, bias, *sources, *(before or ())],
        alias={3 + blocks: 0, 4 + blocks: 1} if aliased else None,
        flops=blocks * (6 * rows * width * part + 8 * heads * rows * slot_rows * 256),
    )


def row_tiles(rows, tile):
    return [pl.ds(start, tile) for start in range(0, rows, tile)]


def ffn_forward_kernel(own_ref, mixed_hbm, x_hbm, wo_hbm, wu_ref, wd_ref, bu_ref, small_ref,
                       u1_hbm, hr_hbm, gr_hbm, gp_hbm, u2_hbm, low_hbm,
                       o_ref, x_ref, wo_ref, u1_ref, hr_ref, gr_ref, gp_ref, u2_ref, low_ref, in_sems, out_sems, g_sems,
                       *, layer, tile, renorm):
    step, steps = pl.program_id(0), pl.num_programs(0)
    part = o_ref.shape[2]
    tiles = row_tiles(x_ref.shape[0], tile)
    wo_copy = pltpu.make_async_copy(wo_hbm.at[layer], wo_ref, in_sems.at[0, 0])
    loads, first_out, last_out = [], [], []
    for t, at in enumerate(tiles):
        loads.append(
            [
                pltpu.make_async_copy(mixed_hbm.at[:, 3, at], o_ref.at[:, at], in_sems.at[1, t]),
                pltpu.make_async_copy(x_hbm.at[at], x_ref.at[at], in_sems.at[2, t]),
            ]
        )
        first_out.append(
            [
                pltpu.make_async_copy(u1_ref.at[at], u1_hbm.at[at], out_sems.at[0, t]),
                pltpu.make_async_copy(hr_ref.at[at], hr_hbm.at[at], out_sems.at[1, t]),
            ]
        )
        last_out.append(
            [
                pltpu.make_async_copy(u2_ref.at[at], u2_hbm.at[at], out_sems.at[2, t]),
                pltpu.make_async_copy(low_ref.at[at], low_hbm.at[at], out_sems.at[3, t]),
            ]
        )

    def g_out(chunk, slot):
        return [
            pltpu.make_async_copy(gr_ref.at[slot], gr_hbm.at[chunk], g_sems.at[0, slot]),
            pltpu.make_async_copy(gp_ref.at[slot], gp_hbm.at[chunk], g_sems.at[1, slot]),
        ]

    @pl.when(step == 0)
    def _():
        wo_copy.start()
        for pair in loads:
            for copy in pair:
                copy.start()
        wo_copy.wait()
        for t, at in enumerate(tiles):
            for copy in loads[t]:
                copy.wait()
            residual = x_ref[at].astype(WIDE)
            if renorm:
                residual = row_stats(residual)[0] * small_ref[6:7] + small_ref[7:8]
            u1 = residual + small_ref[0:1]
            for block in range(4):
                rows = pl.ds(pl.multiple_of((own_ref[0] ^ block) * part, 16), part)
                u1 = u1 + dot_nn(o_ref[block, at], wo_ref[rows, :])
            u1_ref[at] = u1
            normed = row_stats(u1)[0] * small_ref[1:2] + small_ref[2:3]
            hr_ref[at] = normed.astype(LOW)
            u2_ref[at] = normed + small_ref[3:4]
            for copy in first_out[t]:
                copy.start()

    slot = step % 2

    @pl.when(step >= 2)
    def _():
        for copy in g_out(step - 2, slot):
            copy.wait()

    z = dot_nn(hr_ref[...], wu_ref[...]) + bu_ref[...]
    g, slope = gelu_pair(z)
    gr = g.astype(LOW)
    gr_ref[slot] = gr
    gp_ref[slot] = slope.astype(LOW)
    for copy in g_out(step, slot):
        copy.start()
    u2_ref[...] += dot_nn(gr, wd_ref[...])

    @pl.when(step == steps - 1)
    def _():
        for t, at in enumerate(tiles):
            total = u2_ref[at]
            low_ref[at] = (row_stats(total)[0] * small_ref[4:5] + small_ref[5:6]).astype(LOW)
            for copy in last_out[t]:
                copy.start()
        for copy in [*g_out(step - 1, 1 - slot), *g_out(step, slot)]:
            copy.wait()
        for pair in first_out + last_out:
            for copy in pair:
                copy.wait()


def ffn_forward(own, mixed, x, wo, wu, wd, bu, small, layer, renorm, tile=1024):
    _, _, rows, part = mixed.shape
    width, hidden = wu.shape[1:]
    chunks = hidden // width
    fixed = lambda v: pl.BlockSpec(v.shape, lambda i, o: (0,) * v.ndim)
    sems = lambda *shape: pltpu.SemaphoreType.DMA(shape)
    return call(
        functools.partial(ffn_forward_kernel, layer=layer, tile=tile, renorm=renorm),
        "ffn_forward",
        (chunks,),
        [
            in_place(),
            in_place(),
            in_place(),
            pl.BlockSpec((None, width, width), lambda i, o: (layer, 0, i)),
            pl.BlockSpec((None, width, width), lambda i, o: (layer, i, 0)),
            pl.BlockSpec((None, 1, width), lambda i, o: (i, 0, 0)),
            fixed(small),
        ],
        [in_place()] * 6,
        [
            shape_of((rows, width), WIDE),
            shape_of((rows, width), LOW),
            shape_of((chunks, rows, width), LOW),
            shape_of((chunks, rows, width), LOW),
            shape_of((rows, width), WIDE),
            shape_of((rows, width), LOW),
        ],
        [
            pltpu.VMEM((4, rows, part), LOW),
            pltpu.VMEM((rows, width), x.dtype),
            pltpu.VMEM((width, width), LOW),
            pltpu.VMEM((rows, width), WIDE),
            pltpu.VMEM((rows, width), LOW),
            pltpu.VMEM((2, rows, width), LOW),
            pltpu.VMEM((2, rows, width), LOW),
            pltpu.VMEM((rows, width), WIDE),
            pltpu.VMEM((rows, width), LOW),
            sems(3, rows // tile),
            sems(4, rows // tile),
            sems(2, 2),
        ],
        [own],
        [mixed, x, wo, wu, wd, bu, small],
        flops=6 * rows * width * (width + 2 * hidden),
    )


def reversed_bits(value, count):
    made = 0
    for bit in range(count):
        made = made | (((value >> bit) & 1) << (count - 1 - bit))
    return made


def row_halves(depth):
    return [(half, slice(half * depth // 2, (half + 1) * depth // 2)) for half in range(2)]


def each_chunk(made, count, half):
    rows = made.shape[0] // count
    for dp in range(count):
        yield half * count + dp, made[dp * rows : (dp + 1) * rows]


def place(dp, own_dp, dp_count):
    away = dp ^ own_dp
    return away & 1, reversed_bits(away >> 1, dp_count.bit_length() - 2)


def ffn_backward_kernel(own_ref, gx_hbm, u2_hbm, u1_hbm, gp_hbm, hr_hbm, gr_hbm, wo_hbm, wu_ref, wd_ref, gain_ref,
                        da_hbm, do_hbm, du_hbm, sums_ref, zsum_ref, send_ref, keep_ref,
                        gx_ref, u2_ref, u1_ref, gp_ref, hr_ref, gr_ref, wo_ref, acc_ref, df_ref, dz_ref, da_ref, do_ref,
                        in_sems, out_sems, g_sems, *, layer, tile, dp_count):
    step, steps = pl.program_id(0), pl.num_programs(0)
    own, own_dp = own_ref[0], own_ref[1]
    part = do_ref.shape[2]
    tiles = row_tiles(gx_ref.shape[0], tile)
    count = len(tiles)
    loads, last_out = [], []
    for t, at in enumerate(tiles):
        loads.append(
            [
                pltpu.make_async_copy(gx_hbm.at[at], gx_ref.at[at], in_sems.at[0, t]),
                pltpu.make_async_copy(u2_hbm.at[at], u2_ref.at[at], in_sems.at[1, t]),
            ]
        )
        last_out.append(
            [
                pltpu.make_async_copy(u2_ref.at[at], du_hbm.at[at], out_sems.at[0, t]),
                pltpu.make_async_copy(da_ref.at[:, at], da_hbm.at[:, at], out_sems.at[1, t]),
                pltpu.make_async_copy(do_ref.at[:, at], do_hbm.at[:, at], out_sems.at[2, t]),
            ]
        )
    hr_copy = pltpu.make_async_copy(hr_hbm, hr_ref, in_sems.at[2, 0])
    u1_copy = pltpu.make_async_copy(u1_hbm, u1_ref, in_sems.at[2, 1])
    wo_copy = pltpu.make_async_copy(wo_hbm.at[layer], wo_ref, in_sems.at[2, 2])

    def streams(at_step):
        slot, head = at_step % 2, own ^ head_order(at_step)
        return (
            pltpu.make_async_copy(gp_hbm.at[head], gp_ref.at[slot], g_sems.at[0, slot]),
            pltpu.make_async_copy(gr_hbm.at[head], gr_ref.at[slot], g_sems.at[1, slot]),
        )

    slot = step % 2
    gp_copy, gr_copy = streams(step)

    @pl.when(step == 0)
    def _():
        for pair in loads:
            for copy in pair:
                copy.start()

        gp_copy.start()
        hr_copy.start()
        gr_copy.start()

    @pl.when(step < steps - 1)
    def _():
        for copy in streams(step + 1):
            copy.start()

    @pl.when(step == 1)
    def _():
        u1_copy.start()
        wo_copy.start()

    @pl.when(step == 0)
    def _():
        sums_ref[...] = jnp.zeros_like(sums_ref)
        for t, at in enumerate(tiles):
            for copy in loads[t]:
                copy.wait()
            gx = gx_ref[at].astype(WIDE)
            xhat, inverse = row_stats(u2_ref[at])
            sums_ref[0:1] += column_sum(gx * xhat)
            sums_ref[1:2] += column_sum(gx)
            gv = norm_backward(gx, xhat, inverse, gain_ref[1:2])
            df = gv.astype(LOW)
            df_ref[at] = df
            sums_ref[2:3] += column_sum(df.astype(WIDE))
            acc_ref[at] = gv

    gp_copy.wait()
    zsum = jnp.zeros(zsum_ref.shape, WIDE)
    for start in range(0, dz_ref.shape[0], 256):
        at = slice(start, start + 256)
        dg = dot_nt(df_ref[at], wd_ref[...])
        dz = (dg * gp_ref[slot, at].astype(WIDE)).astype(LOW)
        dz_ref[at] = dz
        zsum = zsum + column_sum(dz.astype(WIDE))
        acc_ref[at] += dot_nt(dz, wu_ref[...])
    zsum_ref[...] = zsum

    @pl.when(step == 0)
    def _():
        hr_copy.wait()

    gr_copy.wait()
    for out, wanted in ((send_ref, step < 2), (keep_ref, step >= 2)):

        @pl.when(wanted)
        def _():
            for which, (a, b) in enumerate(((hr_ref, dz_ref[...]), (df_ref, gr_ref[slot]))):
                for first, rows in row_halves(hr_ref.shape[1]):
                    made = dot_tn(a[:, rows], b).astype(LOW)
                    for dp, chunk in each_chunk(made, dp_count // 2, first):
                        out[(which, *place(dp, own_dp, dp_count))] = chunk

    @pl.when(step == steps - 1)
    def _():
        u1_copy.wait()
        wo_copy.wait()
        for t, at in enumerate(tiles):
            total = acc_ref[at]
            xhat, inverse = row_stats(u1_ref[at])
            sums_ref[3:4] += column_sum(total * xhat)
            sums_ref[4:5] += column_sum(total)
            du = norm_backward(total, xhat, inverse, gain_ref[0:1])
            u2_ref[at] = du
            da = du.astype(LOW)
            for block in range(4):
                da_ref[block, at] = da[:, block * part : (block + 1) * part]
            sums_ref[5:6] += column_sum(da.astype(WIDE))
            for block in range(4):
                rows = pl.ds(pl.multiple_of((own ^ block) * part, 16), part)
                do_ref[block, at] = dot_nt(da, wo_ref[rows, :]).astype(LOW)
            for copy in last_out[t]:
                copy.start()
        for several in last_out:
            for copy in several:
                copy.wait()


def head_order(step):
    return jnp.where(step < 2, 1 + 2 * step, 2 * (step - 2))


def ffn_backward(own, gx, u2, u1, gp, hr, gr, wo, wu, wd, gains, layer, dp_count, tile=512):
    rows, width = gx.shape
    chunks = gp.shape[0]
    part = width // 4
    chunk_rows = width // dp_count
    rest = dp_count // 2
    fixed = lambda s: pl.BlockSpec(s.shape, lambda i, o: (0,) * len(s.shape))
    head = lambda i, o: o[0] ^ head_order(i)
    block = (2, None, 2, rest, chunk_rows, width)
    sums = shape_of((8, width), WIDE)
    grads = stored((2, 2, 2, rest, chunk_rows, width), LOW)
    sems = lambda *shape: pltpu.SemaphoreType.DMA(shape)
    low = lambda *shape: pltpu.VMEM(shape, LOW)
    wide = lambda *shape: pltpu.VMEM(shape, WIDE)
    return call(
        functools.partial(ffn_backward_kernel, layer=layer, tile=tile, dp_count=dp_count),
        "ffn_backward",
        (chunks,),
        [in_place()] * 7
        + [
            pl.BlockSpec((None, width, width), lambda i, o: (layer, 0, head(i, o))),
            pl.BlockSpec((None, width, width), lambda i, o: (layer, head(i, o), 0)),
            fixed(gains),
        ],
        [
            in_place(),
            in_place(),
            in_place(),
            fixed(sums),
            pl.BlockSpec((None, 1, width), lambda i, o: (head(i, o), 0, 0)),
            pl.BlockSpec(block, lambda i, o: (0, jnp.minimum(i, 1), 0, 0, 0, 0)),
            pl.BlockSpec(block, lambda i, o: (0, jnp.maximum(i - 2, 0), 0, 0, 0, 0)),
        ],
        [
            shape_of((4, rows, part), LOW),
            shape_of((4, rows, part), LOW),
            shape_of((rows, width), WIDE),
            sums,
            shape_of((chunks, 1, width), WIDE),
            grads,
            grads,
        ],
        [
            pltpu.VMEM((rows, width), gx.dtype),
            wide(rows, width),
            wide(rows, width),
            low(2, rows, width),
            low(rows, width),
            low(2, rows, width),
            low(width, width),
            wide(rows, width),
            low(rows, width),
            low(rows, width),
            low(4, rows, part),
            low(4, rows, part),
            sems(3, max(rows // tile, 3)),
            sems(3, rows // tile),
            sems(2, 2),
        ],
        [own],
        [gx, u2, u1, gp, hr, gr, wo, wu, wd, gains],
        flops=4 * rows * width * (width + 4 * chunks * width),
    )


def split_rows(made, half, got_ref, own_dp, dp_count, send_ref, keep_ref):
    for dp, chunk in each_chunk(made, dp_count // 2, half):
        away, rest = place(dp, own_dp, dp_count)
        summed = (chunk + got_ref[away, rest].astype(WIDE)).astype(LOW)

        @pl.when(away == 1)
        def _():
            send_ref[rest] = summed

        @pl.when(away == 0)
        def _():
            keep_ref[rest] = summed


def add_rows(made, half, got_ref, own_dp, dp_count, out_ref):
    for dp, chunk in each_chunk(made, dp_count // 2, half):
        at = place(dp, own_dp, dp_count)
        out_ref[at] = (chunk + got_ref[at].astype(WIDE)).astype(LOW)


def core_add_kernel(kept_ref, got_ref, up_send, up_keep, down_send, down_keep):
    step = pl.program_id(0)

    which, away = step // 2, jnp.where(step < 2, step, 3 - step)

    def summed(at):
        return (kept_ref[at].astype(WIDE) + got_ref[which, away, at].astype(WIDE)).astype(LOW)

    @pl.when(step < 2)
    def _():
        up_keep[...] = summed(0)
        up_send[...] = summed(1)

    for out, wanted in ((down_send, 2), (down_keep, 3)):

        @pl.when(step == wanted)
        def _():
            out[0] = summed(0)
            out[1] = summed(1)


def core_add(kept, got):
    _, _, _, rest, chunk_rows, width = kept.shape

    def at(i):
        return (i // 2, jnp.where(i < 2, i, 3 - i), 0, 0, 0, 0)

    block = pl.BlockSpec((None, None, 2, rest, chunk_rows, width), at)
    up = pl.BlockSpec((None, rest, chunk_rows, width), lambda i: (jnp.minimum(i, 1), 0, 0, 0))
    down = pl.BlockSpec((2, rest, chunk_rows, width), lambda i: (0, 0, 0, 0))
    made = stored((2, rest, chunk_rows, width), LOW)
    return call(
        core_add_kernel,
        "core_add",
        (4,),
        [block, pl.BlockSpec(memory_space=pltpu.VMEM)],
        [up, up, down, down],
        [made] * 4,
        [],
        [],
        [kept, got],
        vmem=24 << 20,
    )


def attention_backward_kernel(own_ref, mixed_ref, do_ref, p_ref, x_ref, o_ref, da_ref, wa_ref, wb_ref, gx_ref, *refs,
                              dp_count, tile, keep):
    if keep:
        got_ref, *refs = refs
    out_ref, sums_ref, *refs = refs
    grads = refs[: 4 if keep else 1]
    t_ref, ds_ref, parts_ref, xt_ref, ot_ref, acc_ref = refs[4 if keep else 1 :]
    slot, block = pl.program_id(0), pl.program_id(1)
    last = pl.num_programs(0) - 1
    own, own_dp = own_ref[0], own_ref[1]
    rows, part = mixed_ref.shape[1:]

    @pl.when((slot == 0) & (block == 0))
    def _():
        xt_ref[...] = x_ref[...].T
        for r in range(4):
            ot_ref[pl.ds(pl.multiple_of((own ^ r) * part, 16), part), :] = o_ref[r].T
        sums_ref[...] = jnp.zeros_like(sums_ref)

    dq = dk = dv = None
    for head, mask in enumerate(head_masks(part)):
        do = pick(mask, do_ref[...])
        t_ref[head] = dot_nt(do, mixed_ref[2])
        for start in range(0, rows, tile):
            at = slice(start, start + tile)
            p = p_ref[head, at].astype(WIDE)
            dp = t_ref[head, at]
            share = jnp.sum(p * dp, axis=1, keepdims=True)
            ds_ref[head, at] = (p * (dp - share)).astype(LOW)
        made = (
            dot_nn(ds_ref[head], pick(mask, mixed_ref[1])),
            dot_tn(ds_ref[head], pick(mask, mixed_ref[0])),
            dot_tn(p_ref[head], do),
        )
        dq, dk, dv = made if dq is None else (dq + made[0], dk + made[1], dv + made[2])
    dq = (dq * HD**-0.5).astype(LOW)
    dk = dk.astype(LOW)
    dv = dv.astype(LOW)
    sums_ref[block, 0:1] += column_sum(dq.astype(WIDE))
    sums_ref[block, 1:2] += column_sum(dv.astype(WIDE))
    joined = jnp.concatenate([dq, dk, dv], axis=1)
    parts_ref[block, pl.ds(pl.multiple_of(slot * rows, rows), rows), :] = joined
    weights = jnp.where(block == 0, wa_ref[...], wb_ref[...])
    passed = dot_nn(joined, weights)

    @pl.when(block == 0)
    def _():
        acc_ref[...] = gx_ref[...] + passed

    @pl.when(block == 1)
    def _():
        out_ref[...] = (acc_ref[...] + passed).astype(out_ref.dtype)

    @pl.when(slot == last)
    def _():
        for half, rows in row_halves(xt_ref.shape[0]):
            first = dot_nn(xt_ref[rows, :], parts_ref[block])
            second = dot_nn(ot_ref[rows, :], da_ref[...])
            made = jnp.concatenate([first, second], axis=1)
            if not keep:
                for dp, chunk in each_chunk(made.astype(LOW), dp_count // 2, half):
                    grads[0][place(dp, own_dp, dp_count)] = chunk
                continue
            cut = made.shape[1] // 2
            a_send, a_keep, b_send, b_keep = grads
            got = [got_ref.at[:, :, :, :cut], got_ref.at[:, :, :, cut:]]
            for where_to, wanted in ((a_keep, 0), (a_send, 1)):

                @pl.when(block == wanted)
                def _():
                    add_rows(made[:, :cut], half, got[0], own_dp, dp_count, where_to)

            split_rows(made[:, cut:], half, got[1], own_dp, dp_count, b_send, b_keep)


def attention_backward(own, mixed, do, probs, x, da, wa, wb, gx, got, dp_count, out_type, tile=64):
    rows, width = x.shape
    part = mixed.shape[3]
    _, slots, heads, slot_rows, _ = probs.shape
    chunk_rows, rest = width // dp_count, dp_count // 2
    keep = got is not None
    away = 0 if keep else 1
    block_of = lambda b: 2 * b + away
    row = pl.BlockSpec((slot_rows, width), lambda s, b, o: (s, 0))
    last = slots - 1
    late = lambda s, b: jnp.where(s == last, b, 0)
    in_specs = [
        pl.BlockSpec((None, 3, slot_rows, part), lambda s, b, o: (block_of(b), 0, s, 0)),
        pl.BlockSpec((None, slot_rows, part), lambda s, b, o: (block_of(b), s, 0)),
        pl.BlockSpec(
            (None, None, heads, slot_rows, slot_rows), lambda s, b, o: (block_of(b), s, 0, 0, 0)
        ),
        whole(x),
        pl.BlockSpec((4, None, rows, part), lambda s, b, o: (0, 3, 0, 0), pipeline_mode=pl.Buffered(1)),
        pl.BlockSpec((None, rows, part), lambda s, b, o: (o[0] ^ block_of(late(s, b)), 0, 0)),
        whole(wa),
        whole(wb),
        row,
    ]
    operands = [mixed, do, probs, x, mixed, da, wa, wb, gx]
    sums = shape_of((2, 8, part), WIDE)
    out_specs = [row, pl.BlockSpec(sums.shape, lambda s, b, o: (0, 0, 0))]
    out_shape = [shape_of((rows, width), out_type), sums]
    whole_block = lambda w: pl.BlockSpec((2, rest, chunk_rows, w), lambda s, b, o: (0, 0, 0, 0))
    if keep:
        in_specs.append(
            pl.BlockSpec(
                (None, 2, rest, chunk_rows, width), lambda s, b, o: (late(s, b), 0, 0, 0, 0)
            )
        )
        operands.append(got)
        half = width // 2
        b_block = pl.BlockSpec(
            (None, rest, chunk_rows, half), lambda s, b, o: (late(s, b), 0, 0, 0)
        )
        out_specs += [whole_block(half)] * 2 + [b_block] * 2
        out_shape += [stored((2, rest, chunk_rows, half), LOW)] * 4
    else:
        out_specs.append(
            pl.BlockSpec(
                (None, 2, rest, chunk_rows, width), lambda s, b, o: (late(s, b), 0, 0, 0, 0)
            )
        )
        out_shape.append(stored((2, 2, rest, chunk_rows, width), LOW))
    return call(
        functools.partial(attention_backward_kernel, dp_count=dp_count, tile=tile, keep=keep),
        "attention_backward",
        (slots, 2),
        in_specs,
        out_specs,
        out_shape,
        [
            pltpu.VMEM((heads, slot_rows, slot_rows), WIDE),
            pltpu.VMEM((heads, slot_rows, slot_rows), LOW),
            pltpu.VMEM((2, rows, 3 * part), LOW),
            pltpu.VMEM((width, rows), LOW),
            pltpu.VMEM((width, rows), LOW),
            pltpu.VMEM((slot_rows, width), WIDE),
        ],
        [own],
        operands,
        flops=36 * heads * rows * slot_rows * 256,
    )


def bits_of(axis):
    size = lax.axis_size(axis)
    return [1 << bit for bit in range(size.bit_length() - 1)]


def swap(value, axis, bit):
    size = lax.axis_size(axis)
    return lax.ppermute(value, axis, [(i, i ^ bit) for i in range(size)])


def add_split_kernel(*refs, merge_in, merge_out, extra, late):
    inputs = 2 if merge_in else 4
    outputs = 2 if merge_out else 4
    ins, refs = refs[:inputs], refs[extra:]
    outs = refs[inputs : inputs + outputs]
    kept_ref, send_ref, keep_ref, in_sems, out_sems = refs[inputs + outputs :]
    half = send_ref.shape[1]
    own, loads, got, stores = [], [], [], []
    for part in range(2):
        kept, came = (ins[0].at[part], ins[1].at[part]) if merge_in else ins[2 * part : 2 * part + 2]
        send, keep = (
            (outs[0].at[part], outs[1].at[part]) if merge_out else outs[2 * part : 2 * part + 2]
        )
        got.append(came)
        if late:
            own.append(kept)
        else:
            own.append(kept_ref.at[part])
            loads.append(pltpu.make_async_copy(kept, kept_ref.at[part], in_sems.at[part]))
        stores.append(
            [
                pltpu.make_async_copy(send_ref.at[part], send, out_sems.at[part, 0]),
                pltpu.make_async_copy(keep_ref.at[part], keep, out_sems.at[part, 1]),
            ]
        )
    for copy in loads:
        copy.start()
    for part in range(2):
        if loads:
            loads[part].wait()
        for at, (out, copy) in enumerate(zip((send_ref, keep_ref), stores[part])):
            rows = pl.ds(half * (1 - at), half)
            out[part] = (own[part][rows].astype(WIDE) + got[part][rows].astype(WIDE)).astype(LOW)
            copy.start()
    for copies in stores:
        for copy in copies:
            copy.wait()


def add_split(ins, merge_in, merge_out, arrived, late):
    size, rows, columns = ins[0].shape[-3:]
    half = (size // 2, rows, columns)
    out_shape = [stored((2, *half), LOW)] * 2 if merge_out else [stored(half, LOW)] * 4
    return pl.pallas_call(
        functools.partial(
            add_split_kernel,
            merge_in=merge_in,
            merge_out=merge_out,
            extra=len(arrived),
            late=late,
        ),
        in_specs=[in_vmem() if late else in_hbm(), in_vmem()] * (len(ins) // 2)
        + [in_place()] * len(arrived),
        out_specs=[in_hbm()] * len(out_shape),
        out_shape=out_shape,
        scratch_shapes=[
            pltpu.VMEM((2, size, rows, columns), LOW),
            pltpu.VMEM((2, *half), LOW),
            pltpu.VMEM((2, *half), LOW),
            pltpu.SemaphoreType.DMA((2,)),
            pltpu.SemaphoreType.DMA((2, 2)),
        ],
        compiler_params=pltpu.CompilerParams(vmem_limit_bytes=16 << 20),
        cost_estimate=pl.CostEstimate(flops=0, bytes_accessed=0, transcendentals=0),
        name="add_split",
    )(*ins, *arrived)


class Summing:
    def __init__(self, a_send, a_keep, b_send, b_keep):
        head, dp = bits_of("head"), bits_of("dp")
        self.stages = [(("dp", dp[0]), ("head", head[1]))] + [(("dp", bit),) for bit in dp[1:]]
        self.at = 0
        self.settled = False
        self.kept = [a_keep, b_keep]
        self.got = [swap(a_send, "head", head[1]), swap(b_send, "dp", dp[0])]

    def busy(self):
        return self.at < len(self.stages)

    def step(self, after, arrived=(), late=False):
        stage = self.stages[self.at]
        merge_in, merge_out = len(self.kept) == 1, len(stage) == 1
        ins = [v for pair in zip(self.kept, self.got) for v in pair]
        lead = 1 if merge_in else 0
        ins = [v.reshape(*v.shape[:lead], -1, *v.shape[-2:]) for v in ins]
        ins, _ = lax.optimization_barrier((ins, after))
        outs = add_split(ins, merge_in, merge_out, arrived, late)
        if merge_out:
            self.got, self.kept = [swap(outs[0], *stage[0])], [outs[1]]
        else:
            self.got = [swap(outs[0], *stage[0]), swap(outs[2], *stage[1])]
            self.kept = [outs[1], outs[3]]
        self.at += 1
        return outs[-1]


def last_sums_kernel(*refs, layers):
    ins, outs = refs[: 4 * layers + 2], refs[4 * layers + 2 :]
    qkv, qv, out_w, out_b, gain1, shift1, up_w, up_b, down_w, down_b, gain2, shift2 = outs
    part = out_w.shape[2]
    width = down_b.shape[1]
    rows = ins[-2][...] + ins[-1][...]
    for layer in range(layers):
        ffn_kept, ffn_got, wide_kept, wide_got = ins[4 * layer : 4 * layer + 4]
        down_w[layer] = ffn_kept[0, 0].astype(WIDE) + ffn_got[0, 0].astype(WIDE)
        up_w[layer] = ffn_kept[1, 0].astype(WIDE) + ffn_got[1, 0].astype(WIDE)
        for half in range(2):
            both = wide_kept[half, 0].astype(WIDE) + wide_got[half, 0].astype(WIDE)
            for at in range(2):
                which = 2 * half + at
                block = both[:, at * part : (at + 1) * part]
                if which < 3:
                    qkv[layer, which] = block
                else:
                    out_w[layer] = block
        for row, out in enumerate((gain2, shift2, down_b, gain1, shift1, out_b)):
            out[layer : layer + 1] = rows[layer, row : row + 1]
        qv[layer] = rows[layer, 6:8]
        for row in range(up_b.shape[1] // width):
            at = slice(row * width, (row + 1) * width)
            up_b[layer : layer + 1, at] = rows[layer, 8 + row : 9 + row]


def last_sums(groups, small, passing):
    layers, _, width = small.shape
    ins, specs = [], []
    for group in groups:
        ins += [group.kept[0], group.got[0]]
    ins = [v.reshape(2, 1, *v.shape[-2:]) for v in ins] + [small, passing]
    rows, part = ins[0].shape[2], ins[2].shape[3] // 2
    hidden = (small.shape[1] - 8) * width
    shapes = [
        (layers, 3, rows, part),
        (layers, 2, width),
        (layers, rows, part),
        (layers, width),
        (layers, width),
        (layers, width),
        (layers, rows, width),
        (layers, hidden),
        (layers, rows, width),
        (layers, width),
        (layers, width),
        (layers, width),
    ]
    spec = lambda shape: pl.BlockSpec(shape, lambda i: (0,) * len(shape))
    specs = [spec(v.shape) for v in ins]
    return call(
        functools.partial(last_sums_kernel, layers=layers),
        "last_sums",
        (1,),
        specs,
        [spec(shape) for shape in shapes],
        [shape_of(shape, WIDE) for shape in shapes],
        [],
        [],
        ins,
        vmem=24 << 20,
    )


def ordered(after, *values):
    values, _ = lax.optimization_barrier((values, after))
    return values


def near_blocks(block, after):
    low, high = bits_of("head")
    near = swap(block, "head", low)
    (later,) = ordered((after, near), block)
    return block, near, swap(later, "head", high)


def gathered_pairs(block, after):
    own, near, far = near_blocks(block, after)
    return jnp.stack([own, near]), jnp.stack([far, swap(far, "head", bits_of("head")[0])])


def on_device(
    tokens,
    seq_lengths,
    qkv_weight,
    qv_bias,
    out_weight,
    out_bias,
    norm1_gain,
    norm1_shift,
    up_weight,
    up_bias,
    down_weight,
    down_bias,
    norm2_gain,
    norm2_shift,
    out_grad,
):
    head_count, dp_count = lax.axis_size("head"), lax.axis_size("dp")
    head_index, dp_index = lax.axis_index("head"), lax.axis_index("dp")
    own = jnp.stack([head_index, dp_index]).astype(jnp.int32)
    local_rows, width = tokens.shape
    slot_rows = local_rows * head_count // seq_lengths.shape[0]
    slots = local_rows // slot_rows
    layers = qkv_weight.shape[0]
    part = width // head_count
    turned = jnp.swapaxes(qkv_weight, 2, 3).reshape(layers, 3 * part, width)
    base = (head_index * slots).astype(jnp.int32).reshape(1)
    bias = mask_bias(seq_lengths, base, slots, slot_rows)
    weights = [near_blocks(turned[0], base)]
    near_bias, far_bias = gathered_pairs(qv_bias[:, :, None], base)
    up_rows = up_bias.reshape(layers, -1, 1, width)
    rounded, residual = tokens, tokens
    kept = []
    for layer in range(layers):
        before = max(layer - 1, 0)
        small = jnp.stack(
            [
                out_bias[layer],
                norm1_gain[layer],
                norm1_shift[layer],
                down_bias[layer],
                norm2_gain[layer],
                norm2_shift[layer],
                norm2_gain[before],
                norm2_shift[before],
            ]
        )
        own_w, near_w, far_w = weights[layer]
        if layer == 0:
            near = attention_forward(rounded, (own_w, near_w), near_bias[:, layer], bias, 0, None)
            (far_w, far_b) = ordered(near[0], far_w, far_bias[:, layer])
            both_w = swap(far_w, "head", bits_of("head")[0])
            for other in range(1, layers):
                (later,) = ordered(near[0], turned[other])
                weights.append(near_blocks(later, near[0]))
            mixed, probs = attention_forward(rounded, (far_w, both_w), far_b, bias, 2, near)
        else:
            both_w = both_ws[layer - 1]
            all_bias = jnp.concatenate([near_bias[:, layer], far_bias[:, layer]])
            mixed, probs = attention_forward(
                rounded, (own_w, near_w, far_w, both_w), all_bias, bias, 0, None
            )
        weights[layer] = w = (own_w, near_w, far_w, both_w)
        u1, hr, gr, slope, u2, low = ffn_forward(
            own,
            mixed,
            residual,
            out_weight,
            up_weight,
            down_weight,
            up_rows[layer],
            small,
            layer,
            layer > 0,
        )
        kept.append((rounded, mixed, probs, u1, hr, gr, slope, u2))
        rounded, residual = low, u2
        if layer == 0:
            (far_ws,) = ordered(u2, [w[2] for w in weights[1:]])
            both_ws = [swap(w, "head", bits_of("head")[0]) for w in far_ws]
    out_state = rounded
    grad_state = out_grad
    small_sums = [None] * layers
    hidden_sums = [None] * layers
    ffn_groups, wide_groups = [None] * layers, [None] * layers
    running = []

    def advance(after, late=False):
        arrived = []
        for group in running:
            if not group.busy() and not group.settled:
                arrived += group.got
                group.settled = True
        for group in running:
            if group.busy():
                after = group.step(after, arrived, late)
                arrived = []
        return after

    for layer in reversed(range(layers)):
        rounded, mixed, probs, u1, hr, gr, slope, u2 = kept[layer]
        w = weights[layer]
        gains = jnp.stack([norm1_gain[layer], norm2_gain[layer]])
        da, do, du, sums, zsums, sent, ffn_kept = ffn_backward(
            own,
            grad_state,
            u2,
            u1,
            slope,
            hr,
            gr,
            out_weight,
            up_weight,
            down_weight,
            gains,
            layer,
            dp_count,
        )
        low_bit = bits_of("head")[0]
        early = bool(running)
        token = advance(do)
        if early:
            (sent,) = ordered(token, sent)
        got = swap(sent, "head", low_bit)

        def sum_ffn(after):
            values = ordered(after, ffn_kept, got)
            up_send, up_keep, down_send, down_keep = core_add(*values)
            ffn_groups[layer] = Summing(down_send, down_keep, up_send, up_keep)
            running.insert(0, ffn_groups[layer])
            return down_keep

        if early:
            token = sum_ffn(token)
        (do, du) = ordered(token, do, du)
        half_grad, away_sums, sent = attention_backward(
            own, mixed, do, probs, rounded, da, w[1], w[3], du, None, dp_count, WIDE
        )
        if early:
            token = advance(half_grad)
            (sent,) = ordered(token, sent)
            wide_got = swap(sent, "head", low_bit)
        else:
            wide_got = swap(sent, "head", low_bit)
            token = sum_ffn(half_grad)
        (half_grad, do) = ordered(token, half_grad, do)
        grad_state, own_sums, *parts = attention_backward(
            own,
            mixed,
            do,
            probs,
            rounded,
            da,
            w[0],
            w[2],
            half_grad,
            wide_got,
            dp_count,
            WIDE if layer else LOW,
        )
        wide_groups[layer] = Summing(*parts)
        token = advance(grad_state) if layer else grad_state
        if layer:
            (grad_state,) = ordered(token, grad_state)
        running.append(wide_groups[layer])
        blocks = [own_sums[0], away_sums[0], own_sums[1], away_sums[1]]
        stacked = jnp.stack(blocks)[:, :2]
        qv_sums = jnp.concatenate(
            [
                lax.dynamic_index_in_dim(stacked, head_index ^ head, 0, keepdims=False)
                for head in range(head_count)
            ],
            axis=1,
        )
        small_sums[layer] = jnp.concatenate([sums[:6], qv_sums, zsums[:, 0]])
    small_sum = jnp.stack(small_sums)
    near, far = bits_of("head")
    waiting = [[("head", near)], [("dp", 1)], [("head", far)], [("dp", 2 * k) for k in range(1, dp_count // 2)]]
    passing = [swap(small_sum, *one) for one in waiting.pop(0)]
    while any(not group.settled for group in running) or waiting:
        if any(group.busy() for group in running):
            token = advance(token, True)
        elif not waiting:
            break
        if waiting:
            small_sum, passing = ordered(token, small_sum, passing)
            small_sum = sum(passing, small_sum)
            token = small_sum
            passing = [swap(small_sum, *one) for one in waiting.pop(0)]
    small_sum, passing = sum(passing[:-1], small_sum), passing[-1]
    groups = [group for pair in zip(ffn_groups, wide_groups) for group in pair]
    qkv, qv, out_w, out_b, gain1, shift1, up_w, up_b, down_w, down_b, gain2, shift2 = last_sums(
        groups, small_sum, passing
    )
    return (
        out_state,
        grad_state,
        qkv,
        qv,
        out_w,
        out_b,
        gain1,
        shift1,
        up_w,
        up_b,
        jnp.swapaxes(down_w, 1, 2),
        down_b,
        gain2,
        shift2,
    )


def solution(mesh):
    in_specs = (
        P(("dp", "head"), None),
        P("dp", None),
        P(None, None, None, "head"),
        P(None, None, "head"),
        P(),
        P(),
        P(),
        P(),
        P(),
        P(),
        P(),
        P(),
        P(),
        P(),
        P(("dp", "head"), None),
    )
    out_specs = (
        P(("dp", "head"), None),
        P(("dp", "head"), None),
        P(None, None, "dp", "head"),
        P(),
        P(None, "dp", "head"),
        P(),
        P(),
        P(),
        P(None, "dp", "head"),
        P(),
        P(None, "head", "dp"),
        P(),
        P(),
        P(),
    )
    return jax.shard_map(
        on_device, mesh=mesh, in_specs=in_specs, out_specs=out_specs, check_vma=False
    )
```
